32 devices in a mesh: dp: 8 (over z, y), tensor: 4 (over x, core).
Axes of the slice: x: 2, y: 2, z: 4, core: 2. Of those that a mesh axis runs over, the one named last changes fastest.
Arguments:
- layer_in: bfloat16 [24576, 768], P(('dp', 'tensor')), may hold values from -6 to 6
- prompt_len: int32 [8], P('dp'), may hold values from 512 to 1024, as said below
- cont_len: int32 [8, 8], P('dp'), may hold values from 128 to 256, as said below
- w_qkv: bfloat16 [3, 768, 768], P(None, None, 'tensor'), may hold values from -0.21875 to 0.21875
- b_qv: bfloat16 [2, 768], P(None, 'tensor'), may hold values from -3 to 3
- w_proj: bfloat16 [768, 768], P('tensor'), may hold values from -1.75 to 1.75
- b_proj: bfloat16 [768], replicated, may hold values from -2 to 2
- ln1_gain: bfloat16 [768], replicated, may hold values from 0.25 to 1.75
- ln1_bias: bfloat16 [768], replicated, may hold values from -2 to 2
- ln2_gain: bfloat16 [768], replicated, may hold values from 0.25 to 1.75
- ln2_bias: bfloat16 [768], replicated, may hold values from -2 to 2
- w_in: bfloat16 [768, 3072], P(None, 'tensor'), may hold values from -0.21875 to 0.21875
- b_in: bfloat16 [3072], P('tensor'), may hold values from -2 to 2
- w_out: bfloat16 [3072, 768], P('tensor'), may hold values from -0.109375 to 0.109375
- b_out: bfloat16 [768], replicated, may hold values from -2 to 2
- out_grad: bfloat16 [24576, 768], P(('dp', 'tensor')), may hold values from -6 to 6
Outputs:
- layer_out: bfloat16 [24576, 768], P(('dp', 'tensor'))
- in_grad: float32 [24576, 768], P(('dp', 'tensor'))
- grad_w_qkv: float32 [3, 768, 768], P(None, None, 'tensor')
- grad_b_qv: float32 [2, 768], P(None, 'tensor')
- grad_w_proj: float32 [768, 768], P('tensor')
- grad_b_proj: float32 [768], replicated
- grad_ln1_gain: float32 [768], replicated
- grad_ln1_bias: float32 [768], replicated
- grad_ln2_gain: float32 [768], replicated
- grad_ln2_bias: float32 [768], replicated
- grad_w_in: float32 [768, 3072], P(None, 'tensor')
- grad_b_in: float32 [3072], P('tensor')
- grad_w_out: float32 [3072, 768], P('tensor')
- grad_b_out: float32 [768], replicated
The draws below stay inside these ranges and needn't reach their ends.
Inputs may be any that keep to these rules, and one draw needn't show every extreme that they name: `prompt_len`: in every draw some group's prompt has all 1024 rows valid. `cont_len`: in every group some continuation has all 256 rows valid.
All inputs are finite; a program needn't handle non-finite values.
Results may differ from the reference program's by a relative error of at most 0.018.
Values may be sent and summed in bfloat16 or wider, within the bound.
A program may use at most 192 MiB of HBM per device.

```python
import jax
import jax.numpy as jnp
from jax import lax

D = 768
HEADS = 12
HEAD = 64
FF = 3072
PROMPT = 1024
CONT = 8
CLEN = 256
ROWS = 3072
GROUPS = 8


def draw_prompt_len(key, part):
    first_key, second_key = jax.random.split(jax.random.fold_in(key, 17))
    drawn_lens = jax.random.randint(first_key, (GROUPS,), PROMPT // 2, PROMPT + 1)
    chosen = jax.random.randint(second_key, (), 0, GROUPS)
    return jnp.where(jnp.arange(GROUPS) == chosen, PROMPT, drawn_lens).astype(jnp.int32)


def draw_cont_len(key, part):
    first_key, second_key = jax.random.split(jax.random.fold_in(key, 29))
    drawn_lens = jax.random.randint(first_key, (GROUPS, CONT), CLEN // 2, CLEN + 1)
    chosen = jax.random.randint(second_key, (GROUPS, 1), 0, CONT)
    return jnp.where(jnp.arange(CONT)[None, :] == chosen, CLEN, drawn_lens).astype(jnp.int32)


def block_scale(rng, dims, cuts, least, largest):
    def one(axis_at, parts):
        steps = jax.random.uniform(jax.random.fold_in(jax.random.fold_in(rng, 6), axis_at), (parts,), jnp.float32, least / len(cuts), largest / len(cuts))
        return jnp.repeat(jnp.exp(steps), dims[axis_at] // parts).reshape((-1,) + (1,) * (len(dims) - axis_at - 1))

    level = one(*cuts[0])
    for cut in cuts[1:]:
        level = level * one(*cut)
    return level


def noise(stream_key, extent, width, bound, cuts=(), kind=jnp.bfloat16):
    level = block_scale(stream_key, extent, cuts, -0.22, 0.18) if cuts else 1.0
    values = jax.random.normal(stream_key, extent, jnp.float32) * width * level
    return jnp.minimum(jnp.maximum(values, -bound), bound).astype(kind)


def setup_inputs(seed: int = 0) -> dict:
    streams_of = jax.random.split(jax.random.key(seed), 17)
    layer_in = noise(streams_of[0], (GROUPS * ROWS, D), 1.0, 6.0, ((0, 32),))
    prompt_len = draw_prompt_len(jax.random.fold_in(streams_of[16], 71), 0)
    cont_len = draw_cont_len(jax.random.fold_in(streams_of[16], 71), 0)
    w_qkv = noise(streams_of[3], (3, D, D), D ** -0.5, 0.21875, ((2, 4),))
    b_qv = noise(streams_of[4], (2, D), 0.5, 3.0, ((1, 4),))
    w_proj = noise(streams_of[5], (D, D), (max(D // 64, 1)) ** -0.5, 1.75, ((0, 4),))
    b_proj = noise(streams_of[6], (D,), 0.3, 2.0)
    ln1_gain = jnp.clip(1.0 + 0.15 * jax.random.normal(streams_of[7], (D,), jnp.float32), 0.25, 1.75).astype(jnp.bfloat16)
    ln1_bias = noise(streams_of[8], (D,), 0.3, 2.0)
    ln2_gain = jnp.clip(1.0 + 0.15 * jax.random.normal(streams_of[9], (D,), jnp.float32), 0.25, 1.75).astype(jnp.bfloat16)
    ln2_bias = noise(streams_of[10], (D,), 0.3, 2.0)
    w_in = noise(streams_of[11], (D, FF), D ** -0.5, 0.21875, ((1, 4),))
    b_in = noise(streams_of[12], (FF,), 0.3, 2.0, ((0, 4),))
    w_out = noise(streams_of[13], (FF, D), FF ** -0.5, 0.109375, ((0, 4),))
    b_out = noise(streams_of[14], (D,), 0.3, 2.0)
    out_grad = noise(streams_of[15], (GROUPS * ROWS, D), 1.0, 6.0, ((0, 32),))
    return {"layer_in": layer_in, "prompt_len": prompt_len, "cont_len": cont_len, "w_qkv": w_qkv, "b_qv": b_qv, "w_proj": w_proj, "b_proj": b_proj, "ln1_gain": ln1_gain, "ln1_bias": ln1_bias, "ln2_gain": ln2_gain, "ln2_bias": ln2_bias, "w_in": w_in, "b_in": b_in, "w_out": w_out, "b_out": b_out, "out_grad": out_grad}


@jax.custom_vjp
def low(v):
    return lax.optimization_barrier(v.astype(jnp.bfloat16)).astype(jnp.float32)

@jax.custom_vjp
def low_back(v):
    return v

def low_keep(v):
    return (low(v), None)

def low_pass(kept, grad):
    return (grad,)

def back_keep(v):
    return (v, None)

def back_low(kept, grad):
    return (low(grad),)
low.defvjp(low_keep, low_pass)
low_back.defvjp(back_keep, back_low)
epsilon = 1e-06
masked_score = -1000000000.0
highest = lax.Precision.HIGHEST

def layer_norm(values, gain, shift):
    mean_row = lax.optimization_barrier(jnp.mean(values, axis=-1, keepdims=True))
    centred = values - mean_row
    spread = lax.optimization_barrier(jnp.mean(centred * centred, axis=-1, keepdims=True))
    return centred * lax.rsqrt(spread + epsilon) * gain + shift

def attend(queries, key_rows, value_rows, allowed):
    scores = jnp.einsum('bqhe,bkhe->bhqk', queries, key_rows, precision=highest) * 0.125
    scores = low_back(scores)
    scores = jnp.where(allowed[:, None, None, :], scores, masked_score)
    attn_prob = low(jax.nn.softmax(scores, axis=-1))
    return jnp.einsum('bhqk,bkhe->bqhe', attn_prob, value_rows, precision=highest)

def pair_keys(prompt_part, own_part):
    return jnp.concatenate([jnp.broadcast_to(prompt_part, (2,) + prompt_part.shape[1:]), own_part], axis=1)

def pair_mask(prompt_valid, own_valid):
    return jnp.concatenate([jnp.broadcast_to(prompt_valid[None], (2, PROMPT)), own_valid], axis=1)

def group_layer(rows_in, group_prompt, group_conts, params):
    w_qkv, b_qv, w_proj, b_proj, ln1_gain, ln1_bias, ln2_gain, ln2_bias, w_in, b_in, w_out, b_out = params
    block_rows = min(512, PROMPT)
    blocks = PROMPT // block_rows
    pair_count = CONT // 2
    attn_input = low(layer_norm(rows_in, ln1_gain, ln1_bias))
    projected = jnp.einsum('rd,sdf->srf', attn_input, w_qkv, precision=highest)
    queries = low_back(low(projected[0] + b_qv[0])).reshape(ROWS, HEADS, HEAD)
    key_rows = low_back(low(projected[1])).reshape(ROWS, HEADS, HEAD)
    value_rows = low_back(low(projected[2] + b_qv[1])).reshape(ROWS, HEADS, HEAD)
    prompt_valid = jnp.arange(PROMPT) < group_prompt
    own_valid = (jnp.arange(CLEN)[None, :] < group_conts[:, None]).reshape(pair_count, 2, CLEN)
    prompt_keys = key_rows[:PROMPT][None]
    prompt_values = value_rows[:PROMPT][None]

    def prompt_block(block_query):
        return attend(block_query, prompt_keys, prompt_values, prompt_valid[None])
    prompt_ctx = lax.map(jax.checkpoint(prompt_block), queries[:PROMPT].reshape(blocks, 1, block_rows, HEADS, HEAD))

    def cont_block(pieces):
        block_query, own_keys, own_values, own_mask = pieces
        return attend(block_query, pair_keys(prompt_keys, own_keys), pair_keys(prompt_values, own_values), pair_mask(prompt_valid, own_mask))

    def cont_rows(whole):
        return whole[PROMPT:].reshape(pair_count, 2, CLEN, HEADS, HEAD)
    cont_ctx = lax.map(jax.checkpoint(cont_block), (cont_rows(queries), cont_rows(key_rows), cont_rows(value_rows), own_valid))
    context = jnp.concatenate([prompt_ctx.reshape(PROMPT, D), cont_ctx.reshape(CONT * CLEN, D)], axis=0)
    context = low_back(low(context))
    attn_out = low_back(jnp.dot(context, w_proj, precision=highest) + b_proj)
    hidden = rows_in + attn_out
    mlp_input = low(layer_norm(hidden, ln2_gain, ln2_bias))
    pre_act = low_back(jnp.dot(mlp_input, w_in, precision=highest) + b_in)
    gelu_rows = low(jax.nn.gelu(pre_act, approximate=False))
    branch = low_back(jnp.dot(gelu_rows, w_out, precision=highest) + b_out)
    return hidden + branch

def reference(layer_in, prompt_len, cont_len, w_qkv, b_qv, w_proj, b_proj, ln1_gain, ln1_bias, ln2_gain, ln2_bias, w_in, b_in, w_out, b_out, out_grad):
    params = tuple((weight_arg.astype(jnp.float32) for weight_arg in (w_qkv, b_qv, w_proj, b_proj, ln1_gain, ln1_bias, ln2_gain, ln2_bias, w_in, b_in, w_out, b_out)))
    rows_in = layer_in.astype(jnp.float32).reshape(GROUPS, ROWS, D)

    def forward(rows_all, weights):

        def one_group(pieces):
            return group_layer(pieces[0], pieces[1], pieces[2], weights)
        return lax.map(jax.checkpoint(one_group), (rows_all, prompt_len, cont_len))
    result, pullback = jax.vjp(forward, rows_in, params)
    grad_rows, grads = pullback(out_grad.astype(jnp.float32).reshape(GROUPS, ROWS, D))
    return (result.reshape(GROUPS * ROWS, D).astype(jnp.bfloat16), grad_rows.reshape(GROUPS * ROWS, D), grads[0], grads[1], grads[2], grads[3], grads[4], grads[5], grads[6], grads[7], grads[8], grads[9], grads[10], grads[11])
```

```python
import jax
import jax.numpy as jnp
from jax import lax
from jax.experimental import pallas as pl
from jax.experimental.pallas import tpu as pltpu
from jax.sharding import PartitionSpec as P

HEAD = 64
PROMPT = 1024
CONT = 8
CLEN = 256
PIECES = 4

EPS = 1e-06
MASKED = -1000000000.0
BF = jnp.bfloat16
F32 = jnp.float32


def nt(a, b):
    return lax.dot_general(a, b, (((1,), (1,)), ((), ())), preferred_element_type=F32)


def nn(a, b):
    return lax.dot_general(a, b, (((1,), (0,)), ((), ())), preferred_element_type=F32)


def tn(a, b):
    return lax.dot_general(a, b, (((0,), (0,)), ((), ())), preferred_element_type=F32)


def own_lanes(rows, h):
    lane = lax.broadcasted_iota(jnp.int32, (rows, 128), 1)
    return ((lane < 64) if h == 0 else (lane >= 64)), lane - (64 if h == 0 else 0)


def key_aug(k, h, length, base):
    rows = k.shape[0]
    own, extra = own_lanes(rows, h)
    row = lax.broadcasted_iota(jnp.int32, (rows, 128), 0) + base
    bias = jnp.where(jnp.logical_and(extra == 0, row >= length), MASKED, 0.0)
    return jnp.where(own, k.astype(F32), bias).astype(BF)


def query_aug(q, h):
    own, extra = own_lanes(q.shape[0], h)
    return jnp.where(own, q.astype(F32) * 0.125, jnp.where(extra == 0, 1.0, 0.0)).astype(BF)


def value_aug(v, h):
    own, extra = own_lanes(v.shape[0], h)
    ones = jnp.where(jnp.logical_and(extra >= 0, extra < 3), 1.0, 0.0)
    return jnp.where(own, v.astype(F32), ones).astype(BF)


def transposed(v):
    return v.astype(F32).T


def attn_fwd_kernel(lens, q_ref, kp_ref, vp_ref, ko_ref, vo_ref, ctx_ref, lse_ref, kph, vpt):
    blocks = q_ref.shape[0] // CLEN
    prompt = kp_ref.shape[0]
    vt = transposed(vp_ref[...])
    for h in range(2):
        kph[h] = key_aug(kp_ref[...], h, lens[0], 0)
        vpt[h] = jnp.concatenate([vt[64 * h : 64 * h + 64].astype(BF), jnp.ones((16, prompt), BF)], axis=0)

    def block(b, _):
        rows = pl.ds(pl.multiple_of(b * CLEN, CLEN), CLEN)
        q = q_ref[rows, :]
        ko = ko_ref[rows, :]
        vot = transposed(vo_ref[rows, :])
        outs, logs = [], []
        for h in range(2):
            qh = query_aug(q, h)
            vh = jnp.concatenate([vot[64 * h : 64 * h + 64].astype(BF), jnp.ones((16, CLEN), BF)], axis=0)
            sp = nt(kph[h], qh)
            so = nt(key_aug(ko, h, lens[1 + b], 0), qh)
            top = jnp.maximum(jnp.max(sp, axis=0, keepdims=True), jnp.max(so, axis=0, keepdims=True))
            pp = jnp.exp(sp - top).astype(BF)
            po = jnp.exp(so - top).astype(BF)
            ot = nn(vpt[h], pp) + nn(vh, po)
            total = ot[64:65]
            outs.append(ot[:64] * (1.0 / total))
            logs.append(top + jnp.log(total))
        ctx_ref[rows, :] = jnp.concatenate(outs, axis=0).T.astype(BF)
        lse_ref[0, b] = jnp.concatenate(logs + [jnp.zeros((6, CLEN), F32)], axis=0)
        return 0

    lax.fori_loop(0, blocks, block, 0)


def attn_bwd_kernel(lens, q_ref, kp_ref, vp_ref, ko_ref, vo_ref, do_ref, ctx_ref, lse_ref,
                    dq_ref, dkp_ref, dvp_ref, dko_ref, dvo_ref, qh_s, doh_s, dqt):
    rows_all = q_ref.shape[0]
    blocks = rows_all // CLEN
    chunks = kp_ref.shape[0] // CLEN
    prod = do_ref[...].astype(F32) * ctx_ref[...].astype(F32)
    for h in range(2):
        own, extra = own_lanes(rows_all, h)
        qh_s[h] = query_aug(q_ref[...], h)
        d = -jnp.sum(jnp.where(own, prod, 0.0), axis=1, keepdims=True)
        hi = d.astype(BF).astype(F32)
        mid = (d - hi).astype(BF).astype(F32)
        low = d - hi - mid
        aug = jnp.where(extra == 0, hi, jnp.where(extra == 1, mid, jnp.where(extra == 2, low, 0.0)))
        doh_s[h] = jnp.where(own, do_ref[...].astype(F32), aug).astype(BF)
    first = lax.broadcasted_iota(jnp.int32, (CLEN, 128), 1) < 64

    def own_block(b, _):
        rows = pl.ds(pl.multiple_of(b * CLEN, CLEN), CLEN)
        q = q_ref[rows, :]
        k = ko_ref[rows, :]
        v = vo_ref[rows, :]
        do = do_ref[rows, :]
        kt = transposed(k).astype(BF)
        dks, dvs, dqs = [], [], []
        for h in range(2):
            s = nt(key_aug(k, h, lens[1 + b], 0), qh_s[h, rows, :])
            p = jnp.exp(s - lse_ref[0, b, h : h + 1, :])
            dp = nt(value_aug(v, h), doh_s[h, rows, :])
            ds = (p * dp).astype(BF)
            dvs.append(nn(p.astype(BF), do))
            dks.append(nn(ds, q))
            dqs.append(nn(kt[64 * h : 64 * h + 64], ds))
        dvo_ref[rows, :] = jnp.where(first, dvs[0], dvs[1]).astype(BF)
        dko_ref[rows, :] = (jnp.where(first, dks[0], dks[1]) * 0.125).astype(BF)
        dqt[b] = jnp.concatenate(dqs, axis=0)
        return 0

    lax.fori_loop(0, blocks, own_block, 0)

    def chunk(c, _):
        rows = pl.ds(pl.multiple_of(c * CLEN, CLEN), CLEN)
        k = kp_ref[rows, :]
        v = vp_ref[rows, :]
        kt = transposed(k).astype(BF)
        dks, dvs = [], []
        for h in range(2):
            kh = key_aug(k, h, lens[0], c * CLEN)
            vh = value_aug(v, h)
            dk = dv = None
            for b in range(blocks):
                rb = pl.ds(b * CLEN, CLEN)
                s = nt(kh, qh_s[h, rb, :])
                p = jnp.exp(s - lse_ref[0, b, h : h + 1, :])
                dp = nt(vh, doh_s[h, rb, :])
                ds = (p * dp).astype(BF)
                dv_b = nn(p.astype(BF), do_ref[rb, :])
                dk_b = nn(ds, q_ref[rb, :])
                dv = dv_b if b == 0 else dv + dv_b
                dk = dk_b if b == 0 else dk + dk_b
                dqt[b, 64 * h : 64 * h + 64] += nn(kt[64 * h : 64 * h + 64], ds)
            dvs.append(dv)
            dks.append(dk)
        dvp_ref[rows, :] = jnp.where(first, dvs[0], dvs[1]).astype(BF)
        dkp_ref[rows, :] = (jnp.where(first, dks[0], dks[1]) * 0.125).astype(BF)
        return 0

    lax.fori_loop(0, chunks, chunk, 0)
    for b in range(blocks):
        dq_ref[b * CLEN : (b + 1) * CLEN, :] = (dqt[b].T * 0.125).astype(BF)


def attn_specs(rows, prompt, blocks):
    def col(n):
        return pl.BlockSpec((n, 128), lambda i, l: (0, i))

    logs = pl.BlockSpec((1, blocks, 8, CLEN), lambda i, l: (i, 0, 0, 0))
    return col(rows), col(prompt), logs


def attn_fwd(lens, q, kp, vp, ko, vo):
    rows, width = q.shape
    prompt = kp.shape[0]
    blocks = rows // CLEN
    pairs = width // 128
    r, p, logs = attn_specs(rows, prompt, blocks)
    cells = rows * (prompt + CLEN) * pairs * 2
    return pl.pallas_call(
        attn_fwd_kernel,
        out_shape=(
            jax.ShapeDtypeStruct((rows, width), BF),
            jax.ShapeDtypeStruct((pairs, blocks, 8, CLEN), F32),
        ),
        grid_spec=pltpu.PrefetchScalarGridSpec(
            num_scalar_prefetch=1,
            grid=(pairs,),
            in_specs=[r, p, p, r, r],
            out_specs=[r, logs],
            scratch_shapes=[pltpu.VMEM((2, prompt, 128), BF), pltpu.VMEM((2, 80, prompt), BF)],
        ),
        compiler_params=pltpu.CompilerParams(vmem_limit_bytes=40 << 20),
        cost_estimate=pl.CostEstimate(
            flops=cells * 256 * 4, transcendentals=cells, bytes_accessed=2 * width * (4 * rows + 2 * prompt)
        ),
        name="attn_fwd",
    )(lens, q, kp, vp, ko, vo)


def attn_bwd(lens, q, kp, vp, ko, vo, do, ctx, lse):
    rows, width = q.shape
    prompt = kp.shape[0]
    blocks = rows // CLEN
    pairs = width // 128
    r, p, logs = attn_specs(rows, prompt, blocks)
    cells = rows * (prompt + CLEN) * pairs * 2

    def shape(n):
        return jax.ShapeDtypeStruct((n, width), BF)

    return pl.pallas_call(
        attn_bwd_kernel,
        out_shape=(shape(rows), shape(prompt), shape(prompt), shape(rows), shape(rows)),
        grid_spec=pltpu.PrefetchScalarGridSpec(
            num_scalar_prefetch=1,
            grid=(pairs,),
            in_specs=[r, p, p, r, r, r, r, logs],
            out_specs=[r, p, p, r, r],
            scratch_shapes=[
                pltpu.VMEM((2, rows, 128), BF),
                pltpu.VMEM((2, rows, 128), BF),
                pltpu.VMEM((blocks, 128, CLEN), F32),
            ],
        ),
        compiler_params=pltpu.CompilerParams(vmem_limit_bytes=40 << 20),
        cost_estimate=pl.CostEstimate(
            flops=cells * 256 * 10, transcendentals=cells, bytes_accessed=2 * width * (8 * rows + 4 * prompt)
        ),
        name="attn_bwd",
    )(lens, q, kp, vp, ko, vo, do, ctx, lse)


def swap(v, axis, bit):
    return lax.ppermute(v, axis, [(i, i ^ bit) for i in range(lax.axis_size(axis))])


def gather_pieces(own):
    side = swap(own, "tensor", 1)
    across = swap(own, "tensor", 2)
    return [own, side, across, swap(across, "tensor", 1)]


def tensor_sum(pieces):
    g0, g1, g2, g3 = pieces
    r1 = swap(g1.astype(BF), "tensor", 1)
    r3 = swap(g3.astype(BF), "tensor", 1)
    r2 = swap((g2 + r3.astype(F32)).astype(BF), "tensor", 2)
    return g0 + r1.astype(F32) + r2.astype(F32)


def dp_sum(total):
    size = lax.axis_size("dp")
    me = lax.axis_index("dp")
    bits = [b for b in range(size.bit_length()) if (1 << b) < size]
    value = total
    for b in bits:
        half = value.shape[0] // 2
        upper = (me >> b) & 1
        low, high = value[:half], value[half:]
        away = jnp.where(upper == 0, high, low).astype(BF)
        keep = jnp.where(upper == 0, low, high)
        value = keep + swap(away, "dp", 1 << b).astype(F32)
    value = value.astype(BF)
    for b in reversed(bits):
        upper = (me >> b) & 1
        other = swap(value, "dp", 1 << b)
        value = jnp.concatenate([jnp.where(upper == 0, value, other), jnp.where(upper == 0, other, value)], axis=0)
    return value.astype(F32)


def normalize(values):
    centred = values - jnp.mean(values, axis=-1, keepdims=True)
    scale = lax.rsqrt(jnp.mean(centred * centred, axis=-1, keepdims=True) + EPS)
    return centred * scale, scale


def norm_back(grad, normal, scale, gain):
    e = grad * gain
    back = scale * (e - jnp.mean(e, axis=-1, keepdims=True) - normal * jnp.mean(e * normal, axis=-1, keepdims=True))
    return back, jnp.sum(grad * normal, axis=0), jnp.sum(grad, axis=0)


def shards(layer_in, prompt_len, cont_len, w_qkv, b_qv, w_proj, b_proj, ln1_gain, ln1_bias,
           ln2_gain, ln2_bias, w_in, b_in, w_out, b_out, out_grad):
    rows, width = layer_in.shape
    blocks = rows // CLEN
    t = lax.axis_index("tensor")
    odd = (t & 1) == 1
    half_prompt = PROMPT // 2
    g1, c1, g2, c2 = (v.astype(F32) for v in (ln1_gain, ln1_bias, ln2_gain, ln2_bias))

    beside = swap(layer_in, "tensor", 1)
    even_rows = jnp.where(odd, beside, layer_in)
    odd_rows = jnp.where(odd, layer_in, beside)
    here = jnp.concatenate([even_rows, odd_rows[: PROMPT - rows]], axis=0)
    part = jnp.where(odd, here[half_prompt:], here[:half_prompt])
    came = lax.ppermute(part, "tensor", [(0, 2), (1, 3)])
    came_beside = swap(came, "tensor", 1)
    there = jnp.concatenate([jnp.where(odd, came_beside, came), jnp.where(odd, came, came_beside)], axis=0)
    prompt_rows = jnp.where(t < 2, here, there)

    bias_rows = jnp.stack([b_qv[0], jnp.zeros_like(b_qv[0]), b_qv[1]], axis=0)[:, None, :]
    qkv_pack = jnp.concatenate([w_qkv, jnp.pad(bias_rows, ((0, 0), (0, 15), (0, 0)))], axis=1)
    qkv_pieces = gather_pieces(qkv_pack)
    proj_pieces = gather_pieces(w_proj)
    in_pieces = gather_pieces(jnp.concatenate([w_in, jnp.pad(b_in[None], ((0, 15), (0, 0)))], axis=0))
    out_pieces = gather_pieces(w_out)

    rows_in = layer_in.astype(F32)
    normal1, scale1 = normalize(rows_in)
    attn_input = (normal1 * g1 + c1).astype(BF)
    normal_p, _ = normalize(prompt_rows.astype(F32))
    prompt_input = (normal_p * g1 + c1).astype(BF)

    group = t * blocks + jnp.arange(blocks)
    conts = group - PROMPT // CLEN
    own_len = jnp.where(conts >= 0, cont_len[0][jnp.clip(conts, 0, CONT - 1)], 0)
    lens = jnp.concatenate([prompt_len, own_len]).astype(jnp.int32)

    units = []
    for u in range(2):
        pack = jnp.concatenate([qkv_pieces[2 * u], qkv_pieces[2 * u + 1]], axis=2)
        w = pack[:, :width]
        bias = pack[:, width].astype(F32)
        q = (nn(attn_input, w[0]) + bias[0]).astype(BF)
        ko = nn(attn_input, w[1]).astype(BF)
        vo = (nn(attn_input, w[2]) + bias[2]).astype(BF)
        kp = nn(prompt_input, w[1]).astype(BF)
        vp = (nn(prompt_input, w[2]) + bias[2]).astype(BF)
        ctx, lse = attn_fwd(lens, q, kp, vp, ko, vo)
        units.append((w, q, kp, vp, ko, vo, ctx, lse))

    proj_units = [jnp.concatenate(proj_pieces[2 * u : 2 * u + 2], axis=0) for u in range(2)]
    attn_out = nn(units[0][6], proj_units[0]) + nn(units[1][6], proj_units[1]) + b_proj.astype(F32)
    hidden = rows_in + attn_out
    normal2, scale2 = normalize(hidden)
    mlp_input = (normal2 * g2 + c2).astype(BF)

    branch = 0.0
    grad_mlp_in = 0.0
    grad_in_pieces, grad_out_pieces, grad_b_in_pieces = [], [], []
    for r in range(PIECES):
        w1 = in_pieces[r][:width]
        pre = nn(mlp_input, w1) + in_pieces[r][width].astype(F32)
        cdf = 0.5 * (1.0 + lax.erf(pre * (0.5**0.5)))
        pdf = jnp.exp(-0.5 * pre * pre) * 0.3989422804014327
        gelu = (pre * cdf).astype(BF)
        branch = branch + nn(gelu, out_pieces[r])
        grad_pre = (nt(out_grad, out_pieces[r]) * (cdf + pre * pdf)).astype(BF)
        grad_out_pieces.append(tn(gelu, out_grad))
        grad_in_pieces.append(tn(mlp_input, grad_pre))
        grad_b_in_pieces.append(jnp.sum(grad_pre.astype(F32), axis=0))
        grad_mlp_in = grad_mlp_in + nt(grad_pre, w1)
    layer_out = (hidden + (branch + b_out.astype(F32))).astype(BF)

    grad_w_out = dp_sum(tensor_sum(grad_out_pieces))
    grad_w_in = dp_sum(tensor_sum(grad_in_pieces))

    back2, sum_g2, sum_c2 = norm_back(grad_mlp_in, normal2, scale2, g2)
    dy = out_grad.astype(F32)
    grad_hidden = dy + back2
    grad_attn = grad_hidden.astype(BF)
    sum_b_proj = jnp.sum(grad_attn.astype(F32), axis=0)
    sum_b_out = jnp.sum(dy, axis=0)

    grad_own_in = 0.0
    grad_prompt_in = 0.0
    grad_qkv_pieces, grad_proj_pieces, sum_qv_pieces = [None] * 4, [None] * 4, [None] * 4
    both_input = jnp.concatenate([attn_input, prompt_input], axis=0)
    for u in (1, 0):
        w, q, kp, vp, ko, vo, ctx, lse = units[u]
        grad_proj = tn(ctx, grad_attn)
        grad_ctx = nt(grad_attn, proj_units[u]).astype(BF)
        dq, dkp, dvp, dko, dvo = attn_bwd(lens, q, kp, vp, ko, vo, grad_ctx, ctx, lse)
        grad_own_in = grad_own_in + nt(dq, w[0]) + nt(dko, w[1]) + nt(dvo, w[2])
        grad_prompt_in = grad_prompt_in + nt(dkp, w[1]) + nt(dvp, w[2])
        gq = tn(attn_input, dq)
        gk = tn(both_input, jnp.concatenate([dko, dkp], axis=0))
        gv = tn(both_input, jnp.concatenate([dvo, dvp], axis=0))
        sum_q = jnp.sum(dq.astype(F32), axis=0)
        sum_v = jnp.sum(dvo.astype(F32), axis=0) + jnp.sum(dvp.astype(F32), axis=0)
        part_width = gq.shape[1] // 2
        for k in range(2):
            cols = slice(k * part_width, (k + 1) * part_width)
            grad_qkv_pieces[2 * u + k] = jnp.concatenate([gq[:, cols], gk[:, cols], gv[:, cols]], axis=0)
            grad_proj_pieces[2 * u + k] = grad_proj[cols]
            sum_qv_pieces[2 * u + k] = jnp.concatenate([sum_q[cols], sum_v[cols]])
    grad_w_proj = dp_sum(tensor_sum(grad_proj_pieces))
    grad_w_qkv = dp_sum(tensor_sum(grad_qkv_pieces)).reshape((3, width, -1))

    share = grad_prompt_in.astype(BF)
    low, high = share[:half_prompt], share[half_prompt:]
    mine = jnp.where(odd, high, low).astype(F32) + swap(jnp.where(odd, low, high), "tensor", 1).astype(F32)
    mine = mine + lax.ppermute(mine.astype(BF), "tensor", [(2, 0), (3, 1)]).astype(F32)
    spare = rows - half_prompt
    tail = lax.ppermute(mine[:spare].astype(BF), "tensor", [(1, 0)]).astype(F32)
    first_rows = jnp.concatenate([mine, tail], axis=0)
    next_rows = jnp.concatenate([mine[spare:], jnp.zeros((rows - half_prompt + spare, width), F32)], axis=0)
    extra = jnp.where(t == 0, first_rows, jnp.where(t == 1, next_rows, 0.0))
    back1, sum_g1, sum_c1 = norm_back(grad_own_in + extra, normal1, scale1, g1)
    in_grad = grad_hidden + back1

    def ordered(pieces):
        pieces = [jnp.where(odd, pieces[r ^ 1], pieces[r]) for r in range(PIECES)]
        return [jnp.where(t >= 2, pieces[r ^ 2], pieces[r]) for r in range(PIECES)]

    small = jnp.concatenate(
        [sum_b_proj, sum_g1, sum_c1, sum_g2, sum_c2, sum_b_out] + ordered(grad_b_in_pieces) + ordered(sum_qv_pieces)
    )
    small = lax.psum(small, ("dp", "tensor"))
    sums = [small[k * width : (k + 1) * width] for k in range(6)]
    at = 6 * width
    hid = w_in.shape[1]
    grad_b_in = lax.dynamic_slice(small, (at + t * hid,), (hid,))
    qv = 2 * w_qkv.shape[2]
    grad_b_qv = lax.dynamic_slice(small, (at + PIECES * hid + t * qv,), (qv,)).reshape(2, qv // 2)
    return (layer_out, in_grad, grad_w_qkv, grad_b_qv, grad_w_proj, sums[0], sums[1], sums[2], sums[3],
            sums[4], grad_w_in, grad_b_in, grad_w_out, sums[5])


def solution(mesh):
    in_specs = (
        P(("dp", "tensor"), None),
        P("dp"),
        P("dp", None),
        P(None, None, "tensor"),
        P(None, "tensor"),
        P("tensor", None),
        P(),
        P(),
        P(),
        P(),
        P(),
        P(None, "tensor"),
        P("tensor"),
        P("tensor", None),
        P(),
        P(("dp", "tensor"), None),
    )
    out_specs = (
        P(("dp", "tensor"), None),
        P(("dp", "tensor"), None),
        P(None, None, "tensor"),
        P(None, "tensor"),
        P("tensor", None),
        P(),
        P(),
        P(),
        P(),
        P(),
        P(None, "tensor"),
        P("tensor"),
        P("tensor", None),
        P(),
    )
    return jax.shard_map(shards, mesh=mesh, in_specs=in_specs, out_specs=out_specs, check_vma=False)
```

```python
import functools

import jax
import jax.numpy as jnp
from jax import lax
from jax.experimental import pallas as pl
from jax.experimental.pallas import tpu as pltpu
from jax.sharding import PartitionSpec as P

HEAD = 64
PROMPT = 1024
CONT = 8
CLEN = 256
PIECES = 4
MESH = pl.DeviceIdType.MESH
ANY = pl.BlockSpec(memory_space=pl.ANY)

EPS = 1e-06
MASKED = -1000000000.0
BF = jnp.bfloat16
F32 = jnp.float32


def nt(a, b):
    return lax.dot_general(a, b, (((1,), (1,)), ((), ())), preferred_element_type=F32)


def nn(a, b):
    return lax.dot_general(a, b, (((1,), (0,)), ((), ())), preferred_element_type=F32)


def tn(a, b):
    return lax.dot_general(a, b, (((0,), (0,)), ((), ())), preferred_element_type=F32)


class Peers:
    def __init__(self):
        self.t = lax.axis_index("tensor")
        self.d = lax.axis_index("dp")
        self.odd = lax.rem(self.t, 2)
        self.p = lax.rem(self.d, 2)
        self.z = lax.div(self.d, 2)
        self.core = {"tensor": self.t + 1 - 2 * self.odd}
        self.x = {"tensor": lax.rem(self.t + 2, 4)}
        self.y = {"dp": self.d + 1 - 2 * self.p}

    def along(self, k, count):
        return {"dp": lax.rem(self.z + k, count) * 2 + self.p}


def enter(devices):
    barrier = pltpu.get_barrier_semaphore()
    for device in devices:
        pl.semaphore_signal(barrier, inc=1, device_id=device, device_id_type=MESH)
    pl.semaphore_wait(barrier, len(devices))


def remote(src, dst, send, recv, device):
    return pltpu.make_async_remote_copy(
        src_ref=src, dst_ref=dst, send_sem=send, recv_sem=recv, device_id=device, device_id_type=MESH
    )


def split_rows(rows, parts, most):
    best = None
    for count in range(most, 0, -1):
        step = count * parts * 8
        padded = -(-rows // step) * step
        if best is None or padded < best[0]:
            best = (padded, count)
    padded, count = best
    return count, padded // count // parts


def part_of(parts):
    return [2 * (k % (parts // 2)) + k // (parts // 2) for k in range(parts)]


STAGES = 7


def sum_scratch(chunks, parts, rows, width):
    half = parts // 2

    def buf(n, dtype=BF):
        return pltpu.VMEM((chunks, n, rows, width), dtype)

    def dma(n):
        return pltpu.SemaphoreType.DMA((chunks, n))

    return [
        buf(parts), buf(parts), buf(parts), buf(parts), buf(parts),
        buf(half, F32), buf(half), buf(half), buf(half), buf(half), buf(parts),
        dma(2), dma(2), dma(2), dma(2), dma(2), dma(half), dma(half), dma(half), dma(half), dma(2),
    ]


def sum_stages(me, half, g, scratch):
    (g0, g2, r1, r3, xr, keep, ysend, yr, zsend, zr, fin,
     local, core_s, core_r, xs, ys, zs, zrs, fs, frs, gs) = scratch

    def from_core(c, i):
        return remote(g.at[1 + 2 * i, c], (r1, r3)[i].at[c], core_s.at[c, i], core_r.at[c, i], me.core)

    def own(c, i):
        return pltpu.make_async_copy(g.at[2 * i, c], (g0, g2)[i].at[c], local.at[c, i])

    def across(c):
        return remote(g2.at[c], xr.at[c], xs.at[c, 0], xs.at[c, 1], me.x)

    def pair(c):
        return remote(ysend.at[c], yr.at[c], ys.at[c, 0], ys.at[c, 1], me.y)

    def rest(c, k):
        return remote(zsend.at[c, lax.rem(me.z + k, half)], zr.at[c, k], zs.at[c, k], zrs.at[c, k], me.along(k, half))

    def back(c, k):
        spot = fin.at[c, me.p * half + me.z]
        return remote(spot, spot, fs.at[c, k], frs.at[c, k], me.along(k, half))

    def back_pair(c):
        spot = fin.at[c, pl.ds(me.p * half, half)]
        return remote(spot, spot, gs.at[c, 0], gs.at[c, 1], me.y)

    def start(c):
        for i in (1, 0):
            from_core(c, i).start()
            own(c, i).start()

    def to_chip(c):
        from_core(c, 1).wait()
        own(c, 1).wait()
        g2[c] = (g2[c].astype(F32) + r3[c].astype(F32)).astype(BF)
        across(c).start()

    def to_pair(c):
        from_core(c, 0).wait()
        own(c, 0).wait()
        across(c).wait()

        def total(first):
            s = pl.ds(first, half)
            return g0[c, s].astype(F32) + r1[c, s].astype(F32) + xr[c, s].astype(F32)

        ysend[c] = total((1 - me.p) * half).astype(BF)
        pair(c).start()
        keep[c] = total(me.p * half)

    def to_rest(c):
        pair(c).wait()
        total = keep[c] + yr[c].astype(F32)
        keep[c] = total
        zsend[c] = total.astype(BF)
        for k in range(1, half):
            rest(c, k).start()

    def to_back(c):
        total = keep[c, me.z]
        for k in range(1, half):
            rest(c, k).wait()
            total = total + zr[c, k].astype(F32)
        fin[c, me.p * half + me.z] = total.astype(BF)
        for k in range(1, half):
            back(c, k).start()

    def to_back_pair(c):
        for k in range(1, half):
            back(c, k).wait()
        back_pair(c).start()

    def finish(c):
        back_pair(c).wait()

    return [start, to_chip, to_pair, to_rest, to_back, to_back_pair, finish]


def sum_peers(me, half):
    return [me.core, me.x, me.y] + [me.along(k, half) for k in range(1, half)]


def progress(stages, chunks, plan, slot):
    for s in range(STAGES - 1, 0, -1):
        first, step = plan[s]
        since = slot - first
        c = lax.div(since, step)

        @pl.when(jnp.logical_and(jnp.logical_and(since >= 0, lax.rem(since, step) == 0), c < chunks))
        def _():
            stages[s](c)


def plan_end(chunks, plan):
    return max(plan[s][0] + plan[s][1] * (chunks - 1) for s in range(1, STAGES)) + 1


def own_lanes(rows, h):
    lane = lax.broadcasted_iota(jnp.int32, (rows, 128), 1)
    return ((lane < 64) if h == 0 else (lane >= 64)), lane - (64 if h == 0 else 0)


def key_aug(k, h, length, base):
    rows = k.shape[0]
    own, extra = own_lanes(rows, h)
    row = lax.broadcasted_iota(jnp.int32, (rows, 128), 0) + base
    bias = jnp.where(jnp.logical_and(extra == 0, row >= length), MASKED, 0.0)
    return jnp.where(own, k.astype(F32), bias).astype(BF)


def query_aug(q, h):
    own, extra = own_lanes(q.shape[0], h)
    return jnp.where(own, q.astype(F32) * 0.125, jnp.where(extra == 0, 1.0, 0.0)).astype(BF)


def value_aug(v, h):
    own, extra = own_lanes(v.shape[0], h)
    ones = jnp.where(jnp.logical_and(extra >= 0, extra < 3), 1.0, 0.0)
    return jnp.where(own, v.astype(F32), ones).astype(BF)


def transposed(v):
    return v.astype(F32).T


def attn_specs(rows, prompt, blocks):
    def col(n):
        return pl.BlockSpec((n, 128), lambda i, l: (0, i))

    logs = pl.BlockSpec((1, blocks, 8, CLEN), lambda i, l: (i, 0, 0, 0))
    return col(rows), col(prompt), logs


class Weight:
    def __init__(self, me, own, spots, view, sems):
        self.me, self.own, self.spots, self.view = me, own, spots, view
        self.send, self.recv = sems

    def side(self):
        return remote(self.own, self.spots(1), self.send.at[0], self.recv.at[0], self.me.core)

    def across(self):
        p = self.me.p
        return remote(self.view(None, p), self.view(2, p), self.send.at[1], self.recv.at[1], self.me.x)

    def pair(self):
        p = self.me.p
        return remote(self.view(2, p), self.view(2, p), self.send.at[2], self.recv.at[2], self.me.y)

    def over(self, which):
        h = self.me.p if which == 0 else 1 - self.me.p
        return remote(self.view(2, h), self.view(3, h), self.send.at[3 + which], self.recv.at[3 + which], self.me.core)

    def start(self):
        self.side().start()
        self.across().start()

    def relay(self):
        self.across().wait_recv()
        self.pair().start()
        self.over(0).start()

    def relay_pair(self):
        self.pair().wait_recv()
        self.over(1).start()

    def finish(self):
        self.side().wait()
        self.across().wait_send()
        self.pair().wait_send()
        self.over(0).wait()
        self.over(1).wait()


def norm_rows(x, gain, shift):
    x = x.astype(F32)
    centred = x - jnp.mean(x, axis=-1, keepdims=True)
    scale = lax.rsqrt(jnp.mean(centred * centred, axis=-1, keepdims=True) + EPS)
    return (centred * scale * gain + shift).astype(BF)


def front_kernel(lens, x_ref, gain_ref, shift_ref, wq, wp, wi, wo, ws,
                 q_ref, kp_ref, vp_ref, ko_ref, vo_ref, ctx_ref, lse_ref, an_ref, anp_ref,
                 wq_all, wp_all, wi_all, wo_all, ws_all,
                 px, wv, wsv, kph, vpt, px_s, px_r, send, recv, loc):
    me = Peers()
    step = pl.program_id(0)
    rows = x_ref.shape[0]
    blocks = rows // CLEN
    prompt = px.shape[0]
    part = wq.shape[1]
    own_chunks = rows // CLEN
    chunks = prompt // CLEN

    def qkv_view(r, h):
        n = part // 2
        if r is None:
            return wq.at[:, pl.ds(h * n, n)]
        return wv.at[:, pl.ds(r * part + h * n, n)]

    def plain(own, everything):
        n = own.shape[0] // 2

        def view(r, h):
            return own.at[pl.ds(h * n, n)] if r is None else everything.at[r, pl.ds(h * n, n)]

        return view

    def weight(i, own, everything):
        return Weight(me, own, lambda r: everything.at[r], plain(own, everything), (send.at[i], recv.at[i]))

    w_qkv = Weight(me, wq, lambda r: wv.at[:, pl.ds(r * part, part)], qkv_view, (send.at[0], recv.at[0]))
    w_small = weight(1, ws, wsv)
    w_proj = weight(2, wp, wp_all)
    w_in = weight(3, wi, wi_all)
    w_out = weight(4, wo, wo_all)
    later = [w_proj, w_in, w_out]

    def keep(own, spot, i):
        return pltpu.make_async_copy(own, spot, loc.at[i])

    mine = [
        keep(wq, wv.at[:, pl.ds(0, part)], 0), keep(ws, wsv.at[0], 1), keep(wp, wp_all.at[0], 2),
        keep(wi, wi_all.at[0], 3), keep(wo, wo_all.at[0], 4), keep(wv, wq_all, 5), keep(wsv, ws_all, 6),
    ]

    def chunk(k):
        return px.at[pl.ds(k * CLEN, CLEN)]

    def held(k):
        at = k if k < own_chunks else k - own_chunks
        return x_ref.at[pl.ds(at * CLEN, CLEN)]

    def hop(k, src, n, device):
        return remote(src, chunk(k), px_s.at[n, k], px_r.at[n, k], device)

    first = [k for k in range(chunks) if k < own_chunks]
    second = [k for k in range(chunks) if k >= own_chunks]
    low = [k for k in range(chunks) if k < chunks // 2]
    high = second + [k for k in range(chunks // 2, own_chunks)]

    def normed(k):
        anp_ref[k * CLEN : (k + 1) * CLEN, :] = norm_rows(px[k * CLEN : (k + 1) * CLEN, :], gain_ref[...], shift_ref[...])

    @pl.when(step == 0)
    def _():
        enter([me.core, me.x, me.y])

        @pl.when(me.t == 0)
        def _():
            for k in low:
                hop(k, held(k), 1, me.x).start()
            for k in reversed(first):
                hop(k, held(k), 0, me.core).start()

        @pl.when(me.t == 1)
        def _():
            for k in second:
                hop(k, held(k), 1, me.x).start()
                hop(k, held(k), 0, me.core).start()

        for w in (w_qkv, w_small):
            w.side().start()
        for i in range(5):
            mine[i].start()

        @pl.when(me.t == 1)
        def _():
            for k in reversed(first):
                hop(k, held(k), 0, me.core).wait_recv()
                if k in high:
                    hop(k, chunk(k), 1, me.x).start()

        for w in (w_qkv, w_small):
            w.across().start()
        for w in later:
            w.side().start()
        for b in range(blocks):
            an_ref[b * CLEN : (b + 1) * CLEN, :] = norm_rows(x_ref[b * CLEN : (b + 1) * CLEN, :], gain_ref[...], shift_ref[...])

        @pl.when(me.t == 0)
        def _():
            for k in first:
                px[k * CLEN : (k + 1) * CLEN, :] = x_ref[k * CLEN : (k + 1) * CLEN, :]
            for k in second:
                hop(k, held(k), 0, me.core).wait_recv()
            for k in first:
                hop(k, held(k), 0, me.core).wait_send()
            for k in low:
                hop(k, held(k), 1, me.x).wait_send()

        @pl.when(me.t == 1)
        def _():
            for k in second:
                px[k * CLEN : (k + 1) * CLEN, :] = held(k)[...]
                hop(k, held(k), 0, me.core).wait_send()
            for k in high:
                hop(k, chunk(k), 1, me.x).wait_send()

        @pl.when(me.t == 2)
        def _():
            for k in low:
                hop(k, chunk(k), 1, me.x).wait_recv()
                hop(k, chunk(k), 0, me.core).start()
            for k in high:
                hop(k, chunk(k), 0, me.core).wait_recv()
            for k in low:
                hop(k, chunk(k), 0, me.core).wait_send()

        @pl.when(me.t == 3)
        def _():
            for k in high:
                hop(k, chunk(k), 1, me.x).wait_recv()
                hop(k, chunk(k), 0, me.core).start()
            for k in low:
                hop(k, chunk(k), 0, me.core).wait_recv()
            for k in high:
                hop(k, chunk(k), 0, me.core).wait_send()

        for k in range(chunks):
            normed(k)
        w_small.relay()
        for w in (w_qkv, w_small):
            w.side().wait_recv()
        for i in range(2):
            mine[i].wait()

    @pl.when(step == 3)
    def _():
        for w in (w_qkv, w_small):
            w.over(0).wait_recv()
            w.over(1).wait_recv()
        mine[5].start()
        mine[6].start()

    def moves(slot):
        def at(k, *steps):
            @pl.when(slot == k)
            def _():
                for s in steps:
                    s()

        at(2, w_qkv.relay, *[lambda w=w: w.across().start() for w in later])
        at(6, w_qkv.relay_pair, w_small.relay_pair)
        at(9, w_proj.relay)
        at(11, w_proj.relay_pair)
        at(13, w_in.relay)
        at(16, w_in.relay_pair)

    pick = pl.ds(pl.multiple_of(step * 128, 128), 128)
    w3 = jnp.concatenate([wv[0, pick], wv[1, pick], wv[2, pick]], axis=0)
    u = 2 * lax.div(step, 3)
    left = wsv[u, :16, pick].astype(F32)
    right = wsv[u + 1, :16, pick].astype(F32)
    spot = lax.broadcasted_iota(jnp.int32, left.shape, 0)

    def bias(k):
        return jnp.sum(jnp.where(spot == u + k, left, 0.0) + jnp.where(spot == u + 1 + k, right, 0.0), axis=0, keepdims=True)

    bq = bias(0)
    bv = bias(PIECES)
    for b in range(blocks):
        at = slice(b * CLEN, (b + 1) * CLEN)
        got = nt(an_ref[at, :], w3)
        q_ref[at, :] = (got[:, :128] + bq).astype(BF)
        ko_ref[at, :] = got[:, 128:256].astype(BF)
        vo_ref[at, :] = (got[:, 256:] + bv).astype(BF)
    for c in range(chunks):
        at = slice(c * CLEN, (c + 1) * CLEN)
        got = nt(anp_ref[at, :], w3[128:])
        kp_ref[at, :] = got[:, :128].astype(BF)
        vp_ref[at, :] = (got[:, 128:] + bv).astype(BF)

    vt = transposed(vp_ref[...])
    for h in range(2):
        kph[h] = key_aug(kp_ref[...], h, lens[0], 0)
        vpt[h] = jnp.concatenate([vt[64 * h : 64 * h + 64].astype(BF), jnp.ones((16, prompt), BF)], axis=0)

    def block(b, _):
        moves(step * blocks + b)
        at = pl.ds(pl.multiple_of(b * CLEN, CLEN), CLEN)
        q = q_ref[at, :]
        ko = ko_ref[at, :]
        vot = transposed(vo_ref[at, :])
        outs, logs = [], []
        for h in range(2):
            qh = query_aug(q, h)
            vh = jnp.concatenate([vot[64 * h : 64 * h + 64].astype(BF), jnp.ones((16, CLEN), BF)], axis=0)
            sp = nt(kph[h], qh)
            so = nt(key_aug(ko, h, lens[1 + b], 0), qh)
            top = jnp.maximum(jnp.max(sp, axis=0, keepdims=True), jnp.max(so, axis=0, keepdims=True))
            pp = jnp.exp(sp - top).astype(BF)
            po = jnp.exp(so - top).astype(BF)
            ot = nn(vpt[h], pp) + nn(vh, po)
            total = ot[64:65]
            outs.append(ot[:64] * (1.0 / total))
            logs.append(top + jnp.log(total))
        ctx_ref[at, :] = jnp.concatenate(outs, axis=0).T.astype(BF)
        lse_ref[0, b] = jnp.concatenate(logs + [jnp.zeros((6, CLEN), F32)], axis=0)
        return 0

    lax.fori_loop(0, blocks, block, 0)

    @pl.when(step == pl.num_programs(0) - 1)
    def _():
        w_out.relay()
        w_out.relay_pair()
        for w in [w_qkv, w_small]:
            w.side().wait_send()
            w.across().wait_send()
            w.pair().wait_send()
            w.over(0).wait_send()
            w.over(1).wait_send()
        for w in later:
            w.finish()
        for i in range(2, 7):
            mine[i].wait()


def front_call(lens, x, gain, shift, wq, wp, wi, wo, ws):
    rows, width = x.shape
    blocks = rows // CLEN
    pairs = width // 128
    r, p, logs = attn_specs(rows, PROMPT, blocks)
    cells = rows * (PROMPT + CLEN) * pairs * 2

    def whole(n):
        return pl.BlockSpec((n, width), lambda i, l: (0, 0))

    def shape(*s):
        return jax.ShapeDtypeStruct(s, BF)

    part = wq.shape[1]
    return pl.pallas_call(
        front_kernel,
        out_shape=(
            shape(rows, width), shape(PROMPT, width), shape(PROMPT, width), shape(rows, width), shape(rows, width),
            shape(rows, width), jax.ShapeDtypeStruct((pairs, blocks, 8, CLEN), F32),
            shape(rows, width), shape(PROMPT, width),
            shape(3, PIECES * part, width), shape(PIECES, *wp.shape), shape(PIECES, *wi.shape),
            shape(PIECES, *wo.shape), shape(PIECES, *ws.shape),
        ),
        grid_spec=pltpu.PrefetchScalarGridSpec(
            num_scalar_prefetch=1,
            grid=(pairs,),
            in_specs=[whole(rows), whole(1), whole(1), ANY, ANY, ANY, ANY, ANY],
            out_specs=[r, p, p, r, r, r, logs, whole(rows), whole(PROMPT), ANY, ANY, ANY, ANY, ANY],
            scratch_shapes=[
                pltpu.VMEM((PROMPT, width), BF),
                pltpu.VMEM((3, PIECES * part, width), BF),
                pltpu.VMEM((PIECES,) + ws.shape, BF),
                pltpu.VMEM((2, PROMPT, 128), BF),
                pltpu.VMEM((2, 80, PROMPT), BF),
                pltpu.SemaphoreType.DMA((2, PROMPT // CLEN)),
                pltpu.SemaphoreType.DMA((2, PROMPT // CLEN)),
                pltpu.SemaphoreType.DMA((5, 5)),
                pltpu.SemaphoreType.DMA((5, 5)),
                pltpu.SemaphoreType.DMA((7,)),
            ],
        ),
        compiler_params=pltpu.CompilerParams(collective_id=0, has_side_effects=True, vmem_limit_bytes=48 << 20),
        cost_estimate=pl.CostEstimate(flops=cells * 256 * 4, transcendentals=cells, bytes_accessed=4 << 20),
        name="front",
    )(lens, x, gain, shift, wq, wp, wi, wo, ws)


BACK_PLAN = {1: (1, 1), 2: (5, 3), 3: (7, 3), 4: (9, 3), 5: (11, 3), 6: (13, 3)}


def attn_bwd_kernel(chunks_g, half, lens, q_ref, kp_ref, vp_ref, ko_ref, vo_ref, do_ref, ctx_ref, lse_ref, g,
                    dq_ref, dkp_ref, dvp_ref, dko_ref, dvo_ref, g_out, qh_s, doh_s, dqt, out_sem, *scratch):
    me = Peers()
    step = pl.program_id(0)
    stages = sum_stages(me, half, g, scratch)

    @pl.when(step == 0)
    def _():
        enter(sum_peers(me, half))
        for c in range(chunks_g):
            stages[0](c)

    rows_all = q_ref.shape[0]
    blocks = rows_all // CLEN
    chunks = kp_ref.shape[0] // CLEN
    prod = do_ref[...].astype(F32) * ctx_ref[...].astype(F32)
    for h in range(2):
        own, extra = own_lanes(rows_all, h)
        qh_s[h] = query_aug(q_ref[...], h)
        d = -jnp.sum(jnp.where(own, prod, 0.0), axis=1, keepdims=True)
        hi = d.astype(BF).astype(F32)
        mid = (d - hi).astype(BF).astype(F32)
        low = d - hi - mid
        aug = jnp.where(extra == 0, hi, jnp.where(extra == 1, mid, jnp.where(extra == 2, low, 0.0)))
        doh_s[h] = jnp.where(own, do_ref[...].astype(F32), aug).astype(BF)
    first = lax.broadcasted_iota(jnp.int32, (CLEN, 128), 1) < 64

    def own_block(b, _):
        rows = pl.ds(pl.multiple_of(b * CLEN, CLEN), CLEN)
        q = q_ref[rows, :]
        k = ko_ref[rows, :]
        v = vo_ref[rows, :]
        do = do_ref[rows, :]
        kt = transposed(k).astype(BF)
        dks, dvs, dqs = [], [], []
        for h in range(2):
            s = nt(key_aug(k, h, lens[1 + b], 0), qh_s[h, rows, :])
            p = jnp.exp(s - lse_ref[0, b, h : h + 1, :])
            dp = nt(value_aug(v, h), doh_s[h, rows, :])
            ds = (p * dp).astype(BF)
            dvs.append(nn(p.astype(BF), do))
            dks.append(nn(ds, q))
            dqs.append(nn(kt[64 * h : 64 * h + 64], ds))
        dvo_ref[rows, :] = jnp.where(first, dvs[0], dvs[1]).astype(BF)
        dko_ref[rows, :] = (jnp.where(first, dks[0], dks[1]) * 0.125).astype(BF)
        dqt[b] = jnp.concatenate(dqs, axis=0)
        return 0

    lax.fori_loop(0, blocks, own_block, 0)

    def chunk(c, _):
        progress(stages, chunks_g, BACK_PLAN, step * chunks + c)
        rows = pl.ds(pl.multiple_of(c * CLEN, CLEN), CLEN)
        k = kp_ref[rows, :]
        v = vp_ref[rows, :]
        kt = transposed(k).astype(BF)
        dks, dvs = [], []
        for h in range(2):
            kh = key_aug(k, h, lens[0], c * CLEN)
            vh = value_aug(v, h)
            dk = dv = None
            for b in range(blocks):
                rb = pl.ds(b * CLEN, CLEN)
                s = nt(kh, qh_s[h, rb, :])
                p = jnp.exp(s - lse_ref[0, b, h : h + 1, :])
                dp = nt(vh, doh_s[h, rb, :])
                ds = (p * dp).astype(BF)
                dv_b = nn(p.astype(BF), do_ref[rb, :])
                dk_b = nn(ds, q_ref[rb, :])
                dv = dv_b if b == 0 else dv + dv_b
                dk = dk_b if b == 0 else dk + dk_b
                dqt[b, 64 * h : 64 * h + 64] += nn(kt[64 * h : 64 * h + 64], ds)
            dvs.append(dv)
            dks.append(dk)
        dvp_ref[rows, :] = jnp.where(first, dvs[0], dvs[1]).astype(BF)
        dkp_ref[rows, :] = (jnp.where(first, dks[0], dks[1]) * 0.125).astype(BF)
        return 0

    lax.fori_loop(0, chunks, chunk, 0)
    for b in range(blocks):
        dq_ref[b * CLEN : (b + 1) * CLEN, :] = (dqt[b].T * 0.125).astype(BF)

    @pl.when(step == pl.num_programs(0) - 1)
    def _():
        def more(slot, _):
            progress(stages, chunks_g, BACK_PLAN, slot)
            return 0

        lax.fori_loop(chunks * pl.num_programs(0), plan_end(chunks_g, BACK_PLAN), more, 0)
        done = pltpu.make_async_copy(scratch[10], g_out, out_sem)
        done.start()
        done.wait()


def attn_bwd(lens, q, kp, vp, ko, vo, do, ctx, lse, g):
    rows, width = q.shape
    prompt = kp.shape[0]
    blocks = rows // CLEN
    pairs = width // 128
    r, p, logs = attn_specs(rows, prompt, blocks)
    cells = rows * (prompt + CLEN) * pairs * 2
    _, count, parts, part_rows, _ = g.shape

    def shape(n):
        return jax.ShapeDtypeStruct((n, width), BF)

    return pl.pallas_call(
        functools.partial(attn_bwd_kernel, count, parts // 2),
        out_shape=(shape(rows), shape(prompt), shape(prompt), shape(rows), shape(rows),
                   jax.ShapeDtypeStruct(g.shape[1:], BF)),
        grid_spec=pltpu.PrefetchScalarGridSpec(
            num_scalar_prefetch=1,
            grid=(pairs,),
            in_specs=[r, p, p, r, r, r, r, logs, ANY],
            out_specs=[r, p, p, r, r, ANY],
            scratch_shapes=[
                pltpu.VMEM((2, rows, 128), BF),
                pltpu.VMEM((2, rows, 128), BF),
                pltpu.VMEM((blocks, 128, CLEN), F32),
                pltpu.SemaphoreType.DMA,
            ] + sum_scratch(count, parts, part_rows, width),
        ),
        compiler_params=pltpu.CompilerParams(collective_id=1, has_side_effects=True, vmem_limit_bytes=60 << 20),
        cost_estimate=pl.CostEstimate(
            flops=cells * 256 * 10, transcendentals=cells, bytes_accessed=2 * width * (8 * rows + 4 * prompt)
        ),
        name="attn_bwd",
    )(lens, q, kp, vp, ko, vo, do, ctx, lse, g)


def last_kernel(chunks_g, half, g, share, g_out, ex_out, mine, came, total, over, ex, ps, pr, loc, *scratch):
    me = Peers()
    stages = sum_stages(me, half, g, scratch)
    n = mine.shape[0]
    rows = ex.shape[0]
    spare = rows - n
    first = me.t < 2

    enter(sum_peers(me, half))
    side = remote(share.at[pl.ds((1 - me.odd) * n, n)], came, ps.at[0], pr.at[0], me.core)
    own = pltpu.make_async_copy(share.at[pl.ds(me.odd * n, n)], mine, loc.at[0])
    across = remote(total, over, ps.at[1], pr.at[1], me.x)
    end = remote(total.at[pl.ds(0, spare)], ex.at[pl.ds(n, spare)], ps.at[2], pr.at[2], me.core)
    own.start()
    side.start()
    for c in range(chunks_g):
        stages[0](c)
    own.wait()
    side.wait()
    total[...] = (mine[...].astype(F32) + came[...].astype(F32)).astype(BF)

    @pl.when(me.t >= 2)
    def _():
        across.start()
        ex[...] = jnp.zeros_like(ex)

    def run(lo, hi):
        def more(slot, _):
            progress(stages, chunks_g, LAST_PLAN, slot)
            return 0

        lax.fori_loop(lo, hi, more, 0)

    cut = chunks_g + 1
    run(0, cut)

    @pl.when(first)
    def _():
        across.wait_recv()
        total[...] = (total[...].astype(F32) + over[...].astype(F32)).astype(BF)

        @pl.when(me.t == 1)
        def _():
            end.start()
            ex[: n - spare] = total[spare:]
            ex[n - spare :] = jnp.zeros((rows - n + spare, ex.shape[1]), BF)

        @pl.when(me.t == 0)
        def _():
            ex[:n] = total[...]

    run(cut, plan_end(chunks_g, LAST_PLAN))

    @pl.when(me.t >= 2)
    def _():
        across.wait_send()

    @pl.when(me.t == 1)
    def _():
        end.wait_send()

    @pl.when(me.t == 0)
    def _():
        end.wait_recv()

    outs = [pltpu.make_async_copy(scratch[10], g_out, loc.at[1]), pltpu.make_async_copy(ex, ex_out, loc.at[2])]
    for o in outs:
        o.start()
    for o in outs:
        o.wait()


LAST_PLAN = {1: (0, 1), 2: (1, 1), 3: (2, 1), 4: (3, 1), 5: (4, 1), 6: (5, 1)}


def last_call(g, share, rows):
    _, count, parts, part_rows, width = g.shape
    n = share.shape[0] // 2
    return pl.pallas_call(
        functools.partial(last_kernel, count, parts // 2),
        out_shape=(jax.ShapeDtypeStruct(g.shape[1:], BF), jax.ShapeDtypeStruct((rows, width), BF)),
        in_specs=[ANY, ANY],
        out_specs=[ANY, ANY],
        scratch_shapes=[
            pltpu.VMEM((n, width), BF),
            pltpu.VMEM((n, width), BF),
            pltpu.VMEM((n, width), BF),
            pltpu.VMEM((n, width), BF),
            pltpu.VMEM((rows, width), BF),
            pltpu.SemaphoreType.DMA((3,)),
            pltpu.SemaphoreType.DMA((3,)),
            pltpu.SemaphoreType.DMA((3,)),
        ] + sum_scratch(count, parts, part_rows, width),
        compiler_params=pltpu.CompilerParams(collective_id=2, has_side_effects=True, vmem_limit_bytes=48 << 20),
        name="last",
    )(g, share)


def normalize(values):
    centred = values - jnp.mean(values, axis=-1, keepdims=True)
    scale = lax.rsqrt(jnp.mean(centred * centred, axis=-1, keepdims=True) + EPS)
    return centred * scale, scale


def norm_back(grad, normal, scale, gain):
    e = grad * gain
    return scale * (e - jnp.mean(e, axis=-1, keepdims=True) - normal * jnp.mean(e * normal, axis=-1, keepdims=True))


def packed(parts, dp, most):
    pieces, width = parts[0].shape[0], parts[0].shape[2]
    rows = sum(p.shape[1] for p in parts)
    count, part_rows = split_rows(rows, dp, most)
    pad = count * dp * part_rows - rows
    parts = [p.astype(BF) for p in parts]
    if pad:
        parts = parts + [jnp.zeros((pieces, pad, width), BF)]
    return jnp.concatenate(parts, axis=1).reshape(pieces, count, dp, part_rows, width)


def small_rows(rows, rows_pad):
    width = rows[0].shape[-1]
    rows = [jnp.broadcast_to(r, (PIECES, width)) for r in rows]
    rows = rows + [jnp.zeros((PIECES, width), F32)] * (rows_pad - len(rows))
    return jnp.stack(rows, axis=1)


def shards(layer_in, prompt_len, cont_len, w_qkv, b_qv, w_proj, b_proj, ln1_gain, ln1_bias,
           ln2_gain, ln2_bias, w_in, b_in, w_out, b_out, out_grad):
    rows, width = layer_in.shape
    blocks = rows // CLEN
    dp = lax.axis_size("dp")
    part = w_qkv.shape[2]
    t = lax.axis_index("tensor")
    g1, c1, g2, c2 = (v.astype(F32)[None] for v in (ln1_gain, ln1_bias, ln2_gain, ln2_bias))

    group = t * blocks + jnp.arange(blocks)
    conts = group - PROMPT // CLEN
    own_len = jnp.where(conts >= 0, cont_len[0][jnp.clip(conts, 0, CONT - 1)], 0)
    lens = jnp.concatenate([prompt_len, own_len]).astype(jnp.int32)

    bias_rows = [jnp.pad(b_qv[i : i + 1], ((0, 0), (r * part, width - (r + 1) * part))) for i in range(2) for r in range(PIECES)]
    small = jnp.concatenate(bias_rows + [jnp.zeros((8, width), BF), b_in[None], jnp.zeros((15, width), BF)], axis=0)
    (q, kp, vp, ko, vo, ctx, lse, attn_input, prompt_input, wq_all, wp_all, wi_all, wo_all, ws_all) = front_call(
        lens, layer_in, g1, c1, w_qkv.transpose(0, 2, 1), w_proj, w_in, w_out, small
    )

    w_proj_all = wp_all.reshape(width, width)
    rows_in = layer_in.astype(F32)
    hidden = rows_in + nn(ctx, w_proj_all) + b_proj.astype(F32)
    normal2, scale2 = normalize(hidden)
    mlp_input = (normal2 * g2 + c2).astype(BF)

    branch = 0.0
    grad_mlp_in = 0.0
    grad_in_pieces, grad_out_pieces, grad_b_in_pieces = [], [], []
    for r in range(PIECES):
        pre = nn(mlp_input, wi_all[r]) + ws_all[r, 16].astype(F32)
        cdf = 0.5 * (1.0 + lax.erf(pre * (0.5**0.5)))
        pdf = jnp.exp(-0.5 * pre * pre) * 0.3989422804014327
        gelu = (pre * cdf).astype(BF)
        branch = branch + nn(gelu, wo_all[r])
        grad_pre = (nt(out_grad, wo_all[r]) * (cdf + pre * pdf)).astype(BF)
        grad_out_pieces.append(tn(gelu, out_grad).astype(BF))
        grad_in_pieces.append(tn(mlp_input, grad_pre).astype(BF))
        grad_b_in_pieces.append(jnp.sum(grad_pre.astype(F32), axis=0))
        grad_mlp_in = grad_mlp_in + nt(grad_pre, wi_all[r])
    layer_out = (hidden + (branch + b_out.astype(F32))).astype(BF)

    dy = out_grad.astype(F32)
    grad_hidden = dy + norm_back(grad_mlp_in, normal2, scale2, g2)
    grad_attn = grad_hidden.astype(BF)
    sums = [
        jnp.stack(grad_b_in_pieces),
        jnp.sum(grad_attn.astype(F32), axis=0),
        jnp.sum(grad_mlp_in * normal2, axis=0),
        jnp.sum(grad_mlp_in, axis=0),
        jnp.sum(dy, axis=0),
    ]
    grad_ctx = nt(grad_attn, w_proj_all).astype(BF)
    grad_proj = tn(ctx, grad_attn).reshape(PIECES, part, width)
    g_first = packed([jnp.stack(grad_in_pieces), jnp.stack(grad_out_pieces), grad_proj, small_rows(sums, 16)], dp, 7)
    dq, dkp, dvp, dko, dvo, first = attn_bwd(lens, q, kp, vp, ko, vo, grad_ctx, ctx, lse, g_first)
    first = first.reshape(-1, width).astype(F32)
    hid = w_in.shape[1]
    grad_w_in, first = first[:width], first[width:]
    grad_w_out, first = first[:hid], first[hid:]
    grad_w_proj, first = first[:part], first[part:]

    grad_own_in = nn(dq, wq_all[0]) + nn(dko, wq_all[1]) + nn(dvo, wq_all[2])
    grad_prompt_in = nn(dkp, wq_all[1]) + nn(dvp, wq_all[2])
    gq = tn(dq, attn_input)
    gk = tn(dko, attn_input) + tn(dkp, prompt_input)
    gv = tn(dvo, attn_input) + tn(dvp, prompt_input)
    sum_q = jnp.sum(dq.astype(F32), axis=0).reshape(PIECES, part)
    sum_v = (jnp.sum(dvo.astype(F32), axis=0) + jnp.sum(dvp.astype(F32), axis=0)).reshape(PIECES, part)
    sum_qv = jnp.pad(jnp.concatenate([sum_q, sum_v], axis=1), ((0, 0), (0, width - 2 * part)))
    normal1, scale1 = normalize(rows_in)
    gain_off = prompt_input.astype(F32) - c1
    sum_g1 = jnp.sum(grad_own_in * normal1, axis=0) + jnp.sum(grad_prompt_in * gain_off, axis=0) / g1[0]
    sum_c1 = jnp.sum(grad_own_in, axis=0) + jnp.sum(grad_prompt_in, axis=0)
    g_last = packed(
        [v.reshape(PIECES, part, width) for v in (gq, gk, gv)] + [small_rows([sum_qv, sum_g1, sum_c1], 16)], dp, 5
    )
    last, extra = last_call(g_last, grad_prompt_in.astype(BF), rows)
    last = last.reshape(-1, width).astype(F32)
    grad_w_qkv = last[: 3 * part].reshape(3, part, width).transpose(0, 2, 1)
    last = last[3 * part :]
    grad_b_qv = last[0, : 2 * part].reshape(2, part)
    in_grad = grad_hidden + norm_back(grad_own_in + extra.astype(F32), normal1, scale1, g1)
    return (layer_out, in_grad, grad_w_qkv, grad_b_qv, grad_w_proj, first[1], last[1], last[2], first[2],
            first[3], grad_w_in, first[0, :hid], grad_w_out, first[4])


def solution(mesh):
    in_specs = (
        P(("dp", "tensor"), None),
        P("dp"),
        P("dp", None),
        P(None, None, "tensor"),
        P(None, "tensor"),
        P("tensor", None),
        P(),
        P(),
        P(),
        P(),
        P(),
        P(None, "tensor"),
        P("tensor"),
        P("tensor", None),
        P(),
        P(("dp", "tensor"), None),
    )
    out_specs = (
        P(("dp", "tensor"), None),
        P(("dp", "tensor"), None),
        P(None, None, "tensor"),
        P(None, "tensor"),
        P("tensor", None),
        P(),
        P(),
        P(),
        P(),
        P(),
        P(None, "tensor"),
        P("tensor"),
        P("tensor", None),
        P(),
    )
    return jax.shard_map(shards, mesh=mesh, in_specs=in_specs, out_specs=out_specs, check_vma=False)
```

```python
import functools

import jax
import jax.numpy as jnp
from jax import lax
from jax.experimental import pallas as pl
from jax.experimental.pallas import tpu as pltpu
from jax.sharding import PartitionSpec as P

HEAD = 64
PROMPT = 1024
CONT = 8
CLEN = 256
PIECES = 4
MESH = pl.DeviceIdType.MESH
ANY = pl.BlockSpec(memory_space=pl.ANY)

EPS = 1e-06
MASKED = -1000000000.0
BF = jnp.bfloat16
F32 = jnp.float32


def nt(a, b):
    return lax.dot_general(a, b, (((1,), (1,)), ((), ())), preferred_element_type=F32)


def nn(a, b):
    return lax.dot_general(a, b, (((1,), (0,)), ((), ())), preferred_element_type=F32)


def tn(a, b):
    return lax.dot_general(a, b, (((0,), (0,)), ((), ())), preferred_element_type=F32)


NEAR = 8


class Peers:
    def __init__(self):
        self.t = lax.axis_index("tensor")
        self.d = lax.axis_index("dp")
        self.odd = lax.rem(self.t, 2)
        self.p = lax.rem(self.d, 2)
        self.z = lax.div(lax.rem(self.d, NEAR), 2)
        self.base = self.d - lax.rem(self.d, NEAR)
        self.core = {"tensor": self.t + 1 - 2 * self.odd}
        self.x = {"tensor": lax.rem(self.t + 2, 4)}
        self.y = {"dp": self.d + 1 - 2 * self.p}

    def along(self, k, count):
        return {"dp": self.base + lax.rem(self.z + k, count) * 2 + self.p}


def enter(devices):
    barrier = pltpu.get_barrier_semaphore()
    for device in devices:
        pl.semaphore_signal(barrier, inc=1, device_id=device, device_id_type=MESH)
    pl.semaphore_wait(barrier, len(devices))


def remote(src, dst, send, recv, device):
    return pltpu.make_async_remote_copy(
        src_ref=src, dst_ref=dst, send_sem=send, recv_sem=recv, device_id=device, device_id_type=MESH
    )


def beyond(value):
    size = lax.axis_size("dp")
    step = NEAR
    while step < size:
        value = value + lax.ppermute(value, "dp", [(i, i ^ step) for i in range(size)])
        step *= 2
    return value


def own_lanes(rows, h):
    lane = lax.broadcasted_iota(jnp.int32, (rows, 128), 1)
    return ((lane < 64) if h == 0 else (lane >= 64)), lane - (64 if h == 0 else 0)


def key_aug(k, h, length, base):
    rows = k.shape[0]
    own, extra = own_lanes(rows, h)
    row = lax.broadcasted_iota(jnp.int32, (rows, 128), 0) + base
    bias = jnp.where(jnp.logical_and(extra == 0, row >= length), MASKED, 0.0)
    return jnp.where(own, k.astype(F32), bias).astype(BF)


def query_aug(q, h):
    own, extra = own_lanes(q.shape[0], h)
    return jnp.where(own, q.astype(F32) * 0.125, jnp.where(extra == 0, 1.0, 0.0)).astype(BF)


def value_aug(v, h):
    own, extra = own_lanes(v.shape[0], h)
    ones = jnp.where(jnp.logical_and(extra >= 0, extra < 3), 1.0, 0.0)
    return jnp.where(own, v.astype(F32), ones).astype(BF)


def transposed(v):
    return v.astype(F32).T


def wide_keys(k, length, base):
    rows = k.shape[0]
    lane = lax.broadcasted_iota(jnp.int32, (rows, 128), 1)
    row = lax.broadcasted_iota(jnp.int32, (rows, 128), 0) + base
    bias = jnp.where(jnp.logical_and(lane == 0, row >= length), MASKED, 0.0).astype(BF)
    return jnp.concatenate([k, bias], axis=1)


def wide_values(v):
    lane = lax.broadcasted_iota(jnp.int32, v.shape, 1)
    return jnp.concatenate([v, jnp.where(lane < 3, 1.0, 0.0).astype(BF)], axis=1)


def wide_queries(q):
    lane = lax.broadcasted_iota(jnp.int32, q.shape, 1)
    qf = q.astype(F32) * 0.125
    one = jnp.where(lane == 0, 1.0, 0.0)
    heads = [jnp.where(lane < 64, qf, 0.0), jnp.where(lane < 64, 0.0, qf)]
    return jnp.concatenate([jnp.concatenate([h, one], axis=1) for h in heads], axis=0).astype(BF)


def wide_grads(do, ctx):
    lane = lax.broadcasted_iota(jnp.int32, do.shape, 1)
    do = do.astype(F32)
    prod = do * ctx.astype(F32)
    out = []
    for h in range(2):
        mine = (lane < 64) if h == 0 else (lane >= 64)
        d = -jnp.sum(jnp.where(mine, prod, 0.0), axis=1, keepdims=True)
        hi = d.astype(BF).astype(F32)
        mid = (d - hi).astype(BF).astype(F32)
        low = d - hi - mid
        aug = jnp.where(lane == 0, hi, jnp.where(lane == 1, mid, jnp.where(lane == 2, low, 0.0)))
        out.append(jnp.concatenate([jnp.where(mine, do, 0.0), aug], axis=1))
    return jnp.concatenate(out, axis=0).astype(BF)


def attn_specs(rows, prompt, blocks):
    def col(n):
        return pl.BlockSpec((n, 128), lambda i, l: (0, i))

    logs = pl.BlockSpec((1, blocks, 8, CLEN), lambda i, l: (i, 0, 0, 0))
    return col(rows), col(prompt), logs


class Weight:
    def __init__(self, me, own, spots, view, sems):
        self.me, self.own, self.spots, self.view = me, own, spots, view
        self.send, self.recv = sems

    def side(self):
        return remote(self.own, self.spots(1), self.send.at[0], self.recv.at[0], self.me.core)

    def across(self):
        p = self.me.p
        return remote(self.view(None, p), self.view(2, p), self.send.at[1], self.recv.at[1], self.me.x)

    def pair(self):
        p = self.me.p
        return remote(self.view(2, p), self.view(2, p), self.send.at[2], self.recv.at[2], self.me.y)

    def over(self, which):
        h = self.me.p if which == 0 else 1 - self.me.p
        return remote(self.view(2, h), self.view(3, h), self.send.at[3 + which], self.recv.at[3 + which], self.me.core)

    def start(self):
        self.side().start()
        self.across().start()

    def relay(self):
        self.across().wait_recv()
        self.pair().start()
        self.over(0).start()

    def relay_pair(self):
        self.pair().wait_recv()
        self.over(1).start()

    def finish(self):
        self.side().wait()
        self.across().wait_send()
        self.pair().wait_send()
        self.over(0).wait()
        self.over(1).wait()


def norm_rows(x, gain, shift):
    x = x.astype(F32)
    centred = x - jnp.mean(x, axis=-1, keepdims=True)
    scale = lax.rsqrt(jnp.mean(centred * centred, axis=-1, keepdims=True) + EPS)
    return (centred * scale * gain + shift).astype(BF)


def front_kernel(lens, x_ref, gain_ref, shift_ref, wq, wp, wi, wo, ws,
                 q_ref, kp_ref, vp_ref, ko_ref, vo_ref, ctx_ref, lse_ref, an_ref, anp_ref, px_ref,
                 wq_all, wp_all, wi_all, wo_all, ws_all,
                 px, wv, wsv, kph, vpt, px_s, px_r, send, recv, loc):
    me = Peers()
    step = pl.program_id(0)
    rows = x_ref.shape[0]
    blocks = rows // CLEN
    prompt = px.shape[0]
    part = wq.shape[1]
    own_chunks = rows // CLEN
    chunks = prompt // CLEN

    def qkv_view(r, h):
        n = part // 2
        if r is None:
            return wq.at[:, pl.ds(h * n, n)]
        return wv.at[:, pl.ds(r * part + h * n, n)]

    def plain(own, everything):
        n = own.shape[0] // 2

        def view(r, h):
            return own.at[pl.ds(h * n, n)] if r is None else everything.at[r, pl.ds(h * n, n)]

        return view

    def weight(i, own, everything):
        return Weight(me, own, lambda r: everything.at[r], plain(own, everything), (send.at[i], recv.at[i]))

    w_qkv = Weight(me, wq, lambda r: wv.at[:, pl.ds(r * part, part)], qkv_view, (send.at[0], recv.at[0]))
    w_small = weight(1, ws, wsv)
    w_proj = weight(2, wp, wp_all)
    w_in = weight(3, wi, wi_all)
    w_out = weight(4, wo, wo_all)
    later = [w_proj, w_in, w_out]

    def keep(own, spot, i):
        return pltpu.make_async_copy(own, spot, loc.at[i])

    mine = [
        keep(wq, wv.at[:, pl.ds(0, part)], 0), keep(ws, wsv.at[0], 1), keep(wp, wp_all.at[0], 2),
        keep(wi, wi_all.at[0], 3), keep(wo, wo_all.at[0], 4), keep(wv, wq_all, 5), keep(wsv, ws_all, 6), keep(px, px_ref, 7),
    ]

    def chunk(k):
        return px.at[pl.ds(k * CLEN, CLEN)]

    def held(k):
        at = k if k < own_chunks else k - own_chunks
        return x_ref.at[pl.ds(at * CLEN, CLEN)]

    def hop(k, src, n, device):
        return remote(src, chunk(k), px_s.at[n, k], px_r.at[n, k], device)

    first = [k for k in range(chunks) if k < own_chunks]
    second = [k for k in range(chunks) if k >= own_chunks]
    low = [k for k in range(chunks) if k < chunks // 2]
    high = second + [k for k in range(chunks // 2, own_chunks)]

    def normed(k):
        anp_ref[k * CLEN : (k + 1) * CLEN, :] = norm_rows(px[k * CLEN : (k + 1) * CLEN, :], gain_ref[...], shift_ref[...])

    @pl.when(step == 0)
    def _():
        enter([me.core, me.x, me.y])

        @pl.when(me.t == 0)
        def _():
            for k in low:
                hop(k, held(k), 1, me.x).start()
            for k in reversed(first):
                hop(k, held(k), 0, me.core).start()

        @pl.when(me.t == 1)
        def _():
            for k in second:
                hop(k, held(k), 1, me.x).start()
                hop(k, held(k), 0, me.core).start()

        for w in (w_qkv, w_small):
            w.side().start()
        for i in range(5):
            mine[i].start()

        @pl.when(me.t == 1)
        def _():
            for k in reversed(first):
                hop(k, held(k), 0, me.core).wait_recv()
                if k in high:
                    hop(k, chunk(k), 1, me.x).start()

        for w in (w_qkv, w_small):
            w.across().start()
        for w in later:
            w.side().start()
        for b in range(blocks):
            an_ref[b * CLEN : (b + 1) * CLEN, :] = norm_rows(x_ref[b * CLEN : (b + 1) * CLEN, :], gain_ref[...], shift_ref[...])

        @pl.when(me.t == 0)
        def _():
            for k in first:
                px[k * CLEN : (k + 1) * CLEN, :] = x_ref[k * CLEN : (k + 1) * CLEN, :]
            for k in second:
                hop(k, held(k), 0, me.core).wait_recv()
            for k in first:
                hop(k, held(k), 0, me.core).wait_send()
            for k in low:
                hop(k, held(k), 1, me.x).wait_send()

        @pl.when(me.t == 1)
        def _():
            for k in second:
                px[k * CLEN : (k + 1) * CLEN, :] = held(k)[...]
                hop(k, held(k), 0, me.core).wait_send()
            for k in high:
                hop(k, chunk(k), 1, me.x).wait_send()

        @pl.when(me.t == 2)
        def _():
            for k in low:
                hop(k, chunk(k), 1, me.x).wait_recv()
                hop(k, chunk(k), 0, me.core).start()
            for k in high:
                hop(k, chunk(k), 0, me.core).wait_recv()
            for k in low:
                hop(k, chunk(k), 0, me.core).wait_send()

        @pl.when(me.t == 3)
        def _():
            for k in high:
                hop(k, chunk(k), 1, me.x).wait_recv()
                hop(k, chunk(k), 0, me.core).start()
            for k in low:
                hop(k, chunk(k), 0, me.core).wait_recv()
            for k in high:
                hop(k, chunk(k), 0, me.core).wait_send()

        for k in range(chunks):
            normed(k)
        w_small.relay()
        for w in (w_qkv, w_small):
            w.side().wait_recv()
        for i in range(2):
            mine[i].wait()

    @pl.when(step == 3)
    def _():
        for w in (w_qkv, w_small):
            w.over(0).wait_recv()
            w.over(1).wait_recv()
        mine[5].start()
        mine[6].start()
        mine[7].start()

    def moves(slot):
        def at(k, *steps):
            @pl.when(slot == k)
            def _():
                for s in steps:
                    s()

        at(2, w_qkv.relay, *[lambda w=w: w.across().start() for w in later])
        at(6, w_qkv.relay_pair, w_small.relay_pair)
        at(9, w_proj.relay)
        at(11, w_proj.relay_pair)
        at(13, w_in.relay)
        at(16, w_in.relay_pair)

    pick = pl.ds(pl.multiple_of(step * 128, 128), 128)
    w3 = jnp.concatenate([wv[0, pick], wv[1, pick], wv[2, pick]], axis=0)
    u = 2 * lax.div(step, 3)
    left = wsv[u, :16, pick].astype(F32)
    right = wsv[u + 1, :16, pick].astype(F32)
    spot = lax.broadcasted_iota(jnp.int32, left.shape, 0)

    def bias(k):
        return jnp.sum(jnp.where(spot == u + k, left, 0.0) + jnp.where(spot == u + 1 + k, right, 0.0), axis=0, keepdims=True)

    bq = bias(0)
    bv = bias(PIECES)
    for b in range(blocks):
        at = slice(b * CLEN, (b + 1) * CLEN)
        got = nt(an_ref[at, :], w3)
        q_ref[at, :] = (got[:, :128] + bq).astype(BF)
        ko_ref[at, :] = got[:, 128:256].astype(BF)
        vo_ref[at, :] = (got[:, 256:] + bv).astype(BF)
    for c in range(chunks):
        at = slice(c * CLEN, (c + 1) * CLEN)
        got = nt(anp_ref[at, :], w3[128:])
        kp_ref[at, :] = got[:, :128].astype(BF)
        vp_ref[at, :] = (got[:, 128:] + bv).astype(BF)

    vt = transposed(vp_ref[...])
    for h in range(2):
        kph[h] = key_aug(kp_ref[...], h, lens[0], 0)
        vpt[h] = jnp.concatenate([vt[64 * h : 64 * h + 64].astype(BF), jnp.ones((16, prompt), BF)], axis=0)

    def block(b, _):
        moves(step * blocks + b)
        at = pl.ds(pl.multiple_of(b * CLEN, CLEN), CLEN)
        q = q_ref[at, :]
        ko = ko_ref[at, :]
        vot = transposed(vo_ref[at, :])
        outs, logs = [], []
        for h in range(2):
            qh = query_aug(q, h)
            vh = jnp.concatenate([vot[64 * h : 64 * h + 64].astype(BF), jnp.ones((16, CLEN), BF)], axis=0)
            sp = nt(kph[h], qh)
            so = nt(key_aug(ko, h, lens[1 + b], 0), qh)
            top = jnp.maximum(jnp.max(sp, axis=0, keepdims=True), jnp.max(so, axis=0, keepdims=True))
            pp = jnp.exp(sp - top).astype(BF)
            po = jnp.exp(so - top).astype(BF)
            ot = nn(vpt[h], pp) + nn(vh, po)
            total = ot[64:65]
            outs.append(ot[:64] * (1.0 / total))
            logs.append(top + jnp.log(total))
        ctx_ref[at, :] = jnp.concatenate(outs, axis=0).T.astype(BF)
        lse_ref[0, b] = jnp.concatenate(logs + [jnp.zeros((6, CLEN), F32)], axis=0)
        return 0

    lax.fori_loop(0, blocks, block, 0)

    @pl.when(step == pl.num_programs(0) - 1)
    def _():
        w_out.relay()
        w_out.relay_pair()
        for w in [w_qkv, w_small]:
            w.side().wait_send()
            w.across().wait_send()
            w.pair().wait_send()
            w.over(0).wait_send()
            w.over(1).wait_send()
        for w in later:
            w.finish()
        for i in range(2, 8):
            mine[i].wait()


def front_call(lens, x, gain, shift, wq, wp, wi, wo, ws):
    rows, width = x.shape
    blocks = rows // CLEN
    pairs = width // 128
    r, p, logs = attn_specs(rows, PROMPT, blocks)
    cells = rows * (PROMPT + CLEN) * pairs * 2

    def whole(n):
        return pl.BlockSpec((n, width), lambda i, l: (0, 0))

    def shape(*s):
        return jax.ShapeDtypeStruct(s, BF)

    part = wq.shape[1]
    return pl.pallas_call(
        front_kernel,
        out_shape=(
            shape(rows, width), shape(PROMPT, width), shape(PROMPT, width), shape(rows, width), shape(rows, width),
            shape(rows, width), jax.ShapeDtypeStruct((pairs, blocks, 8, CLEN), F32),
            shape(rows, width), shape(PROMPT, width), shape(PROMPT, width),
            shape(3, PIECES * part, width), shape(PIECES, *wp.shape), shape(PIECES, *wi.shape),
            shape(PIECES, *wo.shape), shape(PIECES, *ws.shape),
        ),
        grid_spec=pltpu.PrefetchScalarGridSpec(
            num_scalar_prefetch=1,
            grid=(pairs,),
            in_specs=[whole(rows), whole(1), whole(1), ANY, ANY, ANY, ANY, ANY],
            out_specs=[r, p, p, r, r, r, logs, whole(rows), whole(PROMPT), ANY, ANY, ANY, ANY, ANY, ANY],
            scratch_shapes=[
                pltpu.VMEM((PROMPT, width), BF),
                pltpu.VMEM((3, PIECES * part, width), BF),
                pltpu.VMEM((PIECES,) + ws.shape, BF),
                pltpu.VMEM((2, PROMPT, 128), BF),
                pltpu.VMEM((2, 80, PROMPT), BF),
                pltpu.SemaphoreType.DMA((2, PROMPT // CLEN)),
                pltpu.SemaphoreType.DMA((2, PROMPT // CLEN)),
                pltpu.SemaphoreType.DMA((5, 5)),
                pltpu.SemaphoreType.DMA((5, 5)),
                pltpu.SemaphoreType.DMA((8,)),
            ],
        ),
        compiler_params=pltpu.CompilerParams(collective_id=0, has_side_effects=True, vmem_limit_bytes=48 << 20),
        cost_estimate=pl.CostEstimate(flops=cells * 256 * 4, transcendentals=cells, bytes_accessed=4 << 20),
        name="front",
    )(lens, x, gain, shift, wq, wp, wi, wo, ws)


STAGES = 7


def chunk_rows(rows, dp):
    unit = 16 * (min(dp, NEAR) // 2)
    return -(-rows // unit) * unit


class Sums:
    def __init__(self, me, half, piece_of, keep, scratch):
        self.me, self.half, self.piece_of, self.keep = me, half, piece_of, keep
        if keep is True:
            self.g0, self.g2, self.local = scratch[:3]
            scratch = scratch[3:]
        (self.r1, self.r3, self.xr, self.yr, self.zr, self.own,
         self.core_s, self.core_r, self.xs, self.ys, self.zs, self.zrs, self.fs, self.frs, self.gs) = scratch
        self.chunks, self.rows, self.width = self.r1.shape
        self.wide = self.width // 2
        self.share = self.rows // half
        self.mine = pl.ds(pl.multiple_of(me.p * self.wide, 128), self.wide)
        self.other = pl.ds(pl.multiple_of((1 - me.p) * self.wide, 128), self.wide)

    @staticmethod
    def scratch(chunks, rows, width, half, keep):
        def buf(*s, dtype=BF):
            return pltpu.VMEM((chunks,) + s, dtype)

        def dma(n):
            return pltpu.SemaphoreType.DMA((chunks, n))

        wide = width // 2
        first = [buf(rows, width), buf(rows, width), dma(2)] if keep is True else []
        return first + [
            buf(rows, width), buf(rows, width), buf(rows, width), buf(rows, wide),
            buf(half, rows // half, wide), buf(rows // half, wide, dtype=F32),
            dma(2), dma(2), dma(2), dma(2), dma(half), dma(half), dma(half), dma(half), dma(2),
        ]

    def held(self, c, r):
        if self.keep is True:
            return (self.g0 if r == 0 else self.g2).at[c]
        return self.piece_of(c, None)(r)

    def from_core(self, c, i, src=None):
        into = (self.r1, self.r3)[i].at[c]
        return remote(into if src is None else src, into, self.core_s.at[c, i], self.core_r.at[c, i], self.me.core)

    def load(self, c, i, src=None):
        into = (self.g0, self.g2)[i].at[c]
        return pltpu.make_async_copy(into if src is None else src, into, self.local.at[c, i])

    def across(self, c):
        return remote(self.held(c, 2), self.xr.at[c], self.xs.at[c, 0], self.xs.at[c, 1], self.me.x)

    def pair(self, c):
        return remote(self.held(c, 0).at[:, self.other], self.yr.at[c], self.ys.at[c, 0], self.ys.at[c, 1], self.me.y)

    def rows_of(self, k):
        at = lax.rem(self.me.z + k, self.half) * self.share
        return pl.ds(pl.multiple_of(at, 16), self.share)

    def rest(self, c, k):
        return remote(self.held(c, 0).at[self.rows_of(k), self.mine], self.zr.at[c, k],
                      self.zs.at[c, k], self.zrs.at[c, k], self.me.along(k, self.half))

    def back(self, c, k):
        spot = self.xr.at[c, self.rows_of(0), self.mine]
        return remote(spot, spot, self.fs.at[c, k], self.frs.at[c, k], self.me.along(k, self.half))

    def back_pair(self, c):
        spot = self.xr.at[c, :, self.mine]
        return remote(spot, spot, self.gs.at[c, 0], self.gs.at[c, 1], self.me.y)

    def start(self, c, i):
        def go(piece):
            self.from_core(c, i, piece(1 + 2 * i)).start()
            if self.keep is True:
                self.load(c, i, piece(2 * i)).start()

        self.piece_of(c, go)

    def blocks(self, body):
        def one(k, _):
            body(pl.ds(pl.multiple_of(k * self.share, 16), self.share))
            return 0

        lax.fori_loop(0, self.half, one, 0)

    def to_chip(self, c):
        self.from_core(c, 1).wait()
        if self.keep is True:
            self.load(c, 1).wait()
        g2 = self.held(c, 2)

        def body(s):
            g2[s, :] = (g2[s, :].astype(F32) + self.r3[c, s, :].astype(F32)).astype(BF)

        self.blocks(body)
        self.across(c).start()
        if self.keep is True:
            self.start(c, 0)

            @pl.when(c + 3 < self.chunks)
            def _():
                self.start(c + 3, 1)

    def term(self, c, s, lanes):
        g0 = self.held(c, 0)
        return g0[s, lanes].astype(F32) + self.r1[c, s, lanes].astype(F32) + self.xr[c, s, lanes].astype(F32)

    def to_pair(self, c):
        self.from_core(c, 0).wait()
        if self.keep is True:
            self.load(c, 0).wait()
        self.across(c).wait()

        @pl.when(c + 2 < self.chunks)
        def _():
            self.to_chip(c + 2)

        g0 = self.held(c, 0)

        def body(s):
            g0[s, self.other] = self.term(c, s, self.other).astype(BF)

        self.blocks(body)
        self.pair(c).start()

    def to_rest(self, c):
        self.pair(c).wait()
        g0 = self.held(c, 0)
        at = self.rows_of(0)
        self.own[c] = self.term(c, at, self.mine) + self.yr[c, at, :].astype(F32)

        def body(s):
            g0[s, self.mine] = (self.term(c, s, self.mine) + self.yr[c, s, :].astype(F32)).astype(BF)

        self.blocks(body)
        for k in range(1, self.half):
            self.rest(c, k).start()

    def to_back(self, c):
        total = self.own[c]
        for k in range(1, self.half):
            self.rest(c, k).wait()
            total = total + self.zr[c, k].astype(F32)
        self.xr[c, self.rows_of(0), self.mine] = total.astype(BF)
        for k in range(1, self.half):
            self.back(c, k).start()

    def to_back_pair(self, c):
        for k in range(1, self.half):
            self.back(c, k).wait()
        self.back_pair(c).start()

    def finish(self, c):
        self.back_pair(c).wait()

    def progress(self, plan, slot):
        steps = [None, self.to_chip, self.to_pair, self.to_rest, self.to_back, self.to_back_pair, self.finish]
        for s in range(STAGES - 1, 0, -1):
            since = slot - plan[s]
            c = lax.div(since, 2)
            due = jnp.logical_and(since >= 0, lax.rem(since, 2) == 0)

            @pl.when(jnp.logical_and(due, c < (2 if s == 1 else self.chunks)))
            def _():
                steps[s](c)


class SmallSum:
    def __init__(self, me, half, sm, scratch):
        self.me, self.half, self.sm = me, half, sm
        self.got, self.z, self.s, self.r = scratch

    @staticmethod
    def scratch(rows, width, half):
        return [
            pltpu.VMEM((4, rows, width), F32),
            pltpu.VMEM((half, rows, width), F32),
            pltpu.SemaphoreType.DMA((4 + half,)),
            pltpu.SemaphoreType.DMA((4 + half,)),
        ]

    def copy(self, i):
        src, device = [(1, self.me.core), (3, self.me.core), (2, self.me.x), (0, self.me.y)][i]
        return remote(self.sm.at[src], self.got.at[i], self.s.at[i], self.r.at[i], device)

    def rest(self, k):
        return remote(self.sm.at[0], self.z.at[k], self.s.at[4 + k], self.r.at[4 + k], self.me.along(k, self.half))

    def start(self):
        self.copy(1).start()
        self.copy(0).start()

    def to_chip(self):
        self.copy(1).wait()
        self.sm[2] = self.sm[2] + self.got[1]
        self.copy(2).start()

    def to_pair(self):
        self.copy(0).wait()
        self.copy(2).wait()
        self.sm[0] = self.sm[0] + self.got[0] + self.got[2]
        self.copy(3).start()

    def to_rest(self):
        self.copy(3).wait()
        self.sm[0] = self.sm[0] + self.got[3]
        for k in range(1, self.half):
            self.rest(k).start()

    def finish(self):
        total = self.sm[0]
        for k in range(1, self.half):
            self.rest(k).wait()
            total = total + self.z[k]
        return total


SUB = 3
FFN_PLAN = {1: 0, 2: 4, 3: 6, 4: 8, 5: 10, 6: 12}
QKV_PLAN = {1: 18, 2: 22, 3: 24, 4: 26, 5: 28, 6: 30}
QKV_START = (9, 18)
PROMPT_PLAN = (27, 34)
SMALL_PLAN = (19, 21, 23, 25, 29)
LAST_SLOT = 35


def back_kernel(half, grid_pairs, part, rows_c, lens, q_ref, kp_ref, vp_ref, ko_ref, vo_ref, do_ref, ctx_ref, lse_ref,
                w_ref, an_ref, anp_ref, x_ref, px_ref, sm_ref, gi0, gi1, gi2, gi3, go0, go1, go2, go3, gp,
                own_ref, ffn_out, qkv_out, small_out, extra_out,
                kx, vx, kt_s, acc, dqt, dkt, dvt, prompt_acc, share_s, gq, sm, qv,
                came, total, over, ex, p_s, p_r, o_s, *scratch):
    me = Peers()
    step = pl.program_id(0)
    rows = q_ref.shape[0]
    width = an_ref.shape[1]
    blocks = rows // CLEN
    prompt = kp_ref.shape[0]
    chunks = prompt // CLEN
    n_ffn = 17 + 1
    ffn_scratch, scratch = scratch[:n_ffn], scratch[n_ffn:]
    qkv_scratch, small_scratch = scratch[:15], scratch[15:]
    gin, gout = (gi0, gi1, gi2, gi3), (go0, go1, go2, go3)
    per = gi0.shape[0] // rows_c

    def ffn_piece(c, go):
        @pl.when(c < per)
        def _():
            go(lambda r: gin[r].at[pl.ds(pl.multiple_of(c * rows_c, 16), rows_c)])

        @pl.when(jnp.logical_and(c >= per, c < 2 * per))
        def _():
            go(lambda r: gout[r].at[pl.ds(pl.multiple_of((c - per) * rows_c, 16), rows_c)])

        @pl.when(c >= 2 * per)
        def _():
            go(lambda r: gp.at[r])

    def qkv_piece(c, go):
        def piece(r):
            return gq.at[c, r]

        return piece if go is None else go(piece)

    ffn = Sums(me, half, ffn_piece, True, ffn_scratch)
    qkv = Sums(me, half, qkv_piece, False, qkv_scratch)
    smalls = SmallSum(me, half, sm, small_scratch)
    n = prompt // 2
    spare = rows - n
    side = remote(share_s.at[pl.ds((1 - me.odd) * n, n)], came, p_s.at[0], p_r.at[0], me.core)
    across = remote(total, over, p_s.at[1], p_r.at[1], me.x)
    end = remote(total.at[pl.ds(0, spare)], ex.at[pl.ds(n, spare)], p_s.at[2], p_r.at[2], me.core)

    @pl.when(step == 0)
    def _():
        enter([me.core, me.x, me.y] + [me.along(k, half) for k in range(1, half)])
        for c in range(3):
            ffn.start(jnp.int32(c), 1)
        own_ref[...] = jnp.zeros_like(own_ref)
        prompt_acc[...] = jnp.zeros_like(prompt_acc)
        if rows_c != part:
            gq[...] = jnp.zeros_like(gq)

    spot = lax.rem(step, grid_pairs // 2)

    @pl.when(step < grid_pairs)
    def _():
        acc[...] = jnp.zeros_like(acc)
        kx[:prompt] = wide_keys(kp_ref[...], lens[0], 0)
        vx[:prompt] = wide_values(vp_ref[...])
        vx[prompt:] = wide_values(vo_ref[...])
        kt_s[:, :prompt] = transposed(kp_ref[...]).astype(BF)
        kt_s[:, prompt:] = transposed(ko_ref[...]).astype(BF)
        for b in range(blocks):
            at = slice(b * CLEN, (b + 1) * CLEN)
            kx[prompt + b * CLEN : prompt + (b + 1) * CLEN] = wide_keys(ko_ref[at, :], lens[1 + b], 0)

    def block(b):
        at = pl.ds(pl.multiple_of(b * CLEN, CLEN), CLEN)
        own = pl.ds(pl.multiple_of(prompt + b * CLEN, CLEN), CLEN)
        q = q_ref[at, :]
        do = do_ref[at, :]
        q2 = wide_queries(q)
        do2 = wide_grads(do, ctx_ref[at, :])
        qt = transposed(q).astype(BF)
        dot = transposed(do).astype(BF)
        logs = jnp.concatenate([lse_ref[0, b, 0:1, :], lse_ref[0, b, 1:2, :]], axis=1)

        def scores(keys):
            p = jnp.exp(nt(kx[keys, :], q2) - logs)
            ds = (p * nt(vx[keys, :], do2)).astype(BF)
            p = p.astype(BF)
            parts = []
            for left, m in ((qt, ds), (dot, p)):
                parts.append([nt(left[64 * h : 64 * h + 64], m[:, h * CLEN : (h + 1) * CLEN]) for h in range(2)])
            return parts, nn(kt_s[:, keys], ds)

        (dk, dv), dq = scores(pl.ds(0, prompt))
        for h in range(2):
            rows_h = slice(64 * h, 64 * h + 64)
            acc[0, rows_h, :] += dk[h]
            acc[1, rows_h, :] += dv[h]
        (dk, dv), dq_own = scores(own)
        dkt[spot, :, own] = (jnp.concatenate(dk, axis=0) * 0.125).astype(BF)
        dvt[spot, :, own] = jnp.concatenate(dv, axis=0).astype(BF)
        dq = dq + dq_own
        dqt[spot, :, at] = (jnp.concatenate([dq[:64, :CLEN], dq[64:, CLEN:]], axis=0) * 0.125).astype(BF)

        @pl.when(b == blocks - 1)
        def _():
            dkt[spot, :, :prompt] = (acc[0] * 0.125).astype(BF)
            dvt[spot, :, :prompt] = acc[1].astype(BF)

    def sub_step(sub, _):
        slot = step * SUB + sub
        ffn.progress(FFN_PLAN, slot)

        def at(k, body):
            @pl.when(slot == k)
            def _():
                body()

        def qkv_start(i):
            for c in range(3):
                qkv.start(c, i)

        at(QKV_START[0], lambda: qkv_start(1))
        at(QKV_START[1], lambda: qkv_start(0))
        qkv.progress(QKV_PLAN, slot)

        def prompt_chip():
            side.wait()
            mine = pl.ds(pl.multiple_of(me.odd * n, 16), n)
            total[...] = (share_s[mine, :].astype(F32) + came[...].astype(F32)).astype(BF)

            @pl.when(me.t >= 2)
            def _():
                across.start()

        def prompt_end():
            @pl.when(me.t >= 2)
            def _():
                ex[...] = jnp.zeros_like(ex)
                across.wait_send()

            @pl.when(me.t < 2)
            def _():
                across.wait_recv()
                total[...] = (total[...].astype(F32) + over[...].astype(F32)).astype(BF)

            @pl.when(me.t == 1)
            def _():
                end.start()
                ex[: n - spare] = total[spare:]
                ex[n - spare :] = jnp.zeros((rows - n + spare, width), BF)
                end.wait_send()

            @pl.when(me.t == 0)
            def _():
                ex[:n] = total[...]
                end.wait_recv()

        def small_end():
            small_out[...] = smalls.finish()

        at(SMALL_PLAN[0], smalls.start)
        at(SMALL_PLAN[1], smalls.to_chip)
        at(SMALL_PLAN[2], smalls.to_pair)
        at(SMALL_PLAN[3], smalls.to_rest)
        at(SMALL_PLAN[4], small_end)
        at(PROMPT_PLAN[0], prompt_chip)
        at(PROMPT_PLAN[1], prompt_end)

        @pl.when(step < grid_pairs)
        def _():
            block(sub)

        return 0

    lax.fori_loop(0, SUB, sub_step, 0)

    @pl.when(jnp.logical_and(step < grid_pairs, spot == grid_pairs // 2 - 1))
    def _():
        unit = grid_pairs // 2
        late = step < unit
        feats = unit * 128
        dq, dk, dv = (r[...].reshape(feats, -1) for r in (dqt, dkt, dvt))
        an = an_ref[...]
        anp = anp_ref[...]
        for j, d in enumerate((dq, dk, dv)):
            g = nn(d, an) if j == 0 else nn(d[:, prompt:], an) + nn(d[:, :prompt], anp)
            for k in range(2):
                r = jnp.where(late, 2, 0) + k
                gq[j, r, :part, :] = g[k * part : (k + 1) * part].astype(BF)
        sum_q = jnp.sum(dq.astype(F32), axis=1, keepdims=True)
        sum_v = jnp.sum(dv.astype(F32), axis=1, keepdims=True)
        both = jnp.concatenate([jnp.broadcast_to(sum_q, (feats, 128)), jnp.broadcast_to(sum_v, (feats, 128))], axis=1).T
        lanes = pl.ds(pl.multiple_of(jnp.where(late, feats, 0), 128), feats)
        qv[0:1, lanes] = both[0:1]
        qv[1:2, lanes] = both[128:129]
        d3 = jnp.concatenate([dq, dk[:, prompt:], dv[:, prompt:]], axis=0)
        w3 = jnp.concatenate([w_ref[0], w_ref[1], w_ref[2]], axis=0)
        d2 = jnp.concatenate([dk[:, :prompt], dv[:, :prompt]], axis=0)
        for d, w, out, count in ((d3, w3, own_ref, blocks), (d2, w3[feats:], prompt_acc, chunks)):
            for c in range(count):
                at = slice(c * CLEN, (c + 1) * CLEN)
                got = tn(d[:, at], w)
                out[at, :] += got

    @pl.when(step == grid_pairs - 1)
    def _():
        for c in range(chunks):
            at = slice(c * CLEN, (c + 1) * CLEN)
            share_s[at, :] = prompt_acc[at, :].astype(BF)
        side.start()
        sum_g = jnp.zeros((1, width), F32)
        sum_c = jnp.zeros((1, width), F32)
        for grad, raw, count in ((own_ref, x_ref, blocks), (prompt_acc, px_ref, chunks)):
            for c in range(count):
                at = slice(c * CLEN, (c + 1) * CLEN)
                x = raw[at, :].astype(F32)
                x = x - jnp.mean(x, axis=-1, keepdims=True)
                normal = x * lax.rsqrt(jnp.mean(x * x, axis=-1, keepdims=True) + EPS)
                sum_g = sum_g + jnp.sum(grad[at, :] * normal, axis=0, keepdims=True)
                sum_c = sum_c + jnp.sum(grad[at, :], axis=0, keepdims=True)
        for r in range(PIECES):
            sm[r] = sm_ref[r]
            for i in range(2):
                row = qv[i : i + 1, :]
                sm[r, 8 + i : 9 + i, :] = row if r == 0 else pltpu.roll(row, width - r * part, 1)
            sm[r, 10:11, :] = sum_g
            sm[r, 11:12, :] = sum_c

    @pl.when(step == pl.num_programs(0) - 1)
    def _():
        outs = [(ffn.xr, ffn_out), (qkv.xr, qkv_out), (ex, extra_out)]
        copies = [pltpu.make_async_copy(a, b, o_s.at[i]) for i, (a, b) in enumerate(outs)]
        for c in copies:
            c.start()
        for c in copies:
            c.wait()


def back_call(lens, q, kp, vp, ko, vo, do, ctx, lse, wq_all, an, anp, x, px, small, gin, gout, gproj, dp, part):
    rows, width = q.shape
    prompt = kp.shape[0]
    blocks = rows // CLEN
    pairs = width // 128
    half = min(dp, NEAR) // 2
    rows_c = gproj.shape[1]
    cells = rows * (prompt + CLEN) * pairs * 2
    n_ffn = 2 * (gin[0].shape[0] // rows_c) + 1
    steps = -(-LAST_SLOT // SUB)
    assert blocks == SUB
    small_n = small.shape[1]

    def pair(i):
        return lax.rem(jnp.minimum(i, pairs - 1) + pairs // 2, pairs)

    def col(n):
        return pl.BlockSpec((n, 128), lambda i, l: (0, pair(i)))

    def whole(*s):
        return pl.BlockSpec(s, lambda i, l: (0,) * len(s), pipeline_mode=pl.Buffered(1))

    def result(*s):
        return pl.BlockSpec(s, lambda i, l: (0,) * len(s))

    r, p = col(rows), col(prompt)
    logs = pl.BlockSpec((1, blocks, 8, CLEN), lambda i, l: (pair(i), 0, 0, 0))
    w = pl.BlockSpec((3, width // 2, width), lambda i, l: (0, lax.div(pair(i), pairs // 2), 0))
    return pl.pallas_call(
        functools.partial(back_kernel, half, pairs, part, rows_c),
        out_shape=(
            jax.ShapeDtypeStruct((rows, width), F32),
            jax.ShapeDtypeStruct((n_ffn, rows_c, width), BF),
            jax.ShapeDtypeStruct((3, rows_c, width), BF),
            jax.ShapeDtypeStruct((small_n, width), F32),
            jax.ShapeDtypeStruct((rows, width), BF),
        ),
        grid_spec=pltpu.PrefetchScalarGridSpec(
            num_scalar_prefetch=1,
            grid=(steps,),
            in_specs=[r, p, p, r, r, r, r, logs, w, whole(rows, width), whole(prompt, width), whole(rows, width),
                      whole(prompt, width), whole(PIECES, small_n, width)] + [ANY] * 9,
            out_specs=[result(rows, width), ANY, ANY, result(small_n, width), ANY],
            scratch_shapes=[
                pltpu.VMEM((prompt + rows, 256), BF),
                pltpu.VMEM((prompt + rows, 256), BF),
                pltpu.VMEM((128, prompt + rows), BF),
                pltpu.VMEM((2, 128, prompt), F32),
                pltpu.VMEM((pairs // 2, 128, rows), BF),
                pltpu.VMEM((pairs // 2, 128, prompt + rows), BF),
                pltpu.VMEM((pairs // 2, 128, prompt + rows), BF),
                pltpu.VMEM((prompt, width), F32),
                pltpu.VMEM((prompt, width), BF),
                pltpu.VMEM((3, PIECES, rows_c, width), BF),
                pltpu.VMEM((PIECES, small_n, width), F32),
                pltpu.VMEM((8, width), F32),
                pltpu.VMEM((prompt // 2, width), BF),
                pltpu.VMEM((prompt // 2, width), BF),
                pltpu.VMEM((prompt // 2, width), BF),
                pltpu.VMEM((rows, width), BF),
                pltpu.SemaphoreType.DMA((3,)),
                pltpu.SemaphoreType.DMA((3,)),
                pltpu.SemaphoreType.DMA((3,)),
            ]
            + Sums.scratch(n_ffn, rows_c, width, half, True)
            + Sums.scratch(3, rows_c, width, half, False)
            + SmallSum.scratch(small_n, width, half),
        ),
        compiler_params=pltpu.CompilerParams(collective_id=1, has_side_effects=True, vmem_limit_bytes=62 << 20),
        cost_estimate=pl.CostEstimate(flops=cells * 256 * 10, transcendentals=cells, bytes_accessed=16 << 20),
        name="back",
    )(lens, q, kp, vp, ko, vo, do, ctx, lse, wq_all, an, anp, x, px, small, *gin, *gout, gproj)


def normalize(values):
    centred = values - jnp.mean(values, axis=-1, keepdims=True)
    scale = lax.rsqrt(jnp.mean(centred * centred, axis=-1, keepdims=True) + EPS)
    return centred * scale, scale


def norm_back(grad, normal, scale, gain):
    e = grad * gain
    return scale * (e - jnp.mean(e, axis=-1, keepdims=True) - normal * jnp.mean(e * normal, axis=-1, keepdims=True))


def small_rows(rows, rows_pad):
    width = rows[0].shape[-1]
    rows = [jnp.broadcast_to(r, (PIECES, width)) for r in rows]
    rows = rows + [jnp.zeros((PIECES, width), F32)] * (rows_pad - len(rows))
    return jnp.stack(rows, axis=1)


def shards(layer_in, prompt_len, cont_len, w_qkv, b_qv, w_proj, b_proj, ln1_gain, ln1_bias,
           ln2_gain, ln2_bias, w_in, b_in, w_out, b_out, out_grad):
    rows, width = layer_in.shape
    blocks = rows // CLEN
    dp = lax.axis_size("dp")
    part = w_qkv.shape[2]
    t = lax.axis_index("tensor")
    g1, c1, g2, c2 = (v.astype(F32)[None] for v in (ln1_gain, ln1_bias, ln2_gain, ln2_bias))

    group = t * blocks + jnp.arange(blocks)
    conts = group - PROMPT // CLEN
    own_len = jnp.where(conts >= 0, cont_len[0][jnp.clip(conts, 0, CONT - 1)], 0)
    lens = jnp.concatenate([prompt_len, own_len]).astype(jnp.int32)

    bias_rows = [jnp.pad(b_qv[i : i + 1], ((0, 0), (r * part, width - (r + 1) * part))) for i in range(2) for r in range(PIECES)]
    small = jnp.concatenate(bias_rows + [jnp.zeros((8, width), BF), b_in[None], jnp.zeros((15, width), BF)], axis=0)
    (q, kp, vp, ko, vo, ctx, lse, attn_input, prompt_input, prompt_rows, wq_all, wp_all, wi_all, wo_all, ws_all) = front_call(
        lens, layer_in, g1, c1, w_qkv.transpose(0, 2, 1), w_proj, w_in, w_out, small
    )

    w_proj_all = wp_all.reshape(width, width)
    rows_in = layer_in.astype(F32)
    hidden = rows_in + nn(ctx, w_proj_all) + b_proj.astype(F32)
    normal2, scale2 = normalize(hidden)
    mlp_input = (normal2 * g2 + c2).astype(BF)

    branch = 0.0
    grad_mlp_in = 0.0
    grad_in_pieces, grad_out_pieces, grad_b_in_pieces = [], [], []
    for r in range(PIECES):
        pre = nn(mlp_input, wi_all[r]) + ws_all[r, 16].astype(F32)
        cdf = 0.5 * (1.0 + lax.erf(pre * (0.5**0.5)))
        pdf = jnp.exp(-0.5 * pre * pre) * 0.3989422804014327
        gelu = (pre * cdf).astype(BF)
        branch = branch + nn(gelu, wo_all[r])
        grad_pre = (nt(out_grad, wo_all[r]) * (cdf + pre * pdf)).astype(BF)
        grad_out_pieces.append(tn(gelu, out_grad).astype(BF))
        grad_in_pieces.append(tn(mlp_input, grad_pre).astype(BF))
        grad_b_in_pieces.append(jnp.sum(grad_pre.astype(F32), axis=0))
        grad_mlp_in = grad_mlp_in + nt(grad_pre, wi_all[r])
    layer_out = (hidden + (branch + b_out.astype(F32))).astype(BF)

    dy = out_grad.astype(F32)
    grad_hidden = dy + norm_back(grad_mlp_in, normal2, scale2, g2)
    grad_attn = grad_hidden.astype(BF)
    sums = [
        jnp.stack(grad_b_in_pieces),
        jnp.sum(grad_attn.astype(F32), axis=0),
        jnp.sum(grad_mlp_in * normal2, axis=0),
        jnp.sum(grad_mlp_in, axis=0),
        jnp.sum(dy, axis=0),
    ]
    grad_ctx = nt(grad_attn, w_proj_all).astype(BF)
    grad_proj = tn(ctx, grad_attn).astype(BF).reshape(PIECES, part, width)
    rows_c = chunk_rows(part, dp)

    def chunked(g):
        return jnp.pad(g, ((0, 0),) * (g.ndim - 2) + ((0, -g.shape[-2] % rows_c), (0, 0)))

    grad_own_in, ffn, qkv, small, extra = back_call(
        lens, q, kp, vp, ko, vo, grad_ctx, ctx, lse, wq_all, attn_input, prompt_input, layer_in, prompt_rows,
        small_rows(sums, 16), [chunked(g) for g in grad_in_pieces], [chunked(g) for g in grad_out_pieces],
        chunked(grad_proj), dp, part
    )
    ffn = beyond(ffn.astype(F32))
    qkv = beyond(qkv.astype(F32))
    small = beyond(small)
    per = ffn.shape[0] // 2
    hid = w_in.shape[1]
    grad_w_in = ffn[:per].reshape(-1, width)[:width]
    grad_w_out = ffn[per : 2 * per].reshape(-1, width)[:hid]
    grad_w_proj = ffn[2 * per, :part]
    grad_w_qkv = qkv[:, :part].transpose(0, 2, 1)
    grad_b_qv = small[8:10, :part]
    normal1, scale1 = normalize(rows_in)
    in_grad = grad_hidden + norm_back(grad_own_in + extra.astype(F32), normal1, scale1, g1)
    return (layer_out, in_grad, grad_w_qkv, grad_b_qv, grad_w_proj, small[1], small[10], small[11], small[2],
            small[3], grad_w_in, small[0, :hid], grad_w_out, small[4])


def solution(mesh):
    in_specs = (
        P(("dp", "tensor"), None),
        P("dp"),
        P("dp", None),
        P(None, None, "tensor"),
        P(None, "tensor"),
        P("tensor", None),
        P(),
        P(),
        P(),
        P(),
        P(),
        P(None, "tensor"),
        P("tensor"),
        P("tensor", None),
        P(),
        P(("dp", "tensor"), None),
    )
    out_specs = (
        P(("dp", "tensor"), None),
        P(("dp", "tensor"), None),
        P(None, None, "tensor"),
        P(None, "tensor"),
        P("tensor", None),
        P(),
        P(),
        P(),
        P(),
        P(),
        P(None, "tensor"),
        P("tensor"),
        P("tensor", None),
        P(),
    )
    return jax.shard_map(shards, mesh=mesh, in_specs=in_specs, out_specs=out_specs, check_vma=False)
```

```python
import functools

import jax
import jax.numpy as jnp
from jax import lax
from jax.experimental import pallas as pl
from jax.experimental.pallas import tpu as pltpu
from jax.sharding import PartitionSpec as P

HEAD = 64
PROMPT = 1024
CONT = 8
CLEN = 256
PIECES = 4
MESH = pl.DeviceIdType.MESH
ANY = pl.BlockSpec(memory_space=pl.ANY)

EPS = 1e-06
MASKED = -1000000000.0
BF = jnp.bfloat16
F32 = jnp.float32


def nt(a, b):
    return lax.dot_general(a, b, (((1,), (1,)), ((), ())), preferred_element_type=F32)


def nn(a, b):
    return lax.dot_general(a, b, (((1,), (0,)), ((), ())), preferred_element_type=F32)


def tn(a, b):
    return lax.dot_general(a, b, (((0,), (0,)), ((), ())), preferred_element_type=F32)


NEAR = 8


class Peers:
    def __init__(self):
        self.t = lax.axis_index("tensor")
        self.d = lax.axis_index("dp")
        self.odd = lax.rem(self.t, 2)
        self.p = lax.rem(self.d, 2)
        self.z = lax.div(lax.rem(self.d, NEAR), 2)
        self.base = self.d - lax.rem(self.d, NEAR)
        self.core = {"tensor": self.t + 1 - 2 * self.odd}
        self.x = {"tensor": lax.rem(self.t + 2, 4)}
        self.y = {"dp": self.d + 1 - 2 * self.p}

    def along(self, k, count):
        return {"dp": self.base + lax.rem(self.z + k, count) * 2 + self.p}


def enter(devices):
    barrier = pltpu.get_barrier_semaphore()
    for device in devices:
        pl.semaphore_signal(barrier, inc=1, device_id=device, device_id_type=MESH)
    pl.semaphore_wait(barrier, len(devices))


def remote(src, dst, send, recv, device):
    return pltpu.make_async_remote_copy(
        src_ref=src, dst_ref=dst, send_sem=send, recv_sem=recv, device_id=device, device_id_type=MESH
    )


def beyond(value):
    size = lax.axis_size("dp")
    step = NEAR
    while step < size:
        value = value + lax.ppermute(value, "dp", [(i, i ^ step) for i in range(size)])
        step *= 2
    return value


def own_lanes(rows, h):
    lane = lax.broadcasted_iota(jnp.int32, (rows, 128), 1)
    return ((lane < 64) if h == 0 else (lane >= 64)), lane - (64 if h == 0 else 0)


def key_aug(k, h, length, base):
    rows = k.shape[0]
    own, extra = own_lanes(rows, h)
    row = lax.broadcasted_iota(jnp.int32, (rows, 128), 0) + base
    bias = jnp.where(jnp.logical_and(extra == 0, row >= length), MASKED, 0.0)
    return jnp.where(own, k.astype(F32), bias).astype(BF)


def query_aug(q, h):
    own, extra = own_lanes(q.shape[0], h)
    return jnp.where(own, q.astype(F32) * 0.125, jnp.where(extra == 0, 1.0, 0.0)).astype(BF)


def value_aug(v, h):
    own, extra = own_lanes(v.shape[0], h)
    ones = jnp.where(jnp.logical_and(extra >= 0, extra < 3), 1.0, 0.0)
    return jnp.where(own, v.astype(F32), ones).astype(BF)


def transposed(v):
    return v.astype(F32).T


def wide_keys(k, length, base):
    rows = k.shape[0]
    lane = lax.broadcasted_iota(jnp.int32, (rows, 128), 1)
    row = lax.broadcasted_iota(jnp.int32, (rows, 128), 0) + base
    bias = jnp.where(jnp.logical_and(lane == 0, row >= length), MASKED, 0.0).astype(BF)
    return jnp.concatenate([k, bias], axis=1)


def wide_values(v):
    lane = lax.broadcasted_iota(jnp.int32, v.shape, 1)
    return jnp.concatenate([v, jnp.where(lane < 3, 1.0, 0.0).astype(BF)], axis=1)


def wide_queries(q):
    lane = lax.broadcasted_iota(jnp.int32, q.shape, 1)
    qf = q.astype(F32) * 0.125
    one = jnp.where(lane == 0, 1.0, 0.0)
    heads = [jnp.where(lane < 64, qf, 0.0), jnp.where(lane < 64, 0.0, qf)]
    return jnp.concatenate([jnp.concatenate([h, one], axis=1) for h in heads], axis=0).astype(BF)


def wide_grads(do, ctx):
    lane = lax.broadcasted_iota(jnp.int32, do.shape, 1)
    do = do.astype(F32)
    prod = do * ctx.astype(F32)
    out = []
    for h in range(2):
        mine = (lane < 64) if h == 0 else (lane >= 64)
        d = -jnp.sum(jnp.where(mine, prod, 0.0), axis=1, keepdims=True)
        hi = d.astype(BF).astype(F32)
        mid = (d - hi).astype(BF).astype(F32)
        low = d - hi - mid
        aug = jnp.where(lane == 0, hi, jnp.where(lane == 1, mid, jnp.where(lane == 2, low, 0.0)))
        out.append(jnp.concatenate([jnp.where(mine, do, 0.0), aug], axis=1))
    return jnp.concatenate(out, axis=0).astype(BF)


def attn_specs(rows, prompt, blocks):
    def col(n):
        return pl.BlockSpec((n, 128), lambda i, l: (0, i))

    logs = pl.BlockSpec((1, blocks, 8, CLEN), lambda i, l: (i, 0, 0, 0))
    return col(rows), col(prompt), logs


class Weight:
    def __init__(self, me, own, spots, view, sems):
        self.me, self.own, self.spots, self.view = me, own, spots, view
        self.send, self.recv = sems

    def side(self):
        return remote(self.own, self.spots(1), self.send.at[0], self.recv.at[0], self.me.core)

    def across(self):
        p = self.me.p
        return remote(self.view(None, p), self.view(2, p), self.send.at[1], self.recv.at[1], self.me.x)

    def pair(self):
        p = self.me.p
        return remote(self.view(2, p), self.view(2, p), self.send.at[2], self.recv.at[2], self.me.y)

    def over(self, which):
        h = self.me.p if which == 0 else 1 - self.me.p
        return remote(self.view(2, h), self.view(3, h), self.send.at[3 + which], self.recv.at[3 + which], self.me.core)

    def start(self):
        self.side().start()
        self.across().start()

    def relay(self):
        self.across().wait_recv()
        self.pair().start()
        self.over(0).start()

    def relay_pair(self):
        self.pair().wait_recv()
        self.over(1).start()

    def finish(self):
        self.side().wait()
        self.across().wait_send()
        self.pair().wait_send()
        self.over(0).wait()
        self.over(1).wait()


def norm_rows(x, gain, shift):
    x = x.astype(F32)
    centred = x - jnp.mean(x, axis=-1, keepdims=True)
    scale = lax.rsqrt(jnp.mean(centred * centred, axis=-1, keepdims=True) + EPS)
    return (centred * scale * gain + shift).astype(BF)


def front_kernel(lens, x_ref, gain_ref, shift_ref, wq, wp, wi, wo, ws,
                 q_ref, kp_ref, vp_ref, ko_ref, vo_ref, ctx_ref, lse_ref, an_ref, anp_ref, px_ref,
                 wq_all, wp_all, wi_all, wo_all, ws_all,
                 px, wv, wsv, kph, vpt, px_s, px_r, send, recv, loc):
    me = Peers()
    step = pl.program_id(0)
    rows = x_ref.shape[0]
    blocks = rows // CLEN
    prompt = px.shape[0]
    part = wq.shape[1]
    own_chunks = rows // CLEN
    chunks = prompt // CLEN

    def qkv_view(r, h):
        n = part // 2
        if r is None:
            return wq.at[:, pl.ds(h * n, n)]
        return wv.at[:, pl.ds(r * part + h * n, n)]

    def plain(own, everything):
        n = own.shape[0] // 2

        def view(r, h):
            return own.at[pl.ds(h * n, n)] if r is None else everything.at[r, pl.ds(h * n, n)]

        return view

    def weight(i, own, everything):
        return Weight(me, own, lambda r: everything.at[r], plain(own, everything), (send.at[i], recv.at[i]))

    w_qkv = Weight(me, wq, lambda r: wv.at[:, pl.ds(r * part, part)], qkv_view, (send.at[0], recv.at[0]))
    w_small = weight(1, ws, wsv)
    w_proj = weight(2, wp, wp_all)
    w_in = weight(3, wi, wi_all)
    w_out = weight(4, wo, wo_all)
    later = [w_proj, w_in, w_out]

    def keep(own, spot, i):
        return pltpu.make_async_copy(own, spot, loc.at[i])

    mine = [
        keep(wq, wv.at[:, pl.ds(0, part)], 0), keep(ws, wsv.at[0], 1), keep(wp, wp_all.at[0], 2),
        keep(wi, wi_all.at[0], 3), keep(wo, wo_all.at[0], 4), keep(wv, wq_all, 5), keep(wsv, ws_all, 6), keep(px, px_ref, 7),
    ]

    def chunk(k):
        return px.at[pl.ds(k * CLEN, CLEN)]

    def held(k):
        at = k if k < own_chunks else k - own_chunks
        return x_ref.at[pl.ds(at * CLEN, CLEN)]

    def hop(k, src, n, device):
        return remote(src, chunk(k), px_s.at[n, k], px_r.at[n, k], device)

    first = [k for k in range(chunks) if k < own_chunks]
    second = [k for k in range(chunks) if k >= own_chunks]
    low = [k for k in range(chunks) if k < chunks // 2]
    high = second + [k for k in range(chunks // 2, own_chunks)]

    def normed(k):
        anp_ref[k * CLEN : (k + 1) * CLEN, :] = norm_rows(px[k * CLEN : (k + 1) * CLEN, :], gain_ref[...], shift_ref[...])

    @pl.when(step == 0)
    def _():
        enter([me.core, me.x, me.y])

        @pl.when(me.t == 0)
        def _():
            for k in low:
                hop(k, held(k), 1, me.x).start()
            for k in reversed(first):
                hop(k, held(k), 0, me.core).start()

        @pl.when(me.t == 1)
        def _():
            for k in second:
                hop(k, held(k), 1, me.x).start()
                hop(k, held(k), 0, me.core).start()

        for w in (w_qkv, w_small):
            w.side().start()
        for i in range(5):
            mine[i].start()

        @pl.when(me.t == 1)
        def _():
            for k in reversed(first):
                hop(k, held(k), 0, me.core).wait_recv()
                if k in high:
                    hop(k, chunk(k), 1, me.x).start()

        for w in (w_qkv, w_small):
            w.across().start()
        for w in later:
            w.side().start()
        for b in range(blocks):
            an_ref[b * CLEN : (b + 1) * CLEN, :] = norm_rows(x_ref[b * CLEN : (b + 1) * CLEN, :], gain_ref[...], shift_ref[...])

        @pl.when(me.t == 0)
        def _():
            for k in first:
                px[k * CLEN : (k + 1) * CLEN, :] = x_ref[k * CLEN : (k + 1) * CLEN, :]
            for k in second:
                hop(k, held(k), 0, me.core).wait_recv()
            for k in first:
                hop(k, held(k), 0, me.core).wait_send()
            for k in low:
                hop(k, held(k), 1, me.x).wait_send()

        @pl.when(me.t == 1)
        def _():
            for k in second:
                px[k * CLEN : (k + 1) * CLEN, :] = held(k)[...]
                hop(k, held(k), 0, me.core).wait_send()
            for k in high:
                hop(k, chunk(k), 1, me.x).wait_send()

        @pl.when(me.t == 2)
        def _():
            for k in low:
                hop(k, chunk(k), 1, me.x).wait_recv()
                hop(k, chunk(k), 0, me.core).start()
            for k in high:
                hop(k, chunk(k), 0, me.core).wait_recv()
            for k in low:
                hop(k, chunk(k), 0, me.core).wait_send()

        @pl.when(me.t == 3)
        def _():
            for k in high:
                hop(k, chunk(k), 1, me.x).wait_recv()
                hop(k, chunk(k), 0, me.core).start()
            for k in low:
                hop(k, chunk(k), 0, me.core).wait_recv()
            for k in high:
                hop(k, chunk(k), 0, me.core).wait_send()

        for k in range(chunks):
            normed(k)
        w_small.relay()
        for w in (w_qkv, w_small):
            w.side().wait_recv()
        for i in range(2):
            mine[i].wait()

    @pl.when(step == 3)
    def _():
        for w in (w_qkv, w_small):
            w.over(0).wait_recv()
            w.over(1).wait_recv()
        mine[5].start()
        mine[6].start()
        mine[7].start()

    def moves(slot):
        def at(k, *steps):
            @pl.when(slot == k)
            def _():
                for s in steps:
                    s()

        at(2, w_qkv.relay, *[lambda w=w: w.across().start() for w in later])
        at(6, w_qkv.relay_pair, w_small.relay_pair)
        at(9, w_proj.relay)
        at(11, w_proj.relay_pair)
        at(13, w_in.relay)
        at(16, w_in.relay_pair)

    pick = pl.ds(pl.multiple_of(step * 128, 128), 128)
    w3 = jnp.concatenate([wv[0, pick], wv[1, pick], wv[2, pick]], axis=0)
    u = 2 * lax.div(step, 3)
    left = wsv[u, :16, pick].astype(F32)
    right = wsv[u + 1, :16, pick].astype(F32)
    spot = lax.broadcasted_iota(jnp.int32, left.shape, 0)

    def bias(k):
        return jnp.sum(jnp.where(spot == u + k, left, 0.0) + jnp.where(spot == u + 1 + k, right, 0.0), axis=0, keepdims=True)

    bq = bias(0)
    bv = bias(PIECES)
    for b in range(blocks):
        at = slice(b * CLEN, (b + 1) * CLEN)
        got = nt(an_ref[at, :], w3)
        q_ref[at, :] = (got[:, :128] + bq).astype(BF)
        ko_ref[at, :] = got[:, 128:256].astype(BF)
        vo_ref[at, :] = (got[:, 256:] + bv).astype(BF)
    for c in range(chunks):
        at = slice(c * CLEN, (c + 1) * CLEN)
        got = nt(anp_ref[at, :], w3[128:])
        kp_ref[at, :] = got[:, :128].astype(BF)
        vp_ref[at, :] = (got[:, 128:] + bv).astype(BF)

    kph[...] = wide_keys(kp_ref[...], lens[0], 0)
    ones = jnp.ones((16, prompt), BF)
    vpt[...] = jnp.concatenate([transposed(vp_ref[...]).astype(BF), ones], axis=0)

    def block(b, _):
        moves(step * blocks + b)
        at = pl.ds(pl.multiple_of(b * CLEN, CLEN), CLEN)
        q2 = wide_queries(q_ref[at, :])
        vot = jnp.concatenate([transposed(vo_ref[at, :]).astype(BF), ones[:, :CLEN]], axis=0)
        sp = nt(kph[...], q2)
        so = nt(wide_keys(ko_ref[at, :], lens[1 + b], 0), q2)
        top = jnp.maximum(jnp.max(sp, axis=0, keepdims=True), jnp.max(so, axis=0, keepdims=True))
        pp = jnp.exp(sp - top).astype(BF)
        po = jnp.exp(so - top).astype(BF)
        ot = nn(vpt[...], pp) + nn(vot, po)
        total = ot[128:129]
        ot = ot[:128] * (1.0 / total)
        logs = top + jnp.log(total)
        ctx_ref[at, :] = jnp.concatenate([ot[:64, :CLEN], ot[64:, CLEN:]], axis=0).T.astype(BF)
        lse_ref[0, b] = jnp.concatenate([logs[:, :CLEN], logs[:, CLEN:], jnp.zeros((6, CLEN), F32)], axis=0)
        return 0

    lax.fori_loop(0, blocks, block, 0)

    @pl.when(step == pl.num_programs(0) - 1)
    def _():
        w_out.relay()
        w_out.relay_pair()
        for w in [w_qkv, w_small]:
            w.side().wait_send()
            w.across().wait_send()
            w.pair().wait_send()
            w.over(0).wait_send()
            w.over(1).wait_send()
        for w in later:
            w.finish()
        for i in range(2, 8):
            mine[i].wait()


def front_call(lens, x, gain, shift, wq, wp, wi, wo, ws):
    rows, width = x.shape
    blocks = rows // CLEN
    pairs = width // 128
    r, p, logs = attn_specs(rows, PROMPT, blocks)
    cells = rows * (PROMPT + CLEN) * pairs * 2

    def whole(n):
        return pl.BlockSpec((n, width), lambda i, l: (0, 0))

    def shape(*s):
        return jax.ShapeDtypeStruct(s, BF)

    part = wq.shape[1]
    return pl.pallas_call(
        front_kernel,
        out_shape=(
            shape(rows, width), shape(PROMPT, width), shape(PROMPT, width), shape(rows, width), shape(rows, width),
            shape(rows, width), jax.ShapeDtypeStruct((pairs, blocks, 8, CLEN), F32),
            shape(rows, width), shape(PROMPT, width), shape(PROMPT, width),
            shape(3, PIECES * part, width), shape(PIECES, *wp.shape), shape(PIECES, *wi.shape),
            shape(PIECES, *wo.shape), shape(PIECES, *ws.shape),
        ),
        grid_spec=pltpu.PrefetchScalarGridSpec(
            num_scalar_prefetch=1,
            grid=(pairs,),
            in_specs=[whole(rows), whole(1), whole(1), ANY, ANY, ANY, ANY, ANY],
            out_specs=[r, p, p, r, r, r, logs, whole(rows), whole(PROMPT), ANY, ANY, ANY, ANY, ANY, ANY],
            scratch_shapes=[
                pltpu.VMEM((PROMPT, width), BF),
                pltpu.VMEM((3, PIECES * part, width), BF),
                pltpu.VMEM((PIECES,) + ws.shape, BF),
                pltpu.VMEM((PROMPT, 256), BF),
                pltpu.VMEM((144, PROMPT), BF),
                pltpu.SemaphoreType.DMA((2, PROMPT // CLEN)),
                pltpu.SemaphoreType.DMA((2, PROMPT // CLEN)),
                pltpu.SemaphoreType.DMA((5, 5)),
                pltpu.SemaphoreType.DMA((5, 5)),
                pltpu.SemaphoreType.DMA((8,)),
            ],
        ),
        compiler_params=pltpu.CompilerParams(collective_id=0, has_side_effects=True, vmem_limit_bytes=48 << 20),
        cost_estimate=pl.CostEstimate(flops=cells * 256 * 4, transcendentals=cells, bytes_accessed=4 << 20),
        name="front",
    )(lens, x, gain, shift, wq, wp, wi, wo, ws)


STAGES = 7


def chunk_rows(rows, dp):
    unit = 16 * (min(dp, NEAR) // 2)
    return -(-rows // unit) * unit


class Sums:
    def __init__(self, me, half, held, scratch):
        self.me, self.half, self.held = me, half, held
        (self.r1, self.r3, self.xr, self.yr, self.zr, self.own,
         self.core_s, self.core_r, self.xs, self.ys, self.zs, self.zrs, self.fs, self.frs, self.gs) = scratch
        self.chunks, self.rows, self.width = self.r1.shape
        self.wide = self.width // 2
        self.share = self.rows // half
        self.mine = pl.ds(pl.multiple_of(me.p * self.wide, 128), self.wide)
        self.other = pl.ds(pl.multiple_of((1 - me.p) * self.wide, 128), self.wide)

    @staticmethod
    def scratch(chunks, rows, width, half):
        def buf(*s, dtype=BF):
            return pltpu.VMEM((chunks,) + s, dtype)

        def dma(n):
            return pltpu.SemaphoreType.DMA((chunks, n))

        wide = width // 2
        return [
            buf(rows, width), buf(rows, width), buf(rows, width), buf(rows, wide),
            buf(half, rows // half, wide), buf(rows // half, wide, dtype=F32),
            dma(2), dma(2), dma(2), dma(2), dma(half), dma(half), dma(half), dma(half), dma(2),
        ]

    def from_core(self, c, i, src=None):
        into = (self.r1, self.r3)[i].at[c]
        return remote(into if src is None else src, into, self.core_s.at[c, i], self.core_r.at[c, i], self.me.core)

    def across(self, c):
        return remote(self.held(c, 2), self.xr.at[c], self.xs.at[c, 0], self.xs.at[c, 1], self.me.x)

    def pair(self, c):
        return remote(self.held(c, 0).at[:, self.other], self.yr.at[c], self.ys.at[c, 0], self.ys.at[c, 1], self.me.y)

    def rows_of(self, k):
        at = lax.rem(self.me.z + k, self.half) * self.share
        return pl.ds(pl.multiple_of(at, 16), self.share)

    def rest(self, c, k):
        return remote(self.held(c, 0).at[self.rows_of(k), self.mine], self.zr.at[c, k],
                      self.zs.at[c, k], self.zrs.at[c, k], self.me.along(k, self.half))

    def back(self, c, k):
        spot = self.xr.at[c, self.rows_of(0), self.mine]
        return remote(spot, spot, self.fs.at[c, k], self.frs.at[c, k], self.me.along(k, self.half))

    def back_pair(self, c):
        spot = self.xr.at[c, :, self.mine]
        return remote(spot, spot, self.gs.at[c, 0], self.gs.at[c, 1], self.me.y)

    def start(self, c, i, src):
        self.from_core(c, i, src).start()

    def blocks(self, body):
        def one(k, _):
            body(pl.ds(pl.multiple_of(k * self.share, 16), self.share))
            return 0

        lax.fori_loop(0, self.half, one, 0)

    def to_chip(self, c):
        self.from_core(c, 1).wait_recv()
        g2 = self.held(c, 2)

        def body(s):
            g2[s, :] = (g2[s, :].astype(F32) + self.r3[c, s, :].astype(F32)).astype(BF)

        self.blocks(body)
        self.across(c).start()

    def term(self, c, s, lanes):
        g0 = self.held(c, 0)
        return g0[s, lanes].astype(F32) + self.r1[c, s, lanes].astype(F32) + self.xr[c, s, lanes].astype(F32)

    def to_pair(self, c):
        self.from_core(c, 0).wait()
        self.across(c).wait()
        g0 = self.held(c, 0)

        def body(s):
            g0[s, self.other] = self.term(c, s, self.other).astype(BF)

        self.blocks(body)
        self.pair(c).start()

    def to_rest(self, c):
        self.pair(c).wait()
        g0 = self.held(c, 0)
        at = self.rows_of(0)
        self.own[c] = self.term(c, at, self.mine) + self.yr[c, at, :].astype(F32)

        def body(s):
            g0[s, self.mine] = (self.term(c, s, self.mine) + self.yr[c, s, :].astype(F32)).astype(BF)

        self.blocks(body)
        for k in range(1, self.half):
            self.rest(c, k).start()

    def to_back(self, c):
        total = self.own[c]
        for k in range(1, self.half):
            self.rest(c, k).wait()
            total = total + self.zr[c, k].astype(F32)
        self.xr[c, self.rows_of(0), self.mine] = total.astype(BF)
        for k in range(1, self.half):
            self.back(c, k).start()

    def to_back_pair(self, c):
        for k in range(1, self.half):
            self.back(c, k).wait()
        self.back_pair(c).start()

    def finish(self, c):
        self.back_pair(c).wait()

    def progress(self, plan, slot):
        steps = [None, self.to_chip, self.to_pair, self.to_rest, self.to_back, self.to_back_pair]
        for k in plan["order"]:
            since = slot - plan[k]
            c = lax.div(since, plan["gap"])
            due = since >= 0
            if plan["gap"] > 1:
                due = jnp.logical_and(due, lax.rem(since, plan["gap"]) == 0)

            @pl.when(jnp.logical_and(due, c < self.chunks))
            def _():
                steps[k](c)

    def finish_all(self):
        for c in range(self.chunks):
            self.finish(c)


class SmallSum:
    def __init__(self, me, half, sm, scratch):
        self.me, self.half, self.sm = me, half, sm
        self.got, self.z, self.s, self.r = scratch

    @staticmethod
    def scratch(rows, width, half):
        return [
            pltpu.VMEM((4, rows, width), F32),
            pltpu.VMEM((half, rows, width), F32),
            pltpu.SemaphoreType.DMA((4 + half,)),
            pltpu.SemaphoreType.DMA((4 + half,)),
        ]

    def copy(self, i):
        src, device = [(1, self.me.core), (3, self.me.core), (2, self.me.x), (0, self.me.y)][i]
        return remote(self.sm.at[src], self.got.at[i], self.s.at[i], self.r.at[i], device)

    def rest(self, k):
        return remote(self.sm.at[0], self.z.at[k], self.s.at[4 + k], self.r.at[4 + k], self.me.along(k, self.half))

    def start(self):
        self.copy(1).start()
        self.copy(0).start()

    def to_chip(self):
        self.copy(1).wait()
        self.sm[2] = self.sm[2] + self.got[1]
        self.copy(2).start()

    def to_pair(self):
        self.copy(0).wait()
        self.copy(2).wait()
        self.sm[0] = self.sm[0] + self.got[0] + self.got[2]
        self.copy(3).start()

    def to_rest(self):
        self.copy(3).wait()
        self.sm[0] = self.sm[0] + self.got[3]
        for k in range(1, self.half):
            self.rest(k).start()

    def finish(self):
        total = self.sm[0]
        for k in range(1, self.half):
            self.rest(k).wait()
            total = total + self.z[k]
        return total


SUB = 3
FFN_PLAN = {"gap": 2, "order": (5, 4, 3, 2, 1), 1: 6, 2: 12, 3: 14, 4: 16, 5: 18}
QKV_PLAN = {"gap": 2, "order": (5, 4, 3, 2, 1), 1: 24, 2: 30, 3: 32, 4: 34, 5: 36}
QKV_START = (21, 30)
SMALL_PLAN = (31, 33, 35, 37, 39)
PROMPT_PLAN = (33, 42)
LAST_SLOT = 43


def back_kernel(half, grid_pairs, lens, q_ref, kp_ref, vp_ref, ko_ref, vo_ref, lse_ref,
                w_any, an_any, anp_any, x_ref, px_any, ctx_ref, wp_any, wi_ref, wo_ref, bias_ref, vec_ref, dy_any,
                lo_any, ig_any, ffn_out, qkv_out, small_out,
                w_ref, an_ref, anp_ref, l_s, dy, hid, gs, g0, g2,
                kx, vx, kt_s, acc, dqt, dkt, dvt, prompt_acc, own_acc, share_s, gq, sm, qv, sums,
                came, over, tail, p_s, p_r, o_s, *scratch):
    me = Peers()
    step = pl.program_id(0)
    rows = x_ref.shape[0]
    width = an_ref.shape[1]
    blocks = rows // CLEN
    prompt = kp_ref.shape[0]
    chunks = prompt // CLEN
    part = width // PIECES
    feats = grid_pairs // 2 * 128
    per = width // part
    ffn_scratch, qkv_scratch, small_scratch = scratch[:15], scratch[15:30], scratch[30:]
    branch, gmi, gel, gp, mlp, mlpt = prompt_acc, own_acc, gq.at[0], gq.at[1], gq.at[2], share_s.at[pl.ds(0, width)]
    loads = [pltpu.make_async_copy(a, b, l_s.at[i]) for i, (a, b) in enumerate(((an_any, an_ref), (anp_any, anp_ref)))]

    def load_w(unit):
        return pltpu.make_async_copy(w_any.at[:, pl.ds(unit * feats, feats)], w_ref, l_s.at[2])

    px_parts = [(at, min(part, prompt - at)) for at in range(0, prompt, part)]
    load_px = [
        pltpu.make_async_copy(px_any.at[pl.ds(at, m)], gs.at[i, pl.ds(0, m)], l_s.at[3 + i]) for i, (at, m) in enumerate(px_parts)
    ]
    g1, c1, b_proj, ln2_g, ln2_b, b_out = (vec_ref[k : k + 1, :] for k in range(6))

    def piece_rows(r):
        return pl.ds(pl.multiple_of(r * part, 16), part)

    ffn = Sums(me, half, lambda c, r: (g0 if r == 0 else g2).at[c], ffn_scratch)
    qkv = Sums(me, half, lambda c, r: gq.at[c, piece_rows(r)], qkv_scratch)
    smalls = SmallSum(me, half, sm, small_scratch)
    n = prompt // 2
    spare = rows - n
    mine = pl.ds(pl.multiple_of(me.odd * n, 16), n)
    side = remote(share_s.at[pl.ds(pl.multiple_of((1 - me.odd) * n, 16), n)], came, p_s.at[0], p_r.at[0], me.core)
    across = remote(share_s.at[mine], over, p_s.at[1], p_r.at[1], me.x)
    end = remote(share_s.at[pl.ds(pl.multiple_of(me.odd * n, 16), spare)], tail, p_s.at[2], p_r.at[2], me.core)

    def block_rows(b):
        return slice(b * CLEN, (b + 1) * CLEN)

    def normal_of(x):
        x = x - jnp.mean(x, axis=-1, keepdims=True)
        scale = lax.rsqrt(jnp.mean(x * x, axis=-1, keepdims=True) + EPS)
        return x * scale, scale

    def norm_back(e, normal, scale):
        return scale * (e - jnp.mean(e, axis=-1, keepdims=True) - normal * jnp.mean(e * normal, axis=-1, keepdims=True))

    @pl.when(step == 0)
    def _():
        got = pltpu.make_async_copy(dy_any, dy, o_s.at[0])
        wp = pltpu.make_async_copy(wp_any, w_ref.at[pl.ds(0, 2)], l_s.at[2])
        wp.start()
        got.start()
        enter([me.core, me.x, me.y] + [me.along(k, half) for k in range(1, half)])
        wp.wait()
        for b in range(blocks):
            at = block_rows(b)
            h = x_ref[at, :].astype(F32) + nn(ctx_ref[at, :], w_ref[:2].reshape(width, width)) + b_proj
            hid[at, :] = h
            normal, _ = normal_of(h)
            m = (normal * ln2_g + ln2_b).astype(BF)
            mlp[at, :] = m
            mlpt[:, at] = transposed(m).astype(BF)
        got.wait()
        for c in loads:
            c.start()
        branch[...] = jnp.zeros_like(branch)
        gmi[...] = jnp.zeros_like(gmi)
        sums[...] = jnp.zeros_like(sums)

    def ffn_block(b):
        at = pl.ds(pl.multiple_of(b * CLEN, CLEN), CLEN)
        r = PIECES - 1 - step
        wi = wi_ref[0]
        wo = wo_ref[0]
        pre = nn(mlp[at, :], wi) + bias_ref[r, 16:17, :].astype(F32)
        cdf = 0.5 * (1.0 + lax.erf(pre * (0.5**0.5)))
        pdf = jnp.exp(-0.5 * pre * pre) * 0.3989422804014327
        g = (pre * cdf).astype(BF)
        d = (nt(dy[at, :], wo) * (cdf + pre * pdf)).astype(BF)
        gel[at, :] = g
        gp[at, :] = d
        branch[at, :] += nn(g, wo)
        gmi[at, :] += nt(d, wi)
        sums[pl.ds(r, 1), :] += jnp.sum(d.astype(F32), axis=0, keepdims=True)

    def weight_grads():
        @pl.when(step == 2)
        def _():
            for c in range(2 * per):
                ffn.from_core(c, 1, gs.at[c]).wait_send()

        def one(j, _):
            two = pl.ds(pl.multiple_of(j * 2 * part, 128), 2 * part)
            both = (nn(mlpt[two, :], gp[...]), tn(gel[:, two], dy[...]))
            for k, got in enumerate(both):
                got = got.astype(BF).reshape(2, part, width)
                spot = pl.ds(2 * j + k * per, 2)

                @pl.when(lax.rem(step, 2) == 0)
                def _():
                    gs[spot] = got

                @pl.when(step == 1)
                def _():
                    g2[spot] = got

                @pl.when(step == 3)
                def _():
                    g0[spot] = got

            return 0

        lax.fori_loop(0, per // 2, one, 0)
        for at, i in ((0, 1), (2, 0)):
            @pl.when(step == at)
            def _():
                for c in range(2 * per):
                    ffn.start(c, i, gs.at[c])

    def after_ffn():
        for b in range(blocks):
            at = block_rows(b)
            g = gmi[at, :]
            h = hid[at, :]
            d = dy[at, :].astype(F32)
            normal, scale = normal_of(h)
            mlp[at, :] = (h + (branch[at, :] + b_out)).astype(BF)
            gh = d + norm_back(g * ln2_g, normal, scale)
            hid[at, :] = gh
            ga = gh.astype(BF)
            gel[at, :] = ga
            for k, v in enumerate((ga.astype(F32), g * normal, g, d)):
                sums[PIECES + k : PIECES + k + 1, :] += jnp.sum(v, axis=0, keepdims=True)
            dy[at, :] = nt(ga, w_ref[:2].reshape(width, width)).astype(BF)
        load_w(1).start()
        spots = (g0.at[2 * per], gs.at[2 * per + 1], g2.at[2 * per], gs.at[2 * per])
        for r in range(0, PIECES, 2):
            got = tn(ctx_ref[:, r * part : (r + 2) * part], gel[...]).astype(BF)
            spots[r][...] = got[:part]
            spots[r + 1][...] = got[part:]
        ffn.start(2 * per, 1, gs.at[2 * per])
        ffn.start(2 * per, 0, gs.at[2 * per + 1])
        pltpu.make_async_copy(mlp, lo_any, o_s.at[1]).start()
        own_acc[...] = jnp.zeros_like(own_acc)
        prompt_acc[...] = jnp.zeros_like(prompt_acc)

    sp = step - PIECES
    spot = lax.rem(jnp.maximum(sp, 0), grid_pairs // 2)
    pair = lax.rem(jnp.maximum(sp, 0) + grid_pairs // 2, grid_pairs)
    lanes = pl.ds(pl.multiple_of(pair * 128, 128), 128)
    attending = jnp.logical_and(sp >= 0, sp < grid_pairs)

    @pl.when(attending)
    def _():
        acc[...] = jnp.zeros_like(acc)
        kx[:prompt] = wide_keys(kp_ref[...], lens[0], 0)
        vx[:prompt] = wide_values(vp_ref[...])
        vx[prompt:] = wide_values(vo_ref[...])
        kt_s[:, :prompt] = transposed(kp_ref[...]).astype(BF)
        kt_s[:, prompt:] = transposed(ko_ref[...]).astype(BF)
        for b in range(blocks):
            at = block_rows(b)
            kx[prompt + b * CLEN : prompt + (b + 1) * CLEN] = wide_keys(ko_ref[at, :], lens[1 + b], 0)

    def block(b):
        at = pl.ds(pl.multiple_of(b * CLEN, CLEN), CLEN)
        own = pl.ds(pl.multiple_of(prompt + b * CLEN, CLEN), CLEN)
        q = q_ref[at, :]
        do = dy[at, lanes]
        q2 = wide_queries(q)
        do2 = wide_grads(do, ctx_ref[at, lanes])
        qt = transposed(q).astype(BF)
        dot = transposed(do).astype(BF)
        logs = jnp.concatenate([lse_ref[0, b, 0:1, :], lse_ref[0, b, 1:2, :]], axis=1)

        def scores(keys):
            p = jnp.exp(nt(kx[keys, :], q2) - logs)
            ds = (p * nt(vx[keys, :], do2)).astype(BF)
            p = p.astype(BF)
            parts = []
            for left, m in ((qt, ds), (dot, p)):
                parts.append([nt(left[64 * h : 64 * h + 64], m[:, h * CLEN : (h + 1) * CLEN]) for h in range(2)])
            return parts, nn(kt_s[:, keys], ds)

        (dk, dv), dq = scores(pl.ds(0, prompt))
        for h in range(2):
            rows_h = slice(64 * h, 64 * h + 64)
            acc[0, rows_h, :] += dk[h]
            acc[1, rows_h, :] += dv[h]
        (dk, dv), dq_own = scores(own)
        dkt[spot, :, own] = (jnp.concatenate(dk, axis=0) * 0.125).astype(BF)
        dvt[spot, :, own] = jnp.concatenate(dv, axis=0).astype(BF)
        dq = dq + dq_own
        dqt[spot, :, at] = (jnp.concatenate([dq[:64, :CLEN], dq[64:, CLEN:]], axis=0) * 0.125).astype(BF)

        @pl.when(b == blocks - 1)
        def _():
            dkt[spot, :, :prompt] = (acc[0] * 0.125).astype(BF)
            dvt[spot, :, :prompt] = acc[1].astype(BF)

    def sub_step(sub, _):
        slot = step * SUB + sub
        ffn.progress(FFN_PLAN, slot)

        def at(k, body):
            @pl.when(slot == k)
            def _():
                body()

        def qkv_start(i):
            for c in range(3):
                qkv.start(c, i, gq.at[c, piece_rows(1 + 2 * i)])

        def prompt_chip():
            side.wait()
            share_s[mine, :] = (share_s[mine, :].astype(F32) + came[...].astype(F32)).astype(BF)

            @pl.when(me.t >= 2)
            def _():
                across.start()

        def qkv_sent():
            for c in range(3):
                qkv.from_core(c, 1, gq.at[c, piece_rows(3)]).wait_send()

        at(QKV_START[0], lambda: qkv_start(1))
        at(QKV_START[1], lambda: qkv_start(0))
        at(QKV_START[1], qkv_sent)
        qkv.progress(QKV_PLAN, slot)
        at(SMALL_PLAN[0], smalls.start)
        at(SMALL_PLAN[1], smalls.to_chip)
        at(SMALL_PLAN[2], smalls.to_pair)
        at(SMALL_PLAN[3], smalls.to_rest)
        at(PROMPT_PLAN[0], prompt_chip)

        @pl.when(step < PIECES)
        def _():
            ffn_block(sub)

        @pl.when(attending)
        def _():
            block(sub)

        return 0

    lax.fori_loop(0, SUB, sub_step, 0)

    @pl.when(step < PIECES)
    def _():
        weight_grads()

    @pl.when(step == PIECES - 1)
    def _():
        after_ffn()

    @pl.when(jnp.logical_and(attending, spot == grid_pairs // 2 - 1))
    def _():
        late = sp < grid_pairs // 2

        @pl.when(late)
        def _():
            for c in loads + [pltpu.make_async_copy(mlp, lo_any, o_s.at[1])]:
                c.wait()

        load_w(0).wait()
        dq, dk, dv = (r[...].reshape(feats, -1) for r in (dqt, dkt, dvt))
        an = an_ref[...]
        anp = anp_ref[...]
        for j, d in enumerate((dq, dk, dv)):
            g = nn(d, an) if j == 0 else nn(d[:, prompt:], an) + nn(d[:, :prompt], anp)
            gq[j, pl.ds(pl.multiple_of(jnp.where(late, feats, 0), 16), feats), :] = g.astype(BF)
        sum_q = jnp.sum(dq.astype(F32), axis=1, keepdims=True)
        sum_v = jnp.sum(dv.astype(F32), axis=1, keepdims=True)
        both = jnp.concatenate([jnp.broadcast_to(sum_q, (feats, 128)), jnp.broadcast_to(sum_v, (feats, 128))], axis=1).T
        unit_lanes = pl.ds(pl.multiple_of(jnp.where(late, feats, 0), 128), feats)
        qv[0:1, unit_lanes] = both[0:1]
        qv[1:2, unit_lanes] = both[128:129]
        def turned(ref, at, j):
            return tn(ref[:, :, at : at + CLEN].reshape(feats, CLEN), w_ref[j])

        for b in range(blocks):
            at = b * CLEN
            own_acc[at : at + CLEN, :] += (
                turned(dqt, at, 0) + turned(dkt, prompt + at, 1) + turned(dvt, prompt + at, 2)
            )
        for c in range(chunks):
            at = c * CLEN
            prompt_acc[at : at + CLEN, :] += turned(dkt, at, 1) + turned(dvt, at, 2)

        @pl.when(late)
        def _():
            load_w(0).start()

        @pl.when(jnp.logical_not(late))
        def _():
            for c in load_px:
                c.start()

    @pl.when(sp == grid_pairs - 1)
    def _():
        for c in range(chunks):
            at = block_rows(c)
            share_s[at, :] = prompt_acc[at, :].astype(BF)
        side.start()
        sum_g = jnp.zeros((1, width), F32)
        sum_c = jnp.zeros((1, width), F32)
        raws = [(own_acc, at, m, x_ref.at[pl.ds(at, m)]) for at, m in [(part * k, part) for k in range(rows // part)]]
        raws += [(prompt_acc, at, m, gs.at[i, pl.ds(0, m)]) for i, (at, m) in enumerate(px_parts)]
        for i, (grad, at, m, raw) in enumerate(raws):
            if grad is prompt_acc:
                load_px[i - rows // part].wait()
            normal, _ = normal_of(raw[...].astype(F32))
            g = grad[at : at + m, :]
            sum_g = sum_g + jnp.sum(g * normal, axis=0, keepdims=True)
            sum_c = sum_c + jnp.sum(g, axis=0, keepdims=True)
        for r in range(PIECES):
            sm[r] = jnp.zeros_like(sm[r])
            sm[r, 0:1, :] = sums[r : r + 1, :]
            sm[r, 1:5, :] = sums[PIECES : PIECES + 4, :]
            for i in range(2):
                row = qv[i : i + 1, :]
                sm[r, 8 + i : 9 + i, :] = row if r == 0 else pltpu.roll(row, width - r * part, 1)
            sm[r, 10:11, :] = sum_g
            sm[r, 11:12, :] = sum_c

    @pl.when(step == pl.num_programs(0) - 1)
    def _():
        ffn.finish_all()
        qkv.finish_all()
        outs = [(ffn.xr, ffn_out), (qkv.xr, qkv_out)]
        copies = [pltpu.make_async_copy(a, b, o_s.at[2 + i]) for i, (a, b) in enumerate(outs)]
        for c in copies:
            c.start()
        small_out[...] = smalls.finish()
        ffn.from_core(2 * per, 1, gs.at[2 * per]).wait_send()

        @pl.when(me.t >= 2)
        def _():
            across.wait_send()

        @pl.when(me.t < 2)
        def _():
            across.wait_recv()
            share_s[mine, :] = (share_s[mine, :].astype(F32) + over[...].astype(F32)).astype(BF)

        @pl.when(me.t == 1)
        def _():
            end.start()
            for at in range(0, n - spare, CLEN):
                own_acc[at : at + CLEN, :] += share_s[n + spare + at : n + spare + at + CLEN, :].astype(F32)
            end.wait_send()

        @pl.when(me.t == 0)
        def _():
            for at in range(0, n, CLEN):
                own_acc[at : at + CLEN, :] += share_s[at : at + CLEN, :].astype(F32)
            end.wait_recv()
            own_acc[n:, :] += tail[...].astype(F32)

        for b in range(blocks):
            at = block_rows(b)
            normal, scale = normal_of(x_ref[at, :].astype(F32))
            hid[at, :] += norm_back(own_acc[at, :] * g1, normal, scale)
        last = pltpu.make_async_copy(hid, ig_any, o_s.at[0])
        last.start()
        for c in copies + [last]:
            c.wait()


def back_call(lens, q, kp, vp, ko, vo, lse, wq_all, an, anp, x, px, ctx, wp, wi_all, wo_all, ws_all, vec, dy):
    rows, width = q.shape
    prompt = kp.shape[0]
    blocks = rows // CLEN
    pairs = width // 128
    part = width // PIECES
    half = min(lax.axis_size("dp"), NEAR) // 2
    cells = rows * (prompt + CLEN) * pairs * 2
    n_ffn = 2 * (width // part) + 1
    steps = -(-LAST_SLOT // SUB)
    assert blocks == SUB and wi_all.shape[1:] == (width, width) and part % (16 * half) == 0
    small_n = 16

    def pair(i):
        return lax.rem(jnp.clip(i - PIECES, 0, pairs - 1) + pairs // 2, pairs)

    def col(n):
        return pl.BlockSpec((n, 128), lambda i, l: (0, pair(i)))

    def whole(*s):
        return pl.BlockSpec(s, lambda i, l: (0,) * len(s), pipeline_mode=pl.Buffered(1))

    r, p = col(rows), col(prompt)
    logs = pl.BlockSpec((1, blocks, 8, CLEN), lambda i, l: (pair(i), 0, 0, 0))
    ff = pl.BlockSpec((1, width, width), lambda i, l: (jnp.maximum(PIECES - 1 - i, 0), 0, 0), pipeline_mode=pl.Buffered(1))
    return pl.pallas_call(
        functools.partial(back_kernel, half, pairs),
        out_shape=(
            jax.ShapeDtypeStruct((rows, width), BF),
            jax.ShapeDtypeStruct((rows, width), F32),
            jax.ShapeDtypeStruct((n_ffn, part, width), BF),
            jax.ShapeDtypeStruct((3, part, width), BF),
            jax.ShapeDtypeStruct((small_n, width), F32),
        ),
        grid_spec=pltpu.PrefetchScalarGridSpec(
            num_scalar_prefetch=1,
            grid=(steps,),
            in_specs=[r, p, p, r, r, logs, ANY, ANY, ANY, whole(rows, width),
                      ANY, whole(rows, width), ANY, ff, ff,
                      whole(*ws_all.shape), whole(*vec.shape), ANY],
            out_specs=[ANY, ANY, ANY, ANY, pl.BlockSpec((small_n, width), lambda i, l: (0, 0))],
            scratch_shapes=[
                pltpu.VMEM((3, width // 2, width), BF),
                pltpu.VMEM((rows, width), BF),
                pltpu.VMEM((prompt, width), BF),
                pltpu.SemaphoreType.DMA((3 + -(-prompt // part),)),
                pltpu.VMEM((rows, width), BF),
                pltpu.VMEM((rows, width), F32),
                pltpu.VMEM((n_ffn + 1, part, width), BF),
                pltpu.VMEM((n_ffn, part, width), BF),
                pltpu.VMEM((n_ffn, part, width), BF),
                pltpu.VMEM((prompt + rows, 256), BF),
                pltpu.VMEM((prompt + rows, 256), BF),
                pltpu.VMEM((128, prompt + rows), BF),
                pltpu.VMEM((2, 128, prompt), F32),
                pltpu.VMEM((pairs // 2, 128, rows), BF),
                pltpu.VMEM((pairs // 2, 128, prompt + rows), BF),
                pltpu.VMEM((pairs // 2, 128, prompt + rows), BF),
                pltpu.VMEM((prompt, width), F32),
                pltpu.VMEM((rows, width), F32),
                pltpu.VMEM((prompt, width), BF),
                pltpu.VMEM((3, width, width), BF),
                pltpu.VMEM((PIECES, small_n, width), F32),
                pltpu.VMEM((8, width), F32),
                pltpu.VMEM((8, width), F32),
                pltpu.VMEM((prompt // 2, width), BF),
                pltpu.VMEM((prompt // 2, width), BF),
                pltpu.VMEM((rows - prompt // 2, width), BF),
                pltpu.SemaphoreType.DMA((3,)),
                pltpu.SemaphoreType.DMA((3,)),
                pltpu.SemaphoreType.DMA((4,)),
            ]
            + Sums.scratch(n_ffn, part, width, half)
            + Sums.scratch(3, part, width, half)
            + SmallSum.scratch(small_n, width, half),
        ),
        compiler_params=pltpu.CompilerParams(collective_id=1, has_side_effects=True, vmem_limit_bytes=63 << 20),
        cost_estimate=pl.CostEstimate(flops=cells * 256 * 10, transcendentals=cells, bytes_accessed=16 << 20),
        name="back",
    )(lens, q, kp, vp, ko, vo, lse, wq_all, an, anp, x, px, ctx, wp, wi_all, wo_all, ws_all, vec, dy)


def shards(layer_in, prompt_len, cont_len, w_qkv, b_qv, w_proj, b_proj, ln1_gain, ln1_bias,
           ln2_gain, ln2_bias, w_in, b_in, w_out, b_out, out_grad):
    rows, width = layer_in.shape
    blocks = rows // CLEN
    part = w_qkv.shape[2]
    t = lax.axis_index("tensor")
    g1, c1 = (v.astype(F32)[None] for v in (ln1_gain, ln1_bias))

    group = t * blocks + jnp.arange(blocks)
    conts = group - PROMPT // CLEN
    own_len = jnp.where(conts >= 0, cont_len[0][jnp.clip(conts, 0, CONT - 1)], 0)
    lens = jnp.concatenate([prompt_len, own_len]).astype(jnp.int32)

    bias_rows = [jnp.pad(b_qv[i : i + 1], ((0, 0), (r * part, width - (r + 1) * part))) for i in range(2) for r in range(PIECES)]
    small = jnp.concatenate(bias_rows + [jnp.zeros((8, width), BF), b_in[None], jnp.zeros((15, width), BF)], axis=0)
    row = lax.broadcasted_iota(jnp.int32, (8, 1), 0)
    vec = jnp.zeros((8, width), F32)
    for k, v in enumerate((ln1_gain, ln1_bias, b_proj, ln2_gain, ln2_bias, b_out)):
        vec = jnp.where(row == k, v.astype(F32)[None], vec)
    (q, kp, vp, ko, vo, ctx, lse, attn_input, prompt_input, prompt_rows, wq_all, wp_all, wi_all, wo_all, ws_all) = front_call(
        lens, layer_in, g1, c1, w_qkv.transpose(0, 2, 1), w_proj, w_in, w_out, small
    )
    layer_out, in_grad, ffn, qkv, small = back_call(
        lens, q, kp, vp, ko, vo, lse, wq_all, attn_input, prompt_input, layer_in, prompt_rows, ctx,
        wp_all.reshape(2, width // 2, width), wi_all, wo_all, ws_all, vec, out_grad
    )
    ffn = beyond(ffn.astype(F32))
    qkv = beyond(qkv.astype(F32))
    small = beyond(small)
    per = ffn.shape[0] // 2
    grad_w_in = ffn[:per].reshape(width, -1)
    grad_w_out = ffn[per : 2 * per].reshape(-1, width)
    return (layer_out, in_grad, qkv.transpose(0, 2, 1), small[8:10, :part], ffn[2 * per], small[1], small[10], small[11],
            small[2], small[3], grad_w_in, small[0, : w_in.shape[1]], grad_w_out, small[4])


def solution(mesh):
    in_specs = (
        P(("dp", "tensor"), None),
        P("dp"),
        P("dp", None),
        P(None, None, "tensor"),
        P(None, "tensor"),
        P("tensor", None),
        P(),
        P(),
        P(),
        P(),
        P(),
        P(None, "tensor"),
        P("tensor"),
        P("tensor", None),
        P(),
        P(("dp", "tensor"), None),
    )
    out_specs = (
        P(("dp", "tensor"), None),
        P(("dp", "tensor"), None),
        P(None, None, "tensor"),
        P(None, "tensor"),
        P("tensor", None),
        P(),
        P(),
        P(),
        P(),
        P(),
        P(None, "tensor"),
        P("tensor"),
        P("tensor", None),
        P(),
    )
    return jax.shard_map(shards, mesh=mesh, in_specs=in_specs, out_specs=out_specs, check_vma=False)
```

```python
import functools

import jax
import jax.numpy as jnp
from jax import lax
from jax.experimental import pallas as pl
from jax.experimental.pallas import tpu as pltpu
from jax.sharding import PartitionSpec as P

HEAD = 64
PROMPT = 1024
CONT = 8
CLEN = 256
PIECES = 4
MESH = pl.DeviceIdType.MESH
ANY = pl.BlockSpec(memory_space=pl.ANY)

EPS = 1e-06
MASKED = -1000000000.0
BF = jnp.bfloat16
F32 = jnp.float32


def nt(a, b):
    return lax.dot_general(a, b, (((1,), (1,)), ((), ())), preferred_element_type=F32)


def nn(a, b):
    return lax.dot_general(a, b, (((1,), (0,)), ((), ())), preferred_element_type=F32)


def tn(a, b):
    return lax.dot_general(a, b, (((0,), (0,)), ((), ())), preferred_element_type=F32)


NEAR = 8


class Peers:
    def __init__(self):
        self.t = lax.axis_index("tensor")
        self.d = lax.axis_index("dp")
        self.odd = lax.rem(self.t, 2)
        self.p = lax.rem(self.d, 2)
        self.z = lax.div(lax.rem(self.d, NEAR), 2)
        self.base = self.d - lax.rem(self.d, NEAR)
        self.core = {"tensor": self.t + 1 - 2 * self.odd}
        self.x = {"tensor": lax.rem(self.t + 2, 4)}
        self.y = {"dp": self.d + 1 - 2 * self.p}

    def along(self, k, count):
        return {"dp": self.base + lax.rem(self.z + k, count) * 2 + self.p}


def enter(devices):
    barrier = pltpu.get_barrier_semaphore()
    for device in devices:
        pl.semaphore_signal(barrier, inc=1, device_id=device, device_id_type=MESH)
    pl.semaphore_wait(barrier, len(devices))


def remote(src, dst, send, recv, device):
    return pltpu.make_async_remote_copy(
        src_ref=src, dst_ref=dst, send_sem=send, recv_sem=recv, device_id=device, device_id_type=MESH
    )


def beyond(value):
    size = lax.axis_size("dp")
    step = NEAR
    while step < size:
        value = value + lax.ppermute(value, "dp", [(i, i ^ step) for i in range(size)])
        step *= 2
    return value


def own_lanes(rows, h):
    lane = lax.broadcasted_iota(jnp.int32, (rows, 128), 1)
    return ((lane < 64) if h == 0 else (lane >= 64)), lane - (64 if h == 0 else 0)


def key_aug(k, h, length, base):
    rows = k.shape[0]
    own, extra = own_lanes(rows, h)
    row = lax.broadcasted_iota(jnp.int32, (rows, 128), 0) + base
    bias = jnp.where(jnp.logical_and(extra == 0, row >= length), MASKED, 0.0)
    return jnp.where(own, k.astype(F32), bias).astype(BF)


def query_aug(q, h):
    own, extra = own_lanes(q.shape[0], h)
    return jnp.where(own, q.astype(F32) * 0.125, jnp.where(extra == 0, 1.0, 0.0)).astype(BF)


def value_aug(v, h):
    own, extra = own_lanes(v.shape[0], h)
    ones = jnp.where(jnp.logical_and(extra >= 0, extra < 3), 1.0, 0.0)
    return jnp.where(own, v.astype(F32), ones).astype(BF)


def transposed(v):
    return v.astype(F32).T


def wide_keys(k, length, base):
    rows = k.shape[0]
    lane = lax.broadcasted_iota(jnp.int32, (rows, 128), 1)
    row = lax.broadcasted_iota(jnp.int32, (rows, 128), 0) + base
    bias = jnp.where(jnp.logical_and(lane == 0, row >= length), MASKED, 0.0).astype(BF)
    return jnp.concatenate([k, bias], axis=1)


def wide_values(v):
    lane = lax.broadcasted_iota(jnp.int32, v.shape, 1)
    return jnp.concatenate([v, jnp.where(lane < 3, 1.0, 0.0).astype(BF)], axis=1)


def wide_queries(q):
    lane = lax.broadcasted_iota(jnp.int32, q.shape, 1)
    qf = q.astype(F32) * 0.125
    one = jnp.where(lane == 0, 1.0, 0.0)
    heads = [jnp.where(lane < 64, qf, 0.0), jnp.where(lane < 64, 0.0, qf)]
    return jnp.concatenate([jnp.concatenate([h, one], axis=1) for h in heads], axis=0).astype(BF)


def wide_grads(do, ctx):
    lane = lax.broadcasted_iota(jnp.int32, do.shape, 1)
    do = do.astype(F32)
    prod = do * ctx.astype(F32)
    out = []
    for h in range(2):
        mine = (lane < 64) if h == 0 else (lane >= 64)
        d = -jnp.sum(jnp.where(mine, prod, 0.0), axis=1, keepdims=True)
        hi = d.astype(BF).astype(F32)
        mid = (d - hi).astype(BF).astype(F32)
        low = d - hi - mid
        aug = jnp.where(lane == 0, hi, jnp.where(lane == 1, mid, jnp.where(lane == 2, low, 0.0)))
        out.append(jnp.concatenate([jnp.where(mine, do, 0.0), aug], axis=1))
    return jnp.concatenate(out, axis=0).astype(BF)


def attn_specs(rows, prompt, blocks):
    def col(n):
        return pl.BlockSpec((n, 128), lambda i, *l: (0, i))

    logs = pl.BlockSpec((1, blocks, 8, CLEN), lambda i, *l: (i, 0, 0, 0))
    return col(rows), col(prompt), logs

def own_length(conts, t, blocks, b):
    c = t * blocks + b - PROMPT // CLEN
    return jnp.where(c >= 0, conts[0, jnp.maximum(c, 0)], 0)


class Weight:
    def __init__(self, me, own, spots, view, sems, direct=False):
        self.me, self.own, self.spots, self.view, self.direct = me, own, spots, view, direct
        self.send, self.recv = sems

    def side(self):
        return remote(self.own, self.spots(1), self.send.at[0], self.recv.at[0], self.me.core)

    def across(self):
        p = self.me.p
        src, dst = (self.own, self.spots(2)) if self.direct else (self.view(None, p), self.view(2, p))
        return remote(src, dst, self.send.at[1], self.recv.at[1], self.me.x)

    def pair(self):
        p = self.me.p
        return remote(self.view(2, p), self.view(2, p), self.send.at[2], self.recv.at[2], self.me.y)

    def over(self, which):
        h = self.me.p if which == 0 else 1 - self.me.p
        src, dst = (self.spots(2), self.spots(3)) if self.direct else (self.view(2, h), self.view(3, h))
        return remote(src, dst, self.send.at[3 + which], self.recv.at[3 + which], self.me.core)

    def start(self):
        self.side().start()
        self.across().start()

    def relay(self):
        self.across().wait_recv()
        if not self.direct:
            self.pair().start()
        self.over(0).start()

    def relay_pair(self):
        self.pair().wait_recv()
        self.over(1).start()

    def finish(self):
        self.side().wait()
        self.across().wait_send()
        self.over(0).wait()
        if not self.direct:
            self.pair().wait_send()
            self.over(1).wait()


def norm_rows(x, gain, shift):
    x = x.astype(F32)
    centred = x - jnp.mean(x, axis=-1, keepdims=True)
    scale = lax.rsqrt(jnp.mean(centred * centred, axis=-1, keepdims=True) + EPS)
    return (centred * scale * gain + shift).astype(BF)


def flat(ref):
    return ref[...].astype(F32).reshape(1, ref.shape[0])


def front_kernel(plen, conts, x_ref, gain_ref, shift_ref, bqv_ref, bin_ref, wq, wp, wi, wo,
                 q_ref, kp_ref, vp_ref, ko_ref, vo_ref, ctx_ref, lse_ref, an_ref, anp_ref, px_ref,
                 wq_all, wp_all, wi_all, wo_all, ws_all,
                 px, wv, wsv, kph, vpt, px_s, px_r, send, recv, loc):
    me = Peers()
    step = pl.program_id(0)
    rows = x_ref.shape[0]
    blocks = rows // CLEN
    prompt = px.shape[0]
    part = wq.shape[1]
    own_chunks = rows // CLEN
    chunks = prompt // CLEN

    def qkv_view(r, h):
        n = part // 2
        if r is None:
            return wq.at[:, pl.ds(h * n, n)]
        return wv.at[:, pl.ds(r * part + h * n, n)]

    def plain(own, everything):
        n = own.shape[0] // 2

        def view(r, h):
            return own.at[pl.ds(h * n, n)] if r is None else everything.at[r, pl.ds(h * n, n)]

        return view

    def weight(i, own, everything):
        return Weight(me, own, lambda r: everything.at[r], plain(own, everything), (send.at[i], recv.at[i]))

    w_qkv = Weight(me, wq, lambda r: wv.at[:, pl.ds(r * part, part)], qkv_view, (send.at[0], recv.at[0]))
    w_small = weight(1, wsv.at[0], wsv)
    w_proj = weight(2, wp, wp_all)
    half_in = wi.shape[0] // 2
    half_out = wo.shape[0] // 2

    def rows_of(i, own, everything, first, n, direct=False):
        part_rows = pl.ds(first, n)
        sub = n // 2

        def view(r, h):
            at = pl.ds(first + h * sub, sub)
            return own.at[at] if r is None else everything.at[r, at]

        return Weight(me, own.at[part_rows], lambda r: everything.at[r, part_rows], view, (send.at[i], recv.at[i]), direct)

    in_a = rows_of(3, wi, wi_all, 0, half_in)
    in_b = rows_of(4, wi, wi_all, half_in, half_in)
    out_a = rows_of(5, wo, wo_all, 0, half_out)
    out_b = rows_of(6, wo, wo_all, half_out, half_out, True)
    later = [w_proj, in_a, in_b, out_a, out_b]

    def keep(own, spot, i):
        return pltpu.make_async_copy(own, spot, loc.at[i])

    mine = [keep(wq, wv.at[:, pl.ds(0, part)], 0), keep(wv, wq_all, 1), keep(wsv, ws_all, 2), keep(px, px_ref, 3)]

    def chunk(k):
        return px.at[pl.ds(k * CLEN, CLEN)]

    def held(k):
        at = k if k < own_chunks else k - own_chunks
        return x_ref.at[pl.ds(at * CLEN, CLEN)]

    def hop(k, src, n, device):
        return remote(src, chunk(k), px_s.at[n, k], px_r.at[n, k], device)

    first = [k for k in range(chunks) if k < own_chunks]
    second = [k for k in range(chunks) if k >= own_chunks]
    low = [k for k in range(chunks) if k < chunks // 2]
    high = second + [k for k in range(chunks // 2, own_chunks)]

    def normed(k):
        anp_ref[k * CLEN : (k + 1) * CLEN, :] = norm_rows(px[k * CLEN : (k + 1) * CLEN, :], flat(gain_ref), flat(shift_ref))

    @pl.when(step == 0)
    def _():
        enter([me.core, me.x, me.y])

        @pl.when(me.t == 0)
        def _():
            for k in low:
                hop(k, held(k), 1, me.x).start()
            for k in reversed(first):
                hop(k, held(k), 0, me.core).start()

        @pl.when(me.t == 1)
        def _():
            for k in second:
                hop(k, held(k), 1, me.x).start()
                hop(k, held(k), 0, me.core).start()

        spot = lax.broadcasted_iota(jnp.int32, wsv.shape[1:], 0)
        table = jnp.where(spot == 16, flat(bin_ref), 0.0)
        width = wsv.shape[2]
        for i in range(2):
            row = jnp.concatenate([bqv_ref[i : i + 1, :].astype(F32), jnp.zeros((1, width - part), F32)], axis=1)
            for r in range(PIECES):
                moved = pltpu.roll(row, r * part, 1) if r else row
                table = jnp.where(spot == i * PIECES + r, moved, table)
        wsv[0] = table.astype(BF)
        for w in (w_qkv, w_small):
            w.side().start()
        mine[0].start()

        @pl.when(me.t >= 2)
        def _():
            for w in (w_qkv, w_small):
                w.across().start()

        @pl.when(me.t == 1)
        def _():
            for k in reversed(first):
                hop(k, held(k), 0, me.core).wait_recv()
                if k in high:
                    hop(k, chunk(k), 1, me.x).start()

        for w in later:
            w.side().start()
        for b in range(blocks):
            an_ref[b * CLEN : (b + 1) * CLEN, :] = norm_rows(x_ref[b * CLEN : (b + 1) * CLEN, :], flat(gain_ref), flat(shift_ref))

        @pl.when(me.t == 0)
        def _():
            for k in first:
                px[k * CLEN : (k + 1) * CLEN, :] = x_ref[k * CLEN : (k + 1) * CLEN, :]
            for k in second:
                hop(k, held(k), 0, me.core).wait_recv()
            for k in first:
                hop(k, held(k), 0, me.core).wait_send()
            for k in low:
                hop(k, held(k), 1, me.x).wait_send()

        @pl.when(me.t == 1)
        def _():
            for k in second:
                px[k * CLEN : (k + 1) * CLEN, :] = held(k)[...]
                hop(k, held(k), 0, me.core).wait_send()
            for k in high:
                hop(k, chunk(k), 1, me.x).wait_send()

        @pl.when(me.t == 2)
        def _():
            for k in low:
                hop(k, chunk(k), 1, me.x).wait_recv()
                hop(k, chunk(k), 0, me.core).start()
            for k in high:
                hop(k, chunk(k), 0, me.core).wait_recv()
            for k in low:
                hop(k, chunk(k), 0, me.core).wait_send()

        @pl.when(me.t == 3)
        def _():
            for k in high:
                hop(k, chunk(k), 1, me.x).wait_recv()
                hop(k, chunk(k), 0, me.core).start()
            for k in low:
                hop(k, chunk(k), 0, me.core).wait_recv()
            for k in high:
                hop(k, chunk(k), 0, me.core).wait_send()

        @pl.when(me.t < 2)
        def _():
            for w in (w_qkv, w_small):
                w.across().start()

        for k in range(chunks):
            normed(k)
        for w in (w_qkv, w_small):
            w.side().wait_recv()
        mine[0].wait()

    @pl.when(step == 3)
    def _():
        for w in (w_qkv, w_small):
            w.over(0).wait_recv()
            w.over(1).wait_recv()
        for i in range(1, 4):
            mine[i].start()

    def moves(slot):
        def at(k, *steps):
            @pl.when(slot == k)
            def _():
                for s in steps:
                    s()

        def go(w):
            return lambda: w.across().start()

        at(1, w_small.relay, w_qkv.relay, go(w_proj), go(in_a))
        at(4, w_proj.relay, go(in_b))
        at(6, w_qkv.relay_pair, w_small.relay_pair)
        at(7, in_a.relay, go(out_a))
        at(9, w_proj.relay_pair)
        at(11, in_b.relay, go(out_b))
        at(13, in_a.relay_pair)
        at(14, out_a.relay)
        at(16, in_b.relay_pair)

    pick = pl.ds(pl.multiple_of(step * 128, 128), 128)
    w3 = jnp.concatenate([wv[0, pick], wv[1, pick], wv[2, pick]], axis=0)
    u = 2 * lax.div(step, 3)
    left = wsv[u, :16, pick].astype(F32)
    right = wsv[u + 1, :16, pick].astype(F32)
    spot = lax.broadcasted_iota(jnp.int32, left.shape, 0)

    def bias(k):
        return jnp.sum(jnp.where(spot == u + k, left, 0.0) + jnp.where(spot == u + 1 + k, right, 0.0), axis=0, keepdims=True)

    bq = bias(0)
    bv = bias(PIECES)
    for b in range(blocks):
        at = slice(b * CLEN, (b + 1) * CLEN)
        got = nt(an_ref[at, :], w3)
        q_ref[at, :] = (got[:, :128] + bq).astype(BF)
        ko_ref[at, :] = got[:, 128:256].astype(BF)
        vo_ref[at, :] = (got[:, 256:] + bv).astype(BF)
    for c in range(chunks):
        at = slice(c * CLEN, (c + 1) * CLEN)
        got = nt(anp_ref[at, :], w3[128:])
        kp_ref[at, :] = got[:, :128].astype(BF)
        vp_ref[at, :] = (got[:, 128:] + bv).astype(BF)

    kph[...] = wide_keys(kp_ref[...], plen[0], 0)
    ones = jnp.ones((16, prompt), BF)
    vpt[...] = jnp.concatenate([transposed(vp_ref[...]).astype(BF), ones], axis=0)

    def block(b, _):
        moves(step * blocks + b)
        at = pl.ds(pl.multiple_of(b * CLEN, CLEN), CLEN)
        q2 = wide_queries(q_ref[at, :])
        vot = jnp.concatenate([transposed(vo_ref[at, :]).astype(BF), ones[:, :CLEN]], axis=0)
        sp = nt(kph[...], q2)
        so = nt(wide_keys(ko_ref[at, :], own_length(conts, me.t, blocks, b), 0), q2)
        top = jnp.maximum(jnp.max(sp, axis=0, keepdims=True), jnp.max(so, axis=0, keepdims=True))
        pp = jnp.exp(sp - top).astype(BF)
        po = jnp.exp(so - top).astype(BF)
        ot = nn(vpt[...], pp) + nn(vot, po)
        total = ot[128:129]
        ot = ot[:128] * (1.0 / total)
        logs = top + jnp.log(total)
        ctx_ref[at, :] = jnp.concatenate([ot[:64, :CLEN], ot[64:, CLEN:]], axis=0).T.astype(BF)
        lse_ref[0, b] = jnp.concatenate([logs[:, :CLEN], logs[:, CLEN:], jnp.zeros((6, CLEN), F32)], axis=0)
        return 0

    lax.fori_loop(0, blocks, block, 0)

    @pl.when(step == pl.num_programs(0) - 1)
    def _():
        out_b.relay()
        out_a.relay_pair()
        for w in [w_qkv, w_small]:
            w.side().wait_send()
            w.across().wait_send()
            w.pair().wait_send()
            w.over(0).wait_send()
            w.over(1).wait_send()
        for w in later:
            w.finish()
        for i in range(1, 4):
            mine[i].wait()


def front_call(plen, conts, x, gain, shift, bqv, b_in, wq, wp, wi, wo):
    rows, width = x.shape
    blocks = rows // CLEN
    pairs = width // 128
    r, p, logs = attn_specs(rows, PROMPT, blocks)
    cells = rows * (PROMPT + CLEN) * pairs * 2

    def whole(n):
        return pl.BlockSpec((n, width), lambda i, *l: (0, 0))

    def shape(*s):
        return jax.ShapeDtypeStruct(s, BF)

    part = wq.shape[1]
    small = (PIECES, 32, width)

    def raw(v):
        return pl.BlockSpec(v.shape, lambda i, *l: (0,) * v.ndim)

    return pl.pallas_call(
        front_kernel,
        out_shape=(
            shape(rows, width), shape(PROMPT, width), shape(PROMPT, width), shape(rows, width), shape(rows, width),
            shape(rows, width), jax.ShapeDtypeStruct((pairs, blocks, 8, CLEN), F32),
            shape(rows, width), shape(PROMPT, width), shape(PROMPT, width),
            shape(3, PIECES * part, width), shape(PIECES, *wp.shape), shape(PIECES, *wi.shape),
            shape(PIECES, *wo.shape), shape(*small),
        ),
        grid_spec=pltpu.PrefetchScalarGridSpec(
            num_scalar_prefetch=2,
            grid=(pairs,),
            in_specs=[whole(rows), raw(gain), raw(shift), raw(bqv), raw(b_in), ANY, ANY, ANY, ANY],
            out_specs=[r, p, p, r, r, r, logs, whole(rows), whole(PROMPT), ANY, ANY, ANY, ANY, ANY, ANY],
            scratch_shapes=[
                pltpu.VMEM((PROMPT, width), BF),
                pltpu.VMEM((3, PIECES * part, width), BF),
                pltpu.VMEM(small, BF),
                pltpu.VMEM((PROMPT, 256), BF),
                pltpu.VMEM((144, PROMPT), BF),
                pltpu.SemaphoreType.DMA((2, PROMPT // CLEN)),
                pltpu.SemaphoreType.DMA((2, PROMPT // CLEN)),
                pltpu.SemaphoreType.DMA((7, 5)),
                pltpu.SemaphoreType.DMA((7, 5)),
                pltpu.SemaphoreType.DMA((4,)),
            ],
        ),
        compiler_params=pltpu.CompilerParams(collective_id=0, has_side_effects=True, vmem_limit_bytes=62 << 20),
        cost_estimate=pl.CostEstimate(flops=cells * 256 * 4, transcendentals=cells, bytes_accessed=4 << 20),
        name="front",
    )(plen, conts, x, gain, shift, bqv, b_in, wq, wp, wi, wo)


STAGES = 7


def chunk_rows(rows, dp):
    unit = 16 * (min(dp, NEAR) // 2)
    return -(-rows // unit) * unit


class Sums:
    def __init__(self, me, half, held, scratch):
        self.me, self.half, self.held = me, half, held
        (self.r1, self.r3, self.xr, self.yr, self.zr, self.own,
         self.core_s, self.core_r, self.xs, self.ys, self.zs, self.zrs, self.fs, self.frs, self.gs) = scratch
        self.chunks, self.rows, self.width = self.r1.shape
        self.wide = self.width // 2
        self.share = self.rows // half
        self.mine = pl.ds(pl.multiple_of(me.p * self.wide, 128), self.wide)
        self.other = pl.ds(pl.multiple_of((1 - me.p) * self.wide, 128), self.wide)

    @staticmethod
    def scratch(chunks, rows, width, half):
        def buf(*s, dtype=BF):
            return pltpu.VMEM((chunks,) + s, dtype)

        def dma(n):
            return pltpu.SemaphoreType.DMA((chunks, n))

        wide = width // 2
        return [
            buf(rows, width), buf(rows, width), buf(rows, width), buf(rows, wide),
            buf(half, rows // half, wide), buf(rows // half, wide, dtype=F32),
            dma(2), dma(2), dma(2), dma(2), dma(half), dma(half), dma(half), dma(half), dma(2),
        ]

    def from_core(self, c, i, src=None):
        into = (self.r1, self.r3)[i].at[c]
        return remote(into if src is None else src, into, self.core_s.at[c, i], self.core_r.at[c, i], self.me.core)

    def across(self, c):
        return remote(self.held(c, 2), self.xr.at[c], self.xs.at[c, 0], self.xs.at[c, 1], self.me.x)

    def pair(self, c):
        return remote(self.held(c, 0).at[:, self.other], self.yr.at[c], self.ys.at[c, 0], self.ys.at[c, 1], self.me.y)

    def rows_of(self, k):
        at = lax.rem(self.me.z + k, self.half) * self.share
        return pl.ds(pl.multiple_of(at, 16), self.share)

    def rest(self, c, k):
        return remote(self.held(c, 0).at[self.rows_of(k), self.mine], self.zr.at[c, k],
                      self.zs.at[c, k], self.zrs.at[c, k], self.me.along(k, self.half))

    def back(self, c, k):
        spot = self.xr.at[c, self.rows_of(0), self.mine]
        return remote(spot, spot, self.fs.at[c, k], self.frs.at[c, k], self.me.along(k, self.half))

    def back_pair(self, c):
        spot = self.xr.at[c, :, self.mine]
        return remote(spot, spot, self.gs.at[c, 0], self.gs.at[c, 1], self.me.y)

    def start(self, c, i, src):
        self.from_core(c, i, src).start()

    def blocks(self, body):
        def one(k, _):
            body(pl.ds(pl.multiple_of(k * self.share, 16), self.share))
            return 0

        lax.fori_loop(0, self.half, one, 0)

    def to_chip(self, c):
        self.from_core(c, 1).wait_recv()
        g2 = self.held(c, 2)

        def body(s):
            g2[s, :] = (g2[s, :].astype(F32) + self.r3[c, s, :].astype(F32)).astype(BF)

        self.blocks(body)
        self.across(c).start()

    def term(self, c, s, lanes):
        g0 = self.held(c, 0)
        return g0[s, lanes].astype(F32) + self.r1[c, s, lanes].astype(F32) + self.xr[c, s, lanes].astype(F32)

    def to_pair(self, c):
        self.from_core(c, 0).wait()
        self.across(c).wait()
        g0 = self.held(c, 0)

        def body(s):
            g0[s, self.other] = self.term(c, s, self.other).astype(BF)

        self.blocks(body)
        self.pair(c).start()

    def to_rest(self, c):
        self.pair(c).wait()
        g0 = self.held(c, 0)
        at = self.rows_of(0)
        self.own[c] = self.term(c, at, self.mine) + self.yr[c, at, :].astype(F32)

        def body(s):
            g0[s, self.mine] = (self.term(c, s, self.mine) + self.yr[c, s, :].astype(F32)).astype(BF)

        self.blocks(body)
        for k in range(1, self.half):
            self.rest(c, k).start()

    def to_back(self, c):
        total = self.own[c]
        for k in range(1, self.half):
            self.rest(c, k).wait()
            total = total + self.zr[c, k].astype(F32)
        self.xr[c, self.rows_of(0), self.mine] = total.astype(BF)
        for k in range(1, self.half):
            self.back(c, k).start()

    def to_back_pair(self, c):
        for k in range(1, self.half):
            self.back(c, k).wait()
        self.back_pair(c).start()

    def finish(self, c):
        self.back_pair(c).wait()

    def progress(self, plan, slot):
        steps = [None, self.to_chip, self.to_pair, self.to_rest, self.to_back, self.to_back_pair]
        for k in plan["order"]:
            since = slot - plan[k]
            c = lax.div(since, plan["gap"])
            due = since >= 0
            if plan["gap"] > 1:
                due = jnp.logical_and(due, lax.rem(since, plan["gap"]) == 0)

            @pl.when(jnp.logical_and(due, c < self.chunks))
            def _():
                steps[k](c)

    def finish_all(self):
        for c in range(self.chunks):
            self.finish(c)


class SmallSum:
    def __init__(self, me, half, sm, scratch):
        self.me, self.half, self.sm = me, half, sm
        self.got, self.z, self.s, self.r = scratch

    @staticmethod
    def scratch(rows, width, half):
        return [
            pltpu.VMEM((4, rows, width), F32),
            pltpu.VMEM((half, rows, width), F32),
            pltpu.SemaphoreType.DMA((4 + half,)),
            pltpu.SemaphoreType.DMA((4 + half,)),
        ]

    def copy(self, i):
        src, device = [(1, self.me.core), (3, self.me.core), (2, self.me.x), (0, self.me.y)][i]
        return remote(self.sm.at[src], self.got.at[i], self.s.at[i], self.r.at[i], device)

    def rest(self, k):
        return remote(self.sm.at[0], self.z.at[k], self.s.at[4 + k], self.r.at[4 + k], self.me.along(k, self.half))

    def start(self):
        self.copy(1).start()
        self.copy(0).start()

    def to_chip(self):
        self.copy(1).wait()
        self.sm[2] = self.sm[2] + self.got[1]
        self.copy(2).start()

    def to_pair(self):
        self.copy(0).wait()
        self.copy(2).wait()
        self.sm[0] = self.sm[0] + self.got[0] + self.got[2]
        self.copy(3).start()

    def to_rest(self):
        self.copy(3).wait()
        self.sm[0] = self.sm[0] + self.got[3]
        for k in range(1, self.half):
            self.rest(k).start()

    def finish(self):
        total = self.sm[0]
        for k in range(1, self.half):
            self.rest(k).wait()
            total = total + self.z[k]
        return total


SUB = 3
FFN_PLAN = {"gap": 2, "order": (5, 4, 3, 2, 1), 1: 6, 2: 12, 3: 14, 4: 16, 5: 18}
QKV_PLAN = {"gap": 2, "order": (5, 4, 3, 2, 1), 1: 24, 2: 30, 3: 32, 4: 34, 5: 36}
QKV_START = (21, 30)
SMALL_PLAN = (31, 33, 35, 37, 39)
PROMPT_PLAN = (33, 42)
LAST_SLOT = 43


def back_kernel(half, grid_pairs, plen, conts, q_ref, kp_ref, vp_ref, ko_ref, vo_ref, lse_ref,
                w_any, an_any, anp_any, x_ref, px_any, ctx_ref, wp_any, wi_any, wo_any, wp_own, wi_own, wo_own, bias_ref,
                g1_ref, b_proj_ref, ln2_g_ref, ln2_b_ref, b_out_ref, dy_any,
                lo_any, ig_any, ffn_out, qkv_out, small_out,
                wbuf, wp_ref, l_s, dy, hid, gs, g0, g2,
                kx, vx, kt_s, acc, dqt, dkt, dvt, prompt_acc, own_acc, share_s, gq, sm, qv, sums,
                came, over, tail, w_s, f_s, p_s, p_r, o_s, *scratch):
    me = Peers()
    step = pl.program_id(0)
    rows = x_ref.shape[0]
    width = x_ref.shape[1]
    blocks = rows // CLEN
    prompt = kp_ref.shape[0]
    chunks = prompt // CLEN
    part = width // PIECES
    feats = grid_pairs // 2 * 128
    per = width // part
    ffn_scratch, qkv_scratch, small_scratch = scratch[:15], scratch[15:30], scratch[30:]
    branch, gmi, gel, gp, mlp, mlpt = prompt_acc, own_acc, gq.at[0], gq.at[1], gq.at[2], share_s.at[pl.ds(0, width)]
    an_ref = wbuf.at[pl.ds(0, rows)]
    anp_ref = wbuf.at[pl.ds(rows, prompt)]
    loads = [pltpu.make_async_copy(a, b, l_s.at[i]) for i, (a, b) in enumerate(((an_any, an_ref), (anp_any, anp_ref)))]

    def w_rows(j):
        return pl.ds(rows + prompt + j * feats, feats)

    def load_w(unit):
        return [
            pltpu.make_async_copy(w_any.at[j, pl.ds(unit * feats, feats)], wbuf.at[w_rows(j)], w_s.at[j]) for j in range(3)
        ]

    def ffn_rows(k, j):
        return pl.ds(pl.multiple_of((lax.rem(k, 2) * 2 + j) * width, 16), width)

    def load_ffn(k, own=False):
        srcs = (wi_own, wo_own) if own else [a.at[PIECES - 1 - k] for a in (wi_any, wo_any)]
        return [
            pltpu.make_async_copy(a, wbuf.at[ffn_rows(k, j)], f_s.at[lax.rem(k, 2), j]) for j, a in enumerate(srcs)
        ]

    px_parts = [(at, min(part, prompt - at)) for at in range(0, prompt, part)]
    load_px = [
        pltpu.make_async_copy(px_any.at[pl.ds(at, m)], gs.at[i, pl.ds(0, m)], l_s.at[4 + i]) for i, (at, m) in enumerate(px_parts)
    ]
    g1, b_proj, ln2_g, ln2_b, b_out = (flat(v) for v in (g1_ref, b_proj_ref, ln2_g_ref, ln2_b_ref, b_out_ref))

    def piece_rows(r):
        return pl.ds(pl.multiple_of(r * part, 16), part)

    ffn = Sums(me, half, lambda c, r: (g0 if r == 0 else g2).at[c], ffn_scratch)
    qkv = Sums(me, half, lambda c, r: gq.at[c, piece_rows(r)], qkv_scratch)
    smalls = SmallSum(me, half, sm, small_scratch)
    n = prompt // 2
    spare = rows - n
    mine = pl.ds(pl.multiple_of(me.odd * n, 16), n)
    side = remote(share_s.at[pl.ds(pl.multiple_of((1 - me.odd) * n, 16), n)], came, p_s.at[0], p_r.at[0], me.core)
    across = remote(share_s.at[mine], over, p_s.at[1], p_r.at[1], me.x)
    end = remote(share_s.at[pl.ds(pl.multiple_of(me.odd * n, 16), spare)], tail, p_s.at[2], p_r.at[2], me.core)

    def block_rows(b):
        return slice(b * CLEN, (b + 1) * CLEN)

    def normal_of(x):
        x = x - jnp.mean(x, axis=-1, keepdims=True)
        scale = lax.rsqrt(jnp.mean(x * x, axis=-1, keepdims=True) + EPS)
        return x * scale, scale

    def norm_back(e, normal, scale):
        return scale * (e - jnp.mean(e, axis=-1, keepdims=True) - normal * jnp.mean(e * normal, axis=-1, keepdims=True))

    @pl.when(step == 0)
    def _():
        got = pltpu.make_async_copy(dy_any, dy, o_s.at[0])
        first = pl.ds(0, part)
        rest = pl.ds(part, width - part)
        wp = [
            pltpu.make_async_copy(wp_own, wp_ref.at[first], l_s.at[2]),
            pltpu.make_async_copy(wp_any.at[rest], wp_ref.at[rest], l_s.at[3]),
        ]
        for c in wp:
            c.start()
        got.start()
        for c in load_ffn(0) + load_ffn(1):
            c.start()
        enter([me.core, me.x, me.y] + [me.along(k, half) for k in range(1, half)])
        for c in wp:
            c.wait()
        for b in range(blocks):
            at = block_rows(b)
            h = x_ref[at, :].astype(F32) + nn(ctx_ref[at, :], wp_ref[...]) + b_proj
            hid[at, :] = h
            normal, _ = normal_of(h)
            m = (normal * ln2_g + ln2_b).astype(BF)
            mlp[at, :] = m
            mlpt[:, at] = transposed(m).astype(BF)
        got.wait()
        branch[...] = jnp.zeros_like(branch)
        gmi[...] = jnp.zeros_like(gmi)
        sums[...] = jnp.zeros_like(sums)

    def ffn_block(b):
        at = pl.ds(pl.multiple_of(b * CLEN, CLEN), CLEN)
        r = PIECES - 1 - step
        wi = wbuf[ffn_rows(step, 0), :]
        wo = wbuf[ffn_rows(step, 1), :]
        pre = nn(mlp[at, :], wi) + bias_ref[r, 16:17, :].astype(F32)
        cdf = 0.5 * (1.0 + lax.erf(pre * (0.5**0.5)))
        pdf = jnp.exp(-0.5 * pre * pre) * 0.3989422804014327
        g = (pre * cdf).astype(BF)
        d = (nt(dy[at, :], wo) * (cdf + pre * pdf)).astype(BF)
        gel[at, :] = g
        gp[at, :] = d
        branch[at, :] += nn(g, wo)
        gmi[at, :] += nt(d, wi)
        sums[pl.ds(r, 1), :] += jnp.sum(d.astype(F32), axis=0, keepdims=True)

    def weight_grads():
        @pl.when(step == 2)
        def _():
            for c in range(2 * per):
                ffn.from_core(c, 1, gs.at[c]).wait_send()

        def one(j, _):
            two = pl.ds(pl.multiple_of(j * 2 * part, 128), 2 * part)
            both = (nn(mlpt[two, :], gp[...]), tn(gel[:, two], dy[...]))
            for k, got in enumerate(both):
                got = got.astype(BF).reshape(2, part, width)
                spot = pl.ds(2 * j + k * per, 2)

                @pl.when(lax.rem(step, 2) == 0)
                def _():
                    gs[spot] = got

                @pl.when(step == 1)
                def _():
                    g2[spot] = got

                @pl.when(step == 3)
                def _():
                    g0[spot] = got

            return 0

        lax.fori_loop(0, per // 2, one, 0)
        for at, i in ((0, 1), (2, 0)):
            @pl.when(step == at)
            def _():
                for c in range(2 * per):
                    ffn.start(c, i, gs.at[c])

    def after_ffn():
        for b in range(blocks):
            at = block_rows(b)
            g = gmi[at, :]
            h = hid[at, :]
            d = dy[at, :].astype(F32)
            normal, scale = normal_of(h)
            mlp[at, :] = (h + (branch[at, :] + b_out)).astype(BF)
            gh = d + norm_back(g * ln2_g, normal, scale)
            hid[at, :] = gh
            ga = gh.astype(BF)
            gel[at, :] = ga
            for k, v in enumerate((ga.astype(F32), g * normal, g, d)):
                sums[PIECES + k : PIECES + k + 1, :] += jnp.sum(v, axis=0, keepdims=True)
            dy[at, :] = nt(ga, wp_ref[...]).astype(BF)
        for c in loads + load_w(1):
            c.start()
        spots = (g0.at[2 * per], gs.at[2 * per + 1], g2.at[2 * per], gs.at[2 * per])
        for r in range(0, PIECES, 2):
            got = tn(ctx_ref[:, r * part : (r + 2) * part], gel[...]).astype(BF)
            spots[r][...] = got[:part]
            spots[r + 1][...] = got[part:]
        ffn.start(2 * per, 1, gs.at[2 * per])
        ffn.start(2 * per, 0, gs.at[2 * per + 1])
        pltpu.make_async_copy(mlp, lo_any, o_s.at[1]).start()
        own_acc[...] = jnp.zeros_like(own_acc)
        prompt_acc[...] = jnp.zeros_like(prompt_acc)

    sp = step - PIECES
    spot = lax.rem(jnp.maximum(sp, 0), grid_pairs // 2)
    pair = lax.rem(jnp.maximum(sp, 0) + grid_pairs // 2, grid_pairs)
    lanes = pl.ds(pl.multiple_of(pair * 128, 128), 128)
    attending = jnp.logical_and(sp >= 0, sp < grid_pairs)

    @pl.when(attending)
    def _():
        acc[...] = jnp.zeros_like(acc)
        kx[:prompt] = wide_keys(kp_ref[...], plen[0], 0)
        vx[:prompt] = wide_values(vp_ref[...])
        vx[prompt:] = wide_values(vo_ref[...])
        kt_s[:, :prompt] = transposed(kp_ref[...]).astype(BF)
        kt_s[:, prompt:] = transposed(ko_ref[...]).astype(BF)
        for b in range(blocks):
            at = block_rows(b)
            kx[prompt + b * CLEN : prompt + (b + 1) * CLEN] = wide_keys(ko_ref[at, :], own_length(conts, me.t, blocks, b), 0)

    def block(b):
        at = pl.ds(pl.multiple_of(b * CLEN, CLEN), CLEN)
        own = pl.ds(pl.multiple_of(prompt + b * CLEN, CLEN), CLEN)
        q = q_ref[at, :]
        do = dy[at, lanes]
        q2 = wide_queries(q)
        do2 = wide_grads(do, ctx_ref[at, lanes])
        qt = transposed(q).astype(BF)
        dot = transposed(do).astype(BF)
        logs = jnp.concatenate([lse_ref[0, b, 0:1, :], lse_ref[0, b, 1:2, :]], axis=1)

        def scores(keys):
            p = jnp.exp(nt(kx[keys, :], q2) - logs)
            ds = (p * nt(vx[keys, :], do2)).astype(BF)
            p = p.astype(BF)
            parts = []
            for left, m in ((qt, ds), (dot, p)):
                parts.append([nt(left[64 * h : 64 * h + 64], m[:, h * CLEN : (h + 1) * CLEN]) for h in range(2)])
            return parts, nn(kt_s[:, keys], ds)

        (dk, dv), dq = scores(pl.ds(0, prompt))
        for h in range(2):
            rows_h = slice(64 * h, 64 * h + 64)
            acc[0, rows_h, :] += dk[h]
            acc[1, rows_h, :] += dv[h]
        (dk, dv), dq_own = scores(own)
        dkt[spot, :, own] = (jnp.concatenate(dk, axis=0) * 0.125).astype(BF)
        dvt[spot, :, own] = jnp.concatenate(dv, axis=0).astype(BF)
        dq = dq + dq_own
        dqt[spot, :, at] = (jnp.concatenate([dq[:64, :CLEN], dq[64:, CLEN:]], axis=0) * 0.125).astype(BF)

        @pl.when(b == blocks - 1)
        def _():
            dkt[spot, :, :prompt] = (acc[0] * 0.125).astype(BF)
            dvt[spot, :, :prompt] = acc[1].astype(BF)

    def sub_step(sub, _):
        slot = step * SUB + sub
        ffn.progress(FFN_PLAN, slot)

        def at(k, body):
            @pl.when(slot == k)
            def _():
                body()

        def qkv_start(i):
            for c in range(3):
                qkv.start(c, i, gq.at[c, piece_rows(1 + 2 * i)])

        def prompt_chip():
            side.wait()
            share_s[mine, :] = (share_s[mine, :].astype(F32) + came[...].astype(F32)).astype(BF)

            @pl.when(me.t >= 2)
            def _():
                across.start()

        def qkv_sent():
            for c in range(3):
                qkv.from_core(c, 1, gq.at[c, piece_rows(3)]).wait_send()

        at(QKV_START[0], lambda: qkv_start(1))
        at(QKV_START[1], lambda: qkv_start(0))
        at(QKV_START[1], qkv_sent)
        qkv.progress(QKV_PLAN, slot)
        at(SMALL_PLAN[0], smalls.start)
        at(SMALL_PLAN[1], smalls.to_chip)
        at(SMALL_PLAN[2], smalls.to_pair)
        at(SMALL_PLAN[3], smalls.to_rest)
        at(PROMPT_PLAN[0], prompt_chip)

        @pl.when(step < PIECES)
        def _():
            ffn_block(sub)

        @pl.when(attending)
        def _():
            block(sub)

        return 0

    @pl.when(step < PIECES)
    def _():
        for c in load_ffn(step, True):
            c.wait()

    lax.fori_loop(0, SUB, sub_step, 0)

    @pl.when(step < PIECES)
    def _():
        @pl.when(step == 0)
        def _():
            for c in load_ffn(2):
                c.start()

        @pl.when(step == 1)
        def _():
            for c in load_ffn(3, True):
                c.start()

        weight_grads()

    @pl.when(step == PIECES - 1)
    def _():
        after_ffn()

    @pl.when(jnp.logical_and(attending, spot == grid_pairs // 2 - 1))
    def _():
        late = sp < grid_pairs // 2

        @pl.when(late)
        def _():
            for c in loads + [pltpu.make_async_copy(mlp, lo_any, o_s.at[1])]:
                c.wait()

        for c in load_w(0):
            c.wait()
        dq, dk, dv = (r[...].reshape(feats, -1) for r in (dqt, dkt, dvt))
        an = an_ref[...]
        anp = anp_ref[...]
        for j, d in enumerate((dq, dk, dv)):
            g = nn(d, an) if j == 0 else nn(d[:, prompt:], an) + nn(d[:, :prompt], anp)
            gq[j, pl.ds(pl.multiple_of(jnp.where(late, feats, 0), 16), feats), :] = g.astype(BF)
        sum_q = jnp.sum(dq.astype(F32), axis=1, keepdims=True)
        sum_v = jnp.sum(dv.astype(F32), axis=1, keepdims=True)
        both = jnp.concatenate([jnp.broadcast_to(sum_q, (feats, 128)), jnp.broadcast_to(sum_v, (feats, 128))], axis=1).T
        unit_lanes = pl.ds(pl.multiple_of(jnp.where(late, feats, 0), 128), feats)
        qv[0:1, unit_lanes] = both[0:1]
        qv[1:2, unit_lanes] = both[128:129]
        def turned(ref, at, j):
            return tn(ref[:, :, at : at + CLEN].reshape(feats, CLEN), wbuf[w_rows(j), :])

        for b in range(blocks):
            at = b * CLEN
            own_acc[at : at + CLEN, :] += (
                turned(dqt, at, 0) + turned(dkt, prompt + at, 1) + turned(dvt, prompt + at, 2)
            )
        for c in range(chunks):
            at = c * CLEN
            prompt_acc[at : at + CLEN, :] += turned(dkt, at, 1) + turned(dvt, at, 2)

        @pl.when(late)
        def _():
            for c in load_w(0):
                c.start()

        @pl.when(jnp.logical_not(late))
        def _():
            for c in load_px:
                c.start()

    @pl.when(sp == grid_pairs - 1)
    def _():
        for c in range(chunks):
            at = block_rows(c)
            share_s[at, :] = prompt_acc[at, :].astype(BF)
        side.start()
        sum_g = jnp.zeros((1, width), F32)
        sum_c = jnp.zeros((1, width), F32)
        raws = [(own_acc, at, m, x_ref.at[pl.ds(at, m)]) for at, m in [(part * k, part) for k in range(rows // part)]]
        raws += [(prompt_acc, at, m, gs.at[i, pl.ds(0, m)]) for i, (at, m) in enumerate(px_parts)]
        for i, (grad, at, m, raw) in enumerate(raws):
            if grad is prompt_acc:
                load_px[i - rows // part].wait()
            normal, _ = normal_of(raw[...].astype(F32))
            g = grad[at : at + m, :]
            sum_g = sum_g + jnp.sum(g * normal, axis=0, keepdims=True)
            sum_c = sum_c + jnp.sum(g, axis=0, keepdims=True)
        for r in range(PIECES):
            sm[r] = jnp.zeros_like(sm[r])
            sm[r, 0:1, :] = sums[r : r + 1, :]
            sm[r, 1:5, :] = sums[PIECES : PIECES + 4, :]
            for i in range(2):
                row = qv[i : i + 1, :]
                sm[r, 8 + i : 9 + i, :] = row if r == 0 else pltpu.roll(row, width - r * part, 1)
            sm[r, 10:11, :] = sum_g
            sm[r, 11:12, :] = sum_c

    @pl.when(step == pl.num_programs(0) - 1)
    def _():
        ffn.finish_all()
        qkv.finish_all()
        outs = [(ffn.xr, ffn_out), (qkv.xr, qkv_out)]
        copies = [pltpu.make_async_copy(a, b, o_s.at[2 + i]) for i, (a, b) in enumerate(outs)]
        for c in copies:
            c.start()
        small_out[...] = smalls.finish()
        ffn.from_core(2 * per, 1, gs.at[2 * per]).wait_send()

        @pl.when(me.t >= 2)
        def _():
            across.wait_send()

        @pl.when(me.t < 2)
        def _():
            across.wait_recv()
            share_s[mine, :] = (share_s[mine, :].astype(F32) + over[...].astype(F32)).astype(BF)

        @pl.when(me.t == 1)
        def _():
            end.start()
            for at in range(0, n - spare, CLEN):
                own_acc[at : at + CLEN, :] += share_s[n + spare + at : n + spare + at + CLEN, :].astype(F32)
            end.wait_send()

        @pl.when(me.t == 0)
        def _():
            for at in range(0, n, CLEN):
                own_acc[at : at + CLEN, :] += share_s[at : at + CLEN, :].astype(F32)
            end.wait_recv()
            own_acc[n:, :] += tail[...].astype(F32)

        for b in range(blocks):
            at = block_rows(b)
            normal, scale = normal_of(x_ref[at, :].astype(F32))
            hid[at, :] += norm_back(own_acc[at, :] * g1, normal, scale)
        last = pltpu.make_async_copy(hid, ig_any, o_s.at[0])
        last.start()
        for c in copies + [last]:
            c.wait()


def back_call(plen, conts, q, kp, vp, ko, vo, lse, wq_all, an, anp, x, px, ctx, wp, wi_all, wo_all, wp_own, wi_own, wo_own, ws_all, vecs, dy):
    rows, width = q.shape
    prompt = kp.shape[0]
    blocks = rows // CLEN
    pairs = width // 128
    part = width // PIECES
    half = min(lax.axis_size("dp"), NEAR) // 2
    cells = rows * (prompt + CLEN) * pairs * 2
    n_ffn = 2 * (width // part) + 1
    steps = -(-LAST_SLOT // SUB)
    assert blocks == SUB and wi_all.shape[1:] == (width, width) and rows == width and part % (16 * half) == 0
    small_n = 16

    def pair(i):
        return lax.rem(jnp.clip(i - PIECES, 0, pairs - 1) + pairs // 2, pairs)

    def col(n):
        return pl.BlockSpec((n, 128), lambda i, *l: (0, pair(i)))

    def whole(*s):
        return pl.BlockSpec(s, lambda i, *l: (0,) * len(s), pipeline_mode=pl.Buffered(1))

    r, p = col(rows), col(prompt)
    logs = pl.BlockSpec((1, blocks, 8, CLEN), lambda i, *l: (pair(i), 0, 0, 0))
    return pl.pallas_call(
        functools.partial(back_kernel, half, pairs),
        out_shape=(
            jax.ShapeDtypeStruct((rows, width), BF),
            jax.ShapeDtypeStruct((rows, width), F32),
            jax.ShapeDtypeStruct((n_ffn, part, width), BF),
            jax.ShapeDtypeStruct((3, part, width), BF),
            jax.ShapeDtypeStruct((small_n, width), F32),
        ),
        grid_spec=pltpu.PrefetchScalarGridSpec(
            num_scalar_prefetch=2,
            grid=(steps,),
            in_specs=[r, p, p, r, r, logs, ANY, ANY, ANY, whole(rows, width),
                      ANY, whole(rows, width)] + [ANY] * 6 + [whole(*ws_all.shape)] + [whole(width)] * 5 + [ANY],
            out_specs=[ANY, ANY, ANY, ANY, pl.BlockSpec((small_n, width), lambda i, *l: (0, 0))],
            scratch_shapes=[
                pltpu.VMEM((max(4 * width, rows + prompt + 3 * pairs // 2 * 128), width), BF),
                pltpu.VMEM((width, width), BF),
                pltpu.SemaphoreType.DMA((4 + -(-prompt // part),)),
                pltpu.VMEM((rows, width), BF),
                pltpu.VMEM((rows, width), F32),
                pltpu.VMEM((n_ffn + 1, part, width), BF),
                pltpu.VMEM((n_ffn, part, width), BF),
                pltpu.VMEM((n_ffn, part, width), BF),
                pltpu.VMEM((prompt + rows, 256), BF),
                pltpu.VMEM((prompt + rows, 256), BF),
                pltpu.VMEM((128, prompt + rows), BF),
                pltpu.VMEM((2, 128, prompt), F32),
                pltpu.VMEM((pairs // 2, 128, rows), BF),
                pltpu.VMEM((pairs // 2, 128, prompt + rows), BF),
                pltpu.VMEM((pairs // 2, 128, prompt + rows), BF),
                pltpu.VMEM((prompt, width), F32),
                pltpu.VMEM((rows, width), F32),
                pltpu.VMEM((prompt, width), BF),
                pltpu.VMEM((3, width, width), BF),
                pltpu.VMEM((PIECES, small_n, width), F32),
                pltpu.VMEM((8, width), F32),
                pltpu.VMEM((8, width), F32),
                pltpu.VMEM((prompt // 2, width), BF),
                pltpu.VMEM((prompt // 2, width), BF),
                pltpu.VMEM((rows - prompt // 2, width), BF),
                pltpu.SemaphoreType.DMA((3,)),
                pltpu.SemaphoreType.DMA((2, 2)),
                pltpu.SemaphoreType.DMA((3,)),
                pltpu.SemaphoreType.DMA((3,)),
                pltpu.SemaphoreType.DMA((4,)),
            ]
            + Sums.scratch(n_ffn, part, width, half)
            + Sums.scratch(3, part, width, half)
            + SmallSum.scratch(small_n, width, half),
        ),
        compiler_params=pltpu.CompilerParams(collective_id=1, has_side_effects=True, vmem_limit_bytes=63 << 20),
        cost_estimate=pl.CostEstimate(flops=cells * 256 * 10, transcendentals=cells, bytes_accessed=16 << 20),
        name="back",
    )(plen, conts, q, kp, vp, ko, vo, lse, wq_all, an, anp, x, px, ctx, wp, wi_all, wo_all, wp_own, wi_own, wo_own, ws_all, *vecs, dy)


def shards(layer_in, prompt_len, cont_len, w_qkv, b_qv, w_proj, b_proj, ln1_gain, ln1_bias,
           ln2_gain, ln2_bias, w_in, b_in, w_out, b_out, out_grad):
    rows, width = layer_in.shape
    part = w_qkv.shape[2]
    (q, kp, vp, ko, vo, ctx, lse, attn_input, prompt_input, prompt_rows, wq_all, wp_all, wi_all, wo_all, ws_all) = front_call(
        prompt_len, cont_len, layer_in, ln1_gain, ln1_bias, b_qv, b_in, w_qkv.transpose(0, 2, 1), w_proj, w_in, w_out
    )
    layer_out, in_grad, ffn, qkv, small = back_call(
        prompt_len, cont_len, q, kp, vp, ko, vo, lse, wq_all, attn_input, prompt_input, layer_in, prompt_rows, ctx,
        wp_all.reshape(width, width), wi_all, wo_all, w_proj, w_in, w_out, ws_all,
        (ln1_gain, b_proj, ln2_gain, ln2_bias, b_out), out_grad
    )
    ffn = beyond(ffn.astype(F32))
    qkv = beyond(qkv.astype(F32))
    small = beyond(small)
    per = ffn.shape[0] // 2
    grad_w_in = ffn[:per].reshape(width, -1)
    grad_w_out = ffn[per : 2 * per].reshape(-1, width)
    return (layer_out, in_grad, qkv.transpose(0, 2, 1), small[8:10, :part], ffn[2 * per], small[1], small[10], small[11],
            small[2], small[3], grad_w_in, small[0, : w_in.shape[1]], grad_w_out, small[4])


def solution(mesh):
    in_specs = (
        P(("dp", "tensor"), None),
        P("dp"),
        P("dp", None),
        P(None, None, "tensor"),
        P(None, "tensor"),
        P("tensor", None),
        P(),
        P(),
        P(),
        P(),
        P(),
        P(None, "tensor"),
        P("tensor"),
        P("tensor", None),
        P(),
        P(("dp", "tensor"), None),
    )
    out_specs = (
        P(("dp", "tensor"), None),
        P(("dp", "tensor"), None),
        P(None, None, "tensor"),
        P(None, "tensor"),
        P("tensor", None),
        P(),
        P(),
        P(),
        P(),
        P(),
        P(None, "tensor"),
        P("tensor"),
        P("tensor", None),
        P(),
    )
    return jax.shard_map(shards, mesh=mesh, in_specs=in_specs, out_specs=out_specs, check_vma=False)
```

```python
import functools

import jax
import jax.numpy as jnp
from jax import lax
from jax.experimental import pallas as pl
from jax.experimental.pallas import tpu as pltpu
from jax.sharding import PartitionSpec as P

HEAD = 64
PROMPT = 1024
CONT = 8
CLEN = 256
PIECES = 4
MESH = pl.DeviceIdType.MESH
ANY = pl.BlockSpec(memory_space=pl.ANY)

EPS = 1e-06
MASKED = -1000000000.0
BF = jnp.bfloat16
F32 = jnp.float32


def nt(a, b):
    return lax.dot_general(a, b, (((1,), (1,)), ((), ())), preferred_element_type=F32)


def nn(a, b):
    return lax.dot_general(a, b, (((1,), (0,)), ((), ())), preferred_element_type=F32)


def tn(a, b):
    return lax.dot_general(a, b, (((0,), (0,)), ((), ())), preferred_element_type=F32)


NEAR = 8


class Peers:
    def __init__(self):
        self.t = lax.axis_index("tensor")
        self.d = lax.axis_index("dp")
        self.odd = lax.rem(self.t, 2)
        self.p = lax.rem(self.d, 2)
        self.z = lax.div(lax.rem(self.d, NEAR), 2)
        self.base = self.d - lax.rem(self.d, NEAR)
        self.core = {"tensor": self.t + 1 - 2 * self.odd}
        self.x = {"tensor": lax.rem(self.t + 2, 4)}
        self.y = {"dp": self.d + 1 - 2 * self.p}

    def along(self, k, count):
        return {"dp": self.base + lax.rem(self.z + k, count) * 2 + self.p}


def enter(devices):
    barrier = pltpu.get_barrier_semaphore()
    for device in devices:
        pl.semaphore_signal(barrier, inc=1, device_id=device, device_id_type=MESH)
    pl.semaphore_wait(barrier, len(devices))


def remote(src, dst, send, recv, device):
    return pltpu.make_async_remote_copy(
        src_ref=src, dst_ref=dst, send_sem=send, recv_sem=recv, device_id=device, device_id_type=MESH
    )


def beyond(value):
    size = lax.axis_size("dp")
    step = NEAR
    while step < size:
        value = value + lax.ppermute(value, "dp", [(i, i ^ step) for i in range(size)])
        step *= 2
    return value


def own_lanes(rows, h):
    lane = lax.broadcasted_iota(jnp.int32, (rows, 128), 1)
    return ((lane < 64) if h == 0 else (lane >= 64)), lane - (64 if h == 0 else 0)


def key_aug(k, h, length, base):
    rows = k.shape[0]
    own, extra = own_lanes(rows, h)
    row = lax.broadcasted_iota(jnp.int32, (rows, 128), 0) + base
    bias = jnp.where(jnp.logical_and(extra == 0, row >= length), MASKED, 0.0)
    return jnp.where(own, k.astype(F32), bias).astype(BF)


def query_aug(q, h):
    own, extra = own_lanes(q.shape[0], h)
    return jnp.where(own, q.astype(F32) * 0.125, jnp.where(extra == 0, 1.0, 0.0)).astype(BF)


def value_aug(v, h):
    own, extra = own_lanes(v.shape[0], h)
    ones = jnp.where(jnp.logical_and(extra >= 0, extra < 3), 1.0, 0.0)
    return jnp.where(own, v.astype(F32), ones).astype(BF)


def transposed(v):
    return v.astype(F32).T


def wide_keys(k, length, base):
    rows = k.shape[0]
    lane = lax.broadcasted_iota(jnp.int32, (rows, 128), 1)
    row = lax.broadcasted_iota(jnp.int32, (rows, 128), 0) + base
    bias = jnp.where(jnp.logical_and(lane == 0, row >= length), MASKED, 0.0).astype(BF)
    return jnp.concatenate([k, bias], axis=1)


def wide_values(v):
    lane = lax.broadcasted_iota(jnp.int32, v.shape, 1)
    return jnp.concatenate([v, jnp.where(lane < 3, 1.0, 0.0).astype(BF)], axis=1)


def wide_queries(q):
    lane = lax.broadcasted_iota(jnp.int32, q.shape, 1)
    qf = q.astype(F32) * 0.125
    one = jnp.where(lane == 0, 1.0, 0.0)
    heads = [jnp.where(lane < 64, qf, 0.0), jnp.where(lane < 64, 0.0, qf)]
    return jnp.concatenate([jnp.concatenate([h, one], axis=1) for h in heads], axis=0).astype(BF)


def wide_grads(do, ctx):
    lane = lax.broadcasted_iota(jnp.int32, do.shape, 1)
    do = do.astype(F32)
    prod = do * ctx.astype(F32)
    out = []
    for h in range(2):
        mine = (lane < 64) if h == 0 else (lane >= 64)
        d = -jnp.sum(jnp.where(mine, prod, 0.0), axis=1, keepdims=True)
        hi = d.astype(BF).astype(F32)
        mid = (d - hi).astype(BF).astype(F32)
        low = d - hi - mid
        aug = jnp.where(lane == 0, hi, jnp.where(lane == 1, mid, jnp.where(lane == 2, low, 0.0)))
        out.append(jnp.concatenate([jnp.where(mine, do, 0.0), aug], axis=1))
    return jnp.concatenate(out, axis=0).astype(BF)


def attn_specs(rows, prompt, blocks):
    def col(n):
        return pl.BlockSpec((n, 128), lambda i, *l: (0, i))

    logs = pl.BlockSpec((1, blocks, 8, CLEN), lambda i, *l: (i, 0, 0, 0))
    return col(rows), col(prompt), logs

def own_length(conts, t, blocks, b):
    c = t * blocks + b - PROMPT // CLEN
    return jnp.where(c >= 0, conts[0, jnp.maximum(c, 0)], 0)


class Weight:
    def __init__(self, me, own, spots, view, sems, direct=False):
        self.me, self.own, self.spots, self.view, self.direct = me, own, spots, view, direct
        self.send, self.recv = sems

    def side(self):
        return remote(self.own, self.spots(1), self.send.at[0], self.recv.at[0], self.me.core)

    def across(self):
        p = self.me.p
        src, dst = (self.own, self.spots(2)) if self.direct else (self.view(None, p), self.view(2, p))
        return remote(src, dst, self.send.at[1], self.recv.at[1], self.me.x)

    def pair(self):
        p = self.me.p
        return remote(self.view(2, p), self.view(2, p), self.send.at[2], self.recv.at[2], self.me.y)

    def over(self, which):
        h = self.me.p if which == 0 else 1 - self.me.p
        src, dst = (self.spots(2), self.spots(3)) if self.direct else (self.view(2, h), self.view(3, h))
        return remote(src, dst, self.send.at[3 + which], self.recv.at[3 + which], self.me.core)

    def start(self):
        self.side().start()
        self.across().start()

    def relay(self):
        self.across().wait_recv()
        if not self.direct:
            self.pair().start()
        self.over(0).start()

    def relay_pair(self):
        self.pair().wait_recv()
        self.over(1).start()

    def finish(self):
        self.side().wait()
        self.across().wait_send()
        self.over(0).wait()
        if not self.direct:
            self.pair().wait_send()
            self.over(1).wait()


def norm_rows(x, gain, shift):
    x = x.astype(F32)
    centred = x - jnp.mean(x, axis=-1, keepdims=True)
    scale = lax.rsqrt(jnp.mean(centred * centred, axis=-1, keepdims=True) + EPS)
    return (centred * scale * gain + shift).astype(BF)


def flat(ref):
    return ref[...].astype(F32).reshape(1, ref.shape[0])


def front_kernel(plen, conts, x_ref, gain_ref, shift_ref, bqv_ref, bin_ref, wq, wp, wi, wo,
                 q_ref, kp_ref, vp_ref, ko_ref, vo_ref, ctx_ref, lse_ref, an_ref, anp_ref, px_ref,
                 wq_all, wp_all, wi_all, wo_all, ws_all,
                 px, wv, wsv, kph, vpt, px_s, px_r, send, recv, loc):
    me = Peers()
    step = pl.program_id(0)
    rows = x_ref.shape[0]
    blocks = rows // CLEN
    prompt = px.shape[0]
    part = wq.shape[1]
    own_chunks = rows // CLEN
    chunks = prompt // CLEN

    def qkv_view(r, h):
        n = part // 2
        if r is None:
            return wq.at[:, pl.ds(h * n, n)]
        return wv.at[:, pl.ds(r * part + h * n, n)]

    def plain(own, everything):
        n = own.shape[0] // 2

        def view(r, h):
            return own.at[pl.ds(h * n, n)] if r is None else everything.at[r, pl.ds(h * n, n)]

        return view

    def weight(i, own, everything):
        return Weight(me, own, lambda r: everything.at[r], plain(own, everything), (send.at[i], recv.at[i]))

    w_qkv = Weight(me, wq, lambda r: wv.at[:, pl.ds(r * part, part)], qkv_view, (send.at[0], recv.at[0]))
    w_small = weight(1, wsv.at[0], wsv)
    w_proj = weight(2, wp, wp_all)
    half_in = wi.shape[0] // 2
    half_out = wo.shape[0] // 2

    def rows_of(i, own, everything, first, n, direct=False):
        part_rows = pl.ds(first, n)
        sub = n // 2

        def view(r, h):
            at = pl.ds(first + h * sub, sub)
            return own.at[at] if r is None else everything.at[r, at]

        return Weight(me, own.at[part_rows], lambda r: everything.at[r, part_rows], view, (send.at[i], recv.at[i]), direct)

    in_a = rows_of(3, wi, wi_all, 0, half_in)
    in_b = rows_of(4, wi, wi_all, half_in, half_in)
    out_a = rows_of(5, wo, wo_all, 0, half_out)
    out_b = rows_of(6, wo, wo_all, half_out, half_out, True)
    later = [w_proj, in_a, in_b, out_a, out_b]

    def keep(own, spot, i):
        return pltpu.make_async_copy(own, spot, loc.at[i])

    mine = [keep(wq, wv.at[:, pl.ds(0, part)], 0), keep(wv, wq_all, 1), keep(wsv, ws_all, 2), keep(px, px_ref, 3)]

    def chunk(k):
        return px.at[pl.ds(k * CLEN, CLEN)]

    def held(k):
        at = k if k < own_chunks else k - own_chunks
        return x_ref.at[pl.ds(at * CLEN, CLEN)]

    def hop(k, src, n, device):
        return remote(src, chunk(k), px_s.at[n, k], px_r.at[n, k], device)

    first = [k for k in range(chunks) if k < own_chunks]
    second = [k for k in range(chunks) if k >= own_chunks]
    low = [k for k in range(chunks) if k < chunks // 2]
    high = second + [k for k in range(chunks // 2, own_chunks)]

    def normed(k):
        anp_ref[k * CLEN : (k + 1) * CLEN, :] = norm_rows(px[k * CLEN : (k + 1) * CLEN, :], flat(gain_ref), flat(shift_ref))

    @pl.when(step == 0)
    def _():
        enter([me.core, me.x, me.y])

        @pl.when(me.t == 0)
        def _():
            for k in low:
                hop(k, held(k), 1, me.x).start()
            for k in reversed(first):
                hop(k, held(k), 0, me.core).start()

        @pl.when(me.t == 1)
        def _():
            for k in second:
                hop(k, held(k), 1, me.x).start()
                hop(k, held(k), 0, me.core).start()

        spot = lax.broadcasted_iota(jnp.int32, wsv.shape[1:], 0)
        table = jnp.where(spot == 16, flat(bin_ref), 0.0)
        width = wsv.shape[2]
        for i in range(2):
            row = jnp.concatenate([bqv_ref[i : i + 1, :].astype(F32), jnp.zeros((1, width - part), F32)], axis=1)
            for r in range(PIECES):
                moved = pltpu.roll(row, r * part, 1) if r else row
                table = jnp.where(spot == i * PIECES + r, moved, table)
        wsv[0] = table.astype(BF)
        for w in (w_qkv, w_small):
            w.side().start()
        mine[0].start()

        @pl.when(me.t >= 2)
        def _():
            for w in (w_qkv, w_small):
                w.across().start()

        @pl.when(me.t == 1)
        def _():
            for k in reversed(first):
                hop(k, held(k), 0, me.core).wait_recv()
                if k in high:
                    hop(k, chunk(k), 1, me.x).start()

        for w in later:
            w.side().start()
        for b in range(blocks):
            an_ref[b * CLEN : (b + 1) * CLEN, :] = norm_rows(x_ref[b * CLEN : (b + 1) * CLEN, :], flat(gain_ref), flat(shift_ref))

        @pl.when(me.t == 0)
        def _():
            for k in first:
                px[k * CLEN : (k + 1) * CLEN, :] = x_ref[k * CLEN : (k + 1) * CLEN, :]
            for k in second:
                hop(k, held(k), 0, me.core).wait_recv()
            for k in first:
                hop(k, held(k), 0, me.core).wait_send()
            for k in low:
                hop(k, held(k), 1, me.x).wait_send()

        @pl.when(me.t == 1)
        def _():
            for k in second:
                px[k * CLEN : (k + 1) * CLEN, :] = held(k)[...]
                hop(k, held(k), 0, me.core).wait_send()
            for k in high:
                hop(k, chunk(k), 1, me.x).wait_send()

        @pl.when(me.t == 2)
        def _():
            for k in low:
                hop(k, chunk(k), 1, me.x).wait_recv()
                hop(k, chunk(k), 0, me.core).start()
            for k in high:
                hop(k, chunk(k), 0, me.core).wait_recv()
            for k in low:
                hop(k, chunk(k), 0, me.core).wait_send()

        @pl.when(me.t == 3)
        def _():
            for k in high:
                hop(k, chunk(k), 1, me.x).wait_recv()
                hop(k, chunk(k), 0, me.core).start()
            for k in low:
                hop(k, chunk(k), 0, me.core).wait_recv()
            for k in high:
                hop(k, chunk(k), 0, me.core).wait_send()

        @pl.when(me.t < 2)
        def _():
            for w in (w_qkv, w_small):
                w.across().start()

        for k in range(chunks):
            normed(k)
        for w in (w_qkv, w_small):
            w.side().wait_recv()
        mine[0].wait()

    @pl.when(step == 3)
    def _():
        for w in (w_qkv, w_small):
            w.over(0).wait_recv()
            w.over(1).wait_recv()
        for i in range(1, 4):
            mine[i].start()

    def moves(slot):
        def at(k, *steps):
            @pl.when(slot == k)
            def _():
                for s in steps:
                    s()

        def go(w):
            return lambda: w.across().start()

        at(1, w_small.relay, w_qkv.relay, go(w_proj), go(in_a))
        at(4, w_proj.relay, go(in_b))
        at(6, w_qkv.relay_pair, w_small.relay_pair)
        at(7, in_a.relay, go(out_a))
        at(9, w_proj.relay_pair)
        at(11, in_b.relay, go(out_b))
        at(13, in_a.relay_pair)
        at(14, out_a.relay)
        at(16, in_b.relay_pair)

    pick = pl.ds(pl.multiple_of(step * 128, 128), 128)
    w3 = jnp.concatenate([wv[0, pick], wv[1, pick], wv[2, pick]], axis=0)
    u = 2 * lax.div(step, 3)
    left = wsv[u, :16, pick].astype(F32)
    right = wsv[u + 1, :16, pick].astype(F32)
    spot = lax.broadcasted_iota(jnp.int32, left.shape, 0)

    def bias(k):
        return jnp.sum(jnp.where(spot == u + k, left, 0.0) + jnp.where(spot == u + 1 + k, right, 0.0), axis=0, keepdims=True)

    bq = bias(0)
    bv = bias(PIECES)
    for b in range(blocks):
        at = slice(b * CLEN, (b + 1) * CLEN)
        got = nt(an_ref[at, :], w3)
        q_ref[at, :] = (got[:, :128] + bq).astype(BF)
        ko_ref[at, :] = got[:, 128:256].astype(BF)
        vo_ref[at, :] = (got[:, 256:] + bv).astype(BF)
    for c in range(chunks):
        at = slice(c * CLEN, (c + 1) * CLEN)
        got = nt(anp_ref[at, :], w3[128:])
        kp_ref[at, :] = got[:, :128].astype(BF)
        vp_ref[at, :] = (got[:, 128:] + bv).astype(BF)

    kph[...] = wide_keys(kp_ref[...], plen[0], 0)
    ones = jnp.ones((16, prompt), BF)
    vpt[...] = jnp.concatenate([transposed(vp_ref[...]).astype(BF), ones], axis=0)

    def block(b, _):
        moves(step * blocks + b)
        at = pl.ds(pl.multiple_of(b * CLEN, CLEN), CLEN)
        q2 = wide_queries(q_ref[at, :])
        vot = jnp.concatenate([transposed(vo_ref[at, :]).astype(BF), ones[:, :CLEN]], axis=0)
        sp = nt(kph[...], q2)
        so = nt(wide_keys(ko_ref[at, :], own_length(conts, me.t, blocks, b), 0), q2)
        top = jnp.maximum(jnp.max(sp, axis=0, keepdims=True), jnp.max(so, axis=0, keepdims=True))
        pp = jnp.exp(sp - top).astype(BF)
        po = jnp.exp(so - top).astype(BF)
        ot = nn(vpt[...], pp) + nn(vot, po)
        total = ot[128:129]
        ot = ot[:128] * (1.0 / total)
        logs = top + jnp.log(total)
        ctx_ref[at, :] = jnp.concatenate([ot[:64, :CLEN], ot[64:, CLEN:]], axis=0).T.astype(BF)
        lse_ref[0, b] = jnp.concatenate([logs[:, :CLEN], logs[:, CLEN:], jnp.zeros((6, CLEN), F32)], axis=0)
        return 0

    lax.fori_loop(0, blocks, block, 0)

    @pl.when(step == pl.num_programs(0) - 1)
    def _():
        out_b.relay()
        out_a.relay_pair()
        for w in [w_qkv, w_small]:
            w.side().wait_send()
            w.across().wait_send()
            w.pair().wait_send()
            w.over(0).wait_send()
            w.over(1).wait_send()
        for w in later:
            w.finish()
        for i in range(1, 4):
            mine[i].wait()


def front_call(plen, conts, x, gain, shift, bqv, b_in, wq, wp, wi, wo):
    rows, width = x.shape
    blocks = rows // CLEN
    pairs = width // 128
    r, p, logs = attn_specs(rows, PROMPT, blocks)
    cells = rows * (PROMPT + CLEN) * pairs * 2

    def whole(n):
        return pl.BlockSpec((n, width), lambda i, *l: (0, 0))

    def shape(*s):
        return jax.ShapeDtypeStruct(s, BF)

    part = wq.shape[1]
    small = (PIECES, 32, width)

    def raw(v):
        return pl.BlockSpec(v.shape, lambda i, *l: (0,) * v.ndim)

    return pl.pallas_call(
        front_kernel,
        out_shape=(
            shape(rows, width), shape(PROMPT, width), shape(PROMPT, width), shape(rows, width), shape(rows, width),
            shape(rows, width), jax.ShapeDtypeStruct((pairs, blocks, 8, CLEN), F32),
            shape(rows, width), shape(PROMPT, width), shape(PROMPT, width),
            shape(3, PIECES * part, width), shape(PIECES, *wp.shape), shape(PIECES, *wi.shape),
            shape(PIECES, *wo.shape), shape(*small),
        ),
        grid_spec=pltpu.PrefetchScalarGridSpec(
            num_scalar_prefetch=2,
            grid=(pairs,),
            in_specs=[whole(rows), raw(gain), raw(shift), raw(bqv), raw(b_in), ANY, ANY, ANY, ANY],
            out_specs=[r, p, p, r, r, r, logs, whole(rows), whole(PROMPT), ANY, ANY, ANY, ANY, ANY, ANY],
            scratch_shapes=[
                pltpu.VMEM((PROMPT, width), BF),
                pltpu.VMEM((3, PIECES * part, width), BF),
                pltpu.VMEM(small, BF),
                pltpu.VMEM((PROMPT, 256), BF),
                pltpu.VMEM((144, PROMPT), BF),
                pltpu.SemaphoreType.DMA((2, PROMPT // CLEN)),
                pltpu.SemaphoreType.DMA((2, PROMPT // CLEN)),
                pltpu.SemaphoreType.DMA((7, 5)),
                pltpu.SemaphoreType.DMA((7, 5)),
                pltpu.SemaphoreType.DMA((4,)),
            ],
        ),
        compiler_params=pltpu.CompilerParams(collective_id=0, has_side_effects=True, vmem_limit_bytes=62 << 20),
        cost_estimate=pl.CostEstimate(flops=cells * 256 * 4, transcendentals=cells, bytes_accessed=4 << 20),
        name="front",
    )(plen, conts, x, gain, shift, bqv, b_in, wq, wp, wi, wo)


STAGES = 7


def chunk_rows(rows, dp):
    unit = 16 * (min(dp, NEAR) // 2)
    return -(-rows // unit) * unit


class Sums:
    def __init__(self, me, half, held, scratch):
        self.me, self.half, self.held = me, half, held
        (self.r1, self.r3, self.xr, self.yr, self.zr, self.own,
         self.core_s, self.core_r, self.xs, self.ys, self.zs, self.zrs, self.fs, self.frs, self.gs) = scratch
        self.chunks, self.rows, self.width = self.r1.shape
        self.wide = self.width // 2
        self.share = self.rows // half
        self.mine = pl.ds(pl.multiple_of(me.p * self.wide, 128), self.wide)
        self.other = pl.ds(pl.multiple_of((1 - me.p) * self.wide, 128), self.wide)

    @staticmethod
    def scratch(chunks, rows, width, half):
        def buf(*s, dtype=BF):
            return pltpu.VMEM((chunks,) + s, dtype)

        def dma(n):
            return pltpu.SemaphoreType.DMA((chunks, n))

        wide = width // 2
        return [
            buf(rows, width), buf(rows, width), buf(rows, width), buf(rows, wide),
            buf(half, rows // half, wide), buf(rows // half, wide, dtype=F32),
            dma(2), dma(2), dma(2), dma(2), dma(half), dma(half), dma(half), dma(half), dma(2),
        ]

    def from_core(self, c, i, src=None):
        into = (self.r1, self.r3)[i].at[c]
        return remote(into if src is None else src, into, self.core_s.at[c, i], self.core_r.at[c, i], self.me.core)

    def across(self, c):
        return remote(self.held(c, 2), self.xr.at[c], self.xs.at[c, 0], self.xs.at[c, 1], self.me.x)

    def pair(self, c):
        return remote(self.held(c, 0).at[:, self.other], self.yr.at[c], self.ys.at[c, 0], self.ys.at[c, 1], self.me.y)

    def rows_of(self, k):
        at = lax.rem(self.me.z + k, self.half) * self.share
        return pl.ds(pl.multiple_of(at, 16), self.share)

    def rest(self, c, k):
        return remote(self.held(c, 0).at[self.rows_of(k), self.mine], self.zr.at[c, k],
                      self.zs.at[c, k], self.zrs.at[c, k], self.me.along(k, self.half))

    def back(self, c, k):
        spot = self.xr.at[c, self.rows_of(0), self.mine]
        return remote(spot, spot, self.fs.at[c, k], self.frs.at[c, k], self.me.along(k, self.half))

    def back_pair(self, c):
        spot = self.xr.at[c, :, self.mine]
        return remote(spot, spot, self.gs.at[c, 0], self.gs.at[c, 1], self.me.y)

    def start(self, c, i, src):
        self.from_core(c, i, src).start()

    def blocks(self, body):
        def one(k, _):
            body(pl.ds(pl.multiple_of(k * self.share, 16), self.share))
            return 0

        lax.fori_loop(0, self.half, one, 0)

    def to_chip(self, c):
        self.from_core(c, 1).wait_recv()
        g2 = self.held(c, 2)

        def body(s):
            g2[s, :] = (g2[s, :].astype(F32) + self.r3[c, s, :].astype(F32)).astype(BF)

        self.blocks(body)
        self.across(c).start()

    def term(self, c, s, lanes):
        g0 = self.held(c, 0)
        return g0[s, lanes].astype(F32) + self.r1[c, s, lanes].astype(F32) + self.xr[c, s, lanes].astype(F32)

    def to_pair(self, c):
        self.from_core(c, 0).wait()
        self.across(c).wait()
        g0 = self.held(c, 0)

        def body(s):
            g0[s, self.other] = self.term(c, s, self.other).astype(BF)

        self.blocks(body)
        self.pair(c).start()

    def to_rest(self, c):
        self.pair(c).wait()
        g0 = self.held(c, 0)
        at = self.rows_of(0)
        self.own[c] = self.term(c, at, self.mine) + self.yr[c, at, :].astype(F32)

        def body(s):
            g0[s, self.mine] = (self.term(c, s, self.mine) + self.yr[c, s, :].astype(F32)).astype(BF)

        self.blocks(body)
        for k in range(1, self.half):
            self.rest(c, k).start()

    def to_back(self, c):
        total = self.own[c]
        for k in range(1, self.half):
            self.rest(c, k).wait()
            total = total + self.zr[c, k].astype(F32)
        self.xr[c, self.rows_of(0), self.mine] = total.astype(BF)
        for k in range(1, self.half):
            self.back(c, k).start()

    def to_back_pair(self, c):
        for k in range(1, self.half):
            self.back(c, k).wait()
        self.back_pair(c).start()

    def finish(self, c):
        self.back_pair(c).wait()

    def progress(self, plan, slot):
        steps = [None, self.to_chip, self.to_pair, self.to_rest, self.to_back, self.to_back_pair]
        for k in plan["order"]:
            since = slot - plan[k]
            c = lax.div(since, plan["gap"])
            due = since >= 0
            if plan["gap"] > 1:
                due = jnp.logical_and(due, lax.rem(since, plan["gap"]) == 0)

            @pl.when(jnp.logical_and(due, c < self.chunks))
            def _():
                steps[k](c)

    def finish_all(self):
        for c in range(self.chunks):
            self.finish(c)


class SmallSum:
    def __init__(self, me, half, sm, scratch):
        self.me, self.half, self.sm = me, half, sm
        self.got, self.z, self.s, self.r = scratch

    @staticmethod
    def scratch(rows, width, half):
        return [
            pltpu.VMEM((4, rows, width), F32),
            pltpu.VMEM((half, rows, width), F32),
            pltpu.SemaphoreType.DMA((4 + half,)),
            pltpu.SemaphoreType.DMA((4 + half,)),
        ]

    def copy(self, i):
        src, device = [(1, self.me.core), (3, self.me.core), (2, self.me.x), (0, self.me.y)][i]
        return remote(self.sm.at[src], self.got.at[i], self.s.at[i], self.r.at[i], device)

    def rest(self, k):
        return remote(self.sm.at[0], self.z.at[k], self.s.at[4 + k], self.r.at[4 + k], self.me.along(k, self.half))

    def start(self):
        self.copy(1).start()
        self.copy(0).start()

    def to_chip(self):
        self.copy(1).wait()
        self.sm[2] = self.sm[2] + self.got[1]
        self.copy(2).start()

    def to_pair(self):
        self.copy(0).wait()
        self.copy(2).wait()
        self.sm[0] = self.sm[0] + self.got[0] + self.got[2]
        self.copy(3).start()

    def to_rest(self):
        self.copy(3).wait()
        self.sm[0] = self.sm[0] + self.got[3]
        for k in range(1, self.half):
            self.rest(k).start()

    def finish(self):
        total = self.sm[0]
        for k in range(1, self.half):
            self.rest(k).wait()
            total = total + self.z[k]
        return total


SUB = 3
FFN_PLAN = {"gap": 2, "order": (5, 4, 3, 2, 1), 1: 6, 2: 12, 3: 15, 4: 18, 5: 21}
QKV_PLAN = {"gap": 2, "order": (5, 4, 3, 2, 1), 1: 24, 2: 30, 3: 33, 4: 36, 5: 39}
QKV_START = (21, 30)
SMALL_PLAN = (31, 34, 37, 40)
PROMPT_PLAN = (37,)
LAST_SLOT = 45


def back_kernel(half, grid_pairs, plen, conts, q_ref, kp_ref, vp_ref, ko_ref, vo_ref, lse_ref,
                w_any, an_any, anp_any, x_ref, px_any, ctx_ref, wp_any, wi_any, wo_any, wp_own, wi_own, wo_own, bias_ref,
                g1_ref, b_proj_ref, ln2_g_ref, ln2_b_ref, b_out_ref, dy_any,
                lo_any, ig_any, ffn_out, qkv_out, small_out,
                wbuf, wp_ref, l_s, dy, hid, gs, g0, g2,
                kx, vx, kt_s, acc, dqt, dkt, dvt, prompt_acc, own_acc, share_s, gq, sm, qv, sums,
                came, over, tail, w_s, f_s, p_s, p_r, o_s, *scratch):
    me = Peers()
    step = pl.program_id(0)
    rows = x_ref.shape[0]
    width = x_ref.shape[1]
    blocks = rows // CLEN
    prompt = kp_ref.shape[0]
    chunks = prompt // CLEN
    part = width // PIECES
    feats = grid_pairs // 2 * 128
    per = width // part
    ffn_scratch, qkv_scratch, small_scratch = scratch[:15], scratch[15:30], scratch[30:]
    branch, gmi, gel, gp, mlp, mlpt = prompt_acc, own_acc, gq.at[0], gq.at[1], gq.at[2], share_s.at[pl.ds(0, width)]
    an_ref = wbuf.at[pl.ds(0, rows)]
    anp_ref = wbuf.at[pl.ds(rows, prompt)]
    loads = [pltpu.make_async_copy(a, b, l_s.at[i]) for i, (a, b) in enumerate(((an_any, an_ref), (anp_any, anp_ref)))]

    def w_rows(j):
        return pl.ds(rows + prompt + j * feats, feats)

    def load_w(unit):
        return [
            pltpu.make_async_copy(w_any.at[j, pl.ds(unit * feats, feats)], wbuf.at[w_rows(j)], w_s.at[j]) for j in range(3)
        ]

    def ffn_rows(k, j):
        return pl.ds(pl.multiple_of((lax.rem(k, 2) * 2 + j) * width, 16), width)

    def load_ffn(k, own=False):
        srcs = (wi_own, wo_own) if own else [a.at[PIECES - 1 - k] for a in (wi_any, wo_any)]
        return [
            pltpu.make_async_copy(a, wbuf.at[ffn_rows(k, j)], f_s.at[lax.rem(k, 2), j]) for j, a in enumerate(srcs)
        ]

    px_parts = [(at, min(part, prompt - at)) for at in range(0, prompt, part)]
    load_px = [
        pltpu.make_async_copy(px_any.at[pl.ds(at, m)], gs.at[i, pl.ds(0, m)], l_s.at[4 + i]) for i, (at, m) in enumerate(px_parts)
    ]
    g1, b_proj, ln2_g, ln2_b, b_out = (flat(v) for v in (g1_ref, b_proj_ref, ln2_g_ref, ln2_b_ref, b_out_ref))

    def piece_rows(r):
        return pl.ds(pl.multiple_of(r * part, 16), part)

    ffn = Sums(me, half, lambda c, r: (g0 if r == 0 else g2).at[c], ffn_scratch)
    qkv = Sums(me, half, lambda c, r: gq.at[c, piece_rows(r)], qkv_scratch)
    smalls = SmallSum(me, half, sm, small_scratch)
    n = prompt // 2
    spare = rows - n
    mine = pl.ds(pl.multiple_of(me.odd * n, 16), n)
    side = remote(share_s.at[pl.ds(pl.multiple_of((1 - me.odd) * n, 16), n)], came, p_s.at[0], p_r.at[0], me.core)
    across = remote(share_s.at[mine], over, p_s.at[1], p_r.at[1], me.x)
    end = remote(share_s.at[pl.ds(pl.multiple_of(me.odd * n, 16), spare)], tail, p_s.at[2], p_r.at[2], me.core)

    def block_rows(b):
        return slice(b * CLEN, (b + 1) * CLEN)

    def normal_of(x):
        x = x - jnp.mean(x, axis=-1, keepdims=True)
        scale = lax.rsqrt(jnp.mean(x * x, axis=-1, keepdims=True) + EPS)
        return x * scale, scale

    def norm_back(e, normal, scale):
        return scale * (e - jnp.mean(e, axis=-1, keepdims=True) - normal * jnp.mean(e * normal, axis=-1, keepdims=True))

    @pl.when(step == 0)
    def _():
        got = pltpu.make_async_copy(dy_any, dy, o_s.at[0])
        first = pl.ds(0, part)
        rest = pl.ds(part, width - part)
        wp = [
            pltpu.make_async_copy(wp_own, wp_ref.at[first], l_s.at[2]),
            pltpu.make_async_copy(wp_any.at[rest], wp_ref.at[rest], l_s.at[3]),
        ]
        for c in wp:
            c.start()
        got.start()
        for c in load_ffn(0) + load_ffn(1):
            c.start()
        enter([me.core, me.x, me.y] + [me.along(k, half) for k in range(1, half)])
        for c in wp:
            c.wait()
        for b in range(blocks):
            at = block_rows(b)
            h = x_ref[at, :].astype(F32) + nn(ctx_ref[at, :], wp_ref[...]) + b_proj
            hid[at, :] = h
            normal, _ = normal_of(h)
            m = (normal * ln2_g + ln2_b).astype(BF)
            mlp[at, :] = m
            mlpt[:, at] = transposed(m).astype(BF)
        got.wait()
        branch[...] = jnp.zeros_like(branch)
        gmi[...] = jnp.zeros_like(gmi)
        sums[...] = jnp.zeros_like(sums)

    def ffn_block(b):
        at = pl.ds(pl.multiple_of(b * CLEN, CLEN), CLEN)
        r = PIECES - 1 - step
        wi = wbuf[ffn_rows(step, 0), :]
        wo = wbuf[ffn_rows(step, 1), :]
        pre = nn(mlp[at, :], wi) + bias_ref[r, 16:17, :].astype(F32)
        cdf = 0.5 * (1.0 + lax.erf(pre * (0.5**0.5)))
        pdf = jnp.exp(-0.5 * pre * pre) * 0.3989422804014327
        g = (pre * cdf).astype(BF)
        d = (nt(dy[at, :], wo) * (cdf + pre * pdf)).astype(BF)
        gel[at, :] = g
        gp[at, :] = d
        branch[at, :] += nn(g, wo)
        gmi[at, :] += nt(d, wi)
        sums[pl.ds(r, 1), :] += jnp.sum(d.astype(F32), axis=0, keepdims=True)

    def weight_grads():
        @pl.when(step == 2)
        def _():
            for c in range(2 * per):
                ffn.from_core(c, 1, gs.at[c]).wait_send()

        def one(j, _):
            two = pl.ds(pl.multiple_of(j * 2 * part, 128), 2 * part)
            both = (nn(mlpt[two, :], gp[...]), tn(gel[:, two], dy[...]))
            for k, got in enumerate(both):
                got = got.astype(BF).reshape(2, part, width)
                spot = pl.ds(2 * j + k * per, 2)

                @pl.when(lax.rem(step, 2) == 0)
                def _():
                    gs[spot] = got

                @pl.when(step == 1)
                def _():
                    g2[spot] = got

                @pl.when(step == 3)
                def _():
                    g0[spot] = got

            return 0

        lax.fori_loop(0, per // 2, one, 0)
        for at, i in ((0, 1), (2, 0)):
            @pl.when(step == at)
            def _():
                for c in range(2 * per):
                    ffn.start(c, i, gs.at[c])

    def after_ffn():
        for b in range(blocks):
            at = block_rows(b)
            g = gmi[at, :]
            h = hid[at, :]
            d = dy[at, :].astype(F32)
            normal, scale = normal_of(h)
            mlp[at, :] = (h + (branch[at, :] + b_out)).astype(BF)
            gh = d + norm_back(g * ln2_g, normal, scale)
            hid[at, :] = gh
            ga = gh.astype(BF)
            gel[at, :] = ga
            for k, v in enumerate((ga.astype(F32), g * normal, g, d)):
                sums[PIECES + k : PIECES + k + 1, :] += jnp.sum(v, axis=0, keepdims=True)
            dy[at, :] = nt(ga, wp_ref[...]).astype(BF)
        for c in loads + load_w(1):
            c.start()
        spots = (g0.at[2 * per], gs.at[2 * per + 1], g2.at[2 * per], gs.at[2 * per])
        for r in range(0, PIECES, 2):
            got = tn(ctx_ref[:, r * part : (r + 2) * part], gel[...]).astype(BF)
            spots[r][...] = got[:part]
            spots[r + 1][...] = got[part:]
        ffn.start(2 * per, 1, gs.at[2 * per])
        ffn.start(2 * per, 0, gs.at[2 * per + 1])
        pltpu.make_async_copy(mlp, lo_any, o_s.at[1]).start()
        own_acc[...] = jnp.zeros_like(own_acc)
        prompt_acc[...] = jnp.zeros_like(prompt_acc)

    sp = step - PIECES
    spot = lax.rem(jnp.maximum(sp, 0), grid_pairs // 2)
    pair = lax.rem(jnp.maximum(sp, 0) + grid_pairs // 2, grid_pairs)
    lanes = pl.ds(pl.multiple_of(pair * 128, 128), 128)
    attending = jnp.logical_and(sp >= 0, sp < grid_pairs)

    @pl.when(attending)
    def _():
        acc[...] = jnp.zeros_like(acc)
        kx[:prompt] = wide_keys(kp_ref[...], plen[0], 0)
        vx[:prompt] = wide_values(vp_ref[...])
        vx[prompt:] = wide_values(vo_ref[...])
        kt_s[:, :prompt] = transposed(kp_ref[...]).astype(BF)
        kt_s[:, prompt:] = transposed(ko_ref[...]).astype(BF)
        for b in range(blocks):
            at = block_rows(b)
            kx[prompt + b * CLEN : prompt + (b + 1) * CLEN] = wide_keys(ko_ref[at, :], own_length(conts, me.t, blocks, b), 0)

    def block(b):
        at = pl.ds(pl.multiple_of(b * CLEN, CLEN), CLEN)
        own = pl.ds(pl.multiple_of(prompt + b * CLEN, CLEN), CLEN)
        q = q_ref[at, :]
        do = dy[at, lanes]
        q2 = wide_queries(q)
        do2 = wide_grads(do, ctx_ref[at, lanes])
        qt = transposed(q).astype(BF)
        dot = transposed(do).astype(BF)
        logs = jnp.concatenate([lse_ref[0, b, 0:1, :], lse_ref[0, b, 1:2, :]], axis=1)

        def scores(keys):
            p = jnp.exp(nt(kx[keys, :], q2) - logs)
            ds = (p * nt(vx[keys, :], do2)).astype(BF)
            p = p.astype(BF)
            parts = []
            for left, m in ((qt, ds), (dot, p)):
                parts.append([nt(left[64 * h : 64 * h + 64], m[:, h * CLEN : (h + 1) * CLEN]) for h in range(2)])
            return parts, nn(kt_s[:, keys], ds)

        (dk, dv), dq = scores(pl.ds(0, prompt))
        for h in range(2):
            rows_h = slice(64 * h, 64 * h + 64)
            acc[0, rows_h, :] += dk[h]
            acc[1, rows_h, :] += dv[h]
        (dk, dv), dq_own = scores(own)
        dkt[spot, :, own] = (jnp.concatenate(dk, axis=0) * 0.125).astype(BF)
        dvt[spot, :, own] = jnp.concatenate(dv, axis=0).astype(BF)
        dq = dq + dq_own
        dqt[spot, :, at] = (jnp.concatenate([dq[:64, :CLEN], dq[64:, CLEN:]], axis=0) * 0.125).astype(BF)

        @pl.when(b == blocks - 1)
        def _():
            dkt[spot, :, :prompt] = (acc[0] * 0.125).astype(BF)
            dvt[spot, :, :prompt] = acc[1].astype(BF)

    def sub_step(sub, _):
        slot = step * SUB + sub
        ffn.progress(FFN_PLAN, slot)

        def at(k, body):
            @pl.when(slot == k)
            def _():
                body()

        def qkv_start(i):
            for c in range(3):
                qkv.start(c, i, gq.at[c, piece_rows(1 + 2 * i)])

        def prompt_chip():
            side.wait()
            share_s[mine, :] = (share_s[mine, :].astype(F32) + came[...].astype(F32)).astype(BF)

            @pl.when(me.t >= 2)
            def _():
                across.start()

        def qkv_sent():
            for c in range(3):
                qkv.from_core(c, 1, gq.at[c, piece_rows(3)]).wait_send()

        at(QKV_START[0], lambda: qkv_start(1))
        at(QKV_START[1], lambda: qkv_start(0))
        at(QKV_START[1], qkv_sent)
        qkv.progress(QKV_PLAN, slot)
        at(SMALL_PLAN[0], smalls.start)
        at(SMALL_PLAN[1], smalls.to_chip)
        at(SMALL_PLAN[2], smalls.to_pair)
        at(SMALL_PLAN[3], smalls.to_rest)
        at(PROMPT_PLAN[0], prompt_chip)

        @pl.when(step < PIECES)
        def _():
            ffn_block(sub)

        @pl.when(attending)
        def _():
            block(sub)

        return 0

    @pl.when(step < PIECES)
    def _():
        for c in load_ffn(step, True):
            c.wait()

    lax.fori_loop(0, SUB, sub_step, 0)

    @pl.when(step < PIECES)
    def _():
        @pl.when(step == 0)
        def _():
            for c in load_ffn(2):
                c.start()

        @pl.when(step == 1)
        def _():
            for c in load_ffn(3, True):
                c.start()

        weight_grads()

    @pl.when(step == PIECES - 1)
    def _():
        after_ffn()

    @pl.when(jnp.logical_and(attending, spot == grid_pairs // 2 - 1))
    def _():
        late = sp < grid_pairs // 2

        @pl.when(late)
        def _():
            for c in loads + [pltpu.make_async_copy(mlp, lo_any, o_s.at[1])]:
                c.wait()

        for c in load_w(0):
            c.wait()
        dq, dk, dv = (r[...].reshape(feats, -1) for r in (dqt, dkt, dvt))
        an = an_ref[...]
        anp = anp_ref[...]
        for j, d in enumerate((dq, dk, dv)):
            g = nn(d, an) if j == 0 else nn(d[:, prompt:], an) + nn(d[:, :prompt], anp)
            gq[j, pl.ds(pl.multiple_of(jnp.where(late, feats, 0), 16), feats), :] = g.astype(BF)
        sum_q = jnp.sum(dq.astype(F32), axis=1, keepdims=True)
        sum_v = jnp.sum(dv.astype(F32), axis=1, keepdims=True)
        both = jnp.concatenate([jnp.broadcast_to(sum_q, (feats, 128)), jnp.broadcast_to(sum_v, (feats, 128))], axis=1).T
        unit_lanes = pl.ds(pl.multiple_of(jnp.where(late, feats, 0), 128), feats)
        qv[0:1, unit_lanes] = both[0:1]
        qv[1:2, unit_lanes] = both[128:129]
        def turned(ref, at, j):
            return tn(ref[:, :, at : at + CLEN].reshape(feats, CLEN), wbuf[w_rows(j), :])

        for b in range(blocks):
            at = b * CLEN
            own_acc[at : at + CLEN, :] += (
                turned(dqt, at, 0) + turned(dkt, prompt + at, 1) + turned(dvt, prompt + at, 2)
            )
        for c in range(chunks):
            at = c * CLEN
            prompt_acc[at : at + CLEN, :] += turned(dkt, at, 1) + turned(dvt, at, 2)

        @pl.when(late)
        def _():
            for c in load_w(0):
                c.start()

        @pl.when(jnp.logical_not(late))
        def _():
            for c in load_px:
                c.start()

    @pl.when(sp == grid_pairs - 1)
    def _():
        for c in range(chunks):
            at = block_rows(c)
            share_s[at, :] = prompt_acc[at, :].astype(BF)
        side.start()
        sum_g = jnp.zeros((1, width), F32)
        sum_c = jnp.zeros((1, width), F32)
        raws = [(own_acc, at, m, x_ref.at[pl.ds(at, m)]) for at, m in [(part * k, part) for k in range(rows // part)]]
        raws += [(prompt_acc, at, m, gs.at[i, pl.ds(0, m)]) for i, (at, m) in enumerate(px_parts)]
        for i, (grad, at, m, raw) in enumerate(raws):
            if grad is prompt_acc:
                load_px[i - rows // part].wait()
            normal, _ = normal_of(raw[...].astype(F32))
            g = grad[at : at + m, :]
            sum_g = sum_g + jnp.sum(g * normal, axis=0, keepdims=True)
            sum_c = sum_c + jnp.sum(g, axis=0, keepdims=True)
        for r in range(PIECES):
            sm[r] = jnp.zeros_like(sm[r])
            sm[r, 0:1, :] = sums[r : r + 1, :]
            sm[r, 1:5, :] = sums[PIECES : PIECES + 4, :]
            for i in range(2):
                row = qv[i : i + 1, :]
                sm[r, 8 + i : 9 + i, :] = row if r == 0 else pltpu.roll(row, width - r * part, 1)
            sm[r, 10:11, :] = sum_g
            sm[r, 11:12, :] = sum_c

    @pl.when(step == pl.num_programs(0) - 1)
    def _():
        ffn.finish_all()
        qkv.finish_all()
        outs = [(ffn.xr, ffn_out), (qkv.xr, qkv_out)]
        copies = [pltpu.make_async_copy(a, b, o_s.at[2 + i]) for i, (a, b) in enumerate(outs)]
        for c in copies:
            c.start()
        small_out[...] = smalls.finish()
        ffn.from_core(2 * per, 1, gs.at[2 * per]).wait_send()

        @pl.when(me.t >= 2)
        def _():
            across.wait_send()

        @pl.when(me.t < 2)
        def _():
            across.wait_recv()
            share_s[mine, :] = (share_s[mine, :].astype(F32) + over[...].astype(F32)).astype(BF)

        @pl.when(me.t == 1)
        def _():
            end.start()
            for at in range(0, n - spare, CLEN):
                own_acc[at : at + CLEN, :] += share_s[n + spare + at : n + spare + at + CLEN, :].astype(F32)
            end.wait_send()

        @pl.when(me.t == 0)
        def _():
            for at in range(0, n, CLEN):
                own_acc[at : at + CLEN, :] += share_s[at : at + CLEN, :].astype(F32)
            end.wait_recv()
            own_acc[n:, :] += tail[...].astype(F32)

        for b in range(blocks):
            at = block_rows(b)
            normal, scale = normal_of(x_ref[at, :].astype(F32))
            hid[at, :] += norm_back(own_acc[at, :] * g1, normal, scale)
        last = pltpu.make_async_copy(hid, ig_any, o_s.at[0])
        last.start()
        for c in copies + [last]:
            c.wait()


def back_call(plen, conts, q, kp, vp, ko, vo, lse, wq_all, an, anp, x, px, ctx, wp, wi_all, wo_all, wp_own, wi_own, wo_own, ws_all, vecs, dy):
    rows, width = q.shape
    prompt = kp.shape[0]
    blocks = rows // CLEN
    pairs = width // 128
    part = width // PIECES
    half = min(lax.axis_size("dp"), NEAR) // 2
    cells = rows * (prompt + CLEN) * pairs * 2
    n_ffn = 2 * (width // part) + 1
    steps = -(-LAST_SLOT // SUB)
    assert blocks == SUB and wi_all.shape[1:] == (width, width) and rows == width and part % (16 * half) == 0
    small_n = 16

    def pair(i):
        return lax.rem(jnp.clip(i - PIECES, 0, pairs - 1) + pairs // 2, pairs)

    def col(n):
        return pl.BlockSpec((n, 128), lambda i, *l: (0, pair(i)))

    def whole(*s):
        return pl.BlockSpec(s, lambda i, *l: (0,) * len(s), pipeline_mode=pl.Buffered(1))

    r, p = col(rows), col(prompt)
    logs = pl.BlockSpec((1, blocks, 8, CLEN), lambda i, *l: (pair(i), 0, 0, 0))
    return pl.pallas_call(
        functools.partial(back_kernel, half, pairs),
        out_shape=(
            jax.ShapeDtypeStruct((rows, width), BF),
            jax.ShapeDtypeStruct((rows, width), F32),
            jax.ShapeDtypeStruct((n_ffn, part, width), BF),
            jax.ShapeDtypeStruct((3, part, width), BF),
            jax.ShapeDtypeStruct((small_n, width), F32),
        ),
        grid_spec=pltpu.PrefetchScalarGridSpec(
            num_scalar_prefetch=2,
            grid=(steps,),
            in_specs=[r, p, p, r, r, logs, ANY, ANY, ANY, whole(rows, width),
                      ANY, whole(rows, width)] + [ANY] * 6 + [whole(*ws_all.shape)] + [whole(width)] * 5 + [ANY],
            out_specs=[ANY, ANY, ANY, ANY, pl.BlockSpec((small_n, width), lambda i, *l: (0, 0))],
            scratch_shapes=[
                pltpu.VMEM((max(4 * width, rows + prompt + 3 * pairs // 2 * 128), width), BF),
                pltpu.VMEM((width, width), BF),
                pltpu.SemaphoreType.DMA((4 + -(-prompt // part),)),
                pltpu.VMEM((rows, width), BF),
                pltpu.VMEM((rows, width), F32),
                pltpu.VMEM((n_ffn + 1, part, width), BF),
                pltpu.VMEM((n_ffn, part, width), BF),
                pltpu.VMEM((n_ffn, part, width), BF),
                pltpu.VMEM((prompt + rows, 256), BF),
                pltpu.VMEM((prompt + rows, 256), BF),
                pltpu.VMEM((128, prompt + rows), BF),
                pltpu.VMEM((2, 128, prompt), F32),
                pltpu.VMEM((pairs // 2, 128, rows), BF),
                pltpu.VMEM((pairs // 2, 128, prompt + rows), BF),
                pltpu.VMEM((pairs // 2, 128, prompt + rows), BF),
                pltpu.VMEM((prompt, width), F32),
                pltpu.VMEM((rows, width), F32),
                pltpu.VMEM((prompt, width), BF),
                pltpu.VMEM((3, width, width), BF),
                pltpu.VMEM((PIECES, small_n, width), F32),
                pltpu.VMEM((8, width), F32),
                pltpu.VMEM((8, width), F32),
                pltpu.VMEM((prompt // 2, width), BF),
                pltpu.VMEM((prompt // 2, width), BF),
                pltpu.VMEM((rows - prompt // 2, width), BF),
                pltpu.SemaphoreType.DMA((3,)),
                pltpu.SemaphoreType.DMA((2, 2)),
                pltpu.SemaphoreType.DMA((3,)),
                pltpu.SemaphoreType.DMA((3,)),
                pltpu.SemaphoreType.DMA((4,)),
            ]
            + Sums.scratch(n_ffn, part, width, half)
            + Sums.scratch(3, part, width, half)
            + SmallSum.scratch(small_n, width, half),
        ),
        compiler_params=pltpu.CompilerParams(collective_id=1, has_side_effects=True, vmem_limit_bytes=63 << 20),
        cost_estimate=pl.CostEstimate(flops=cells * 256 * 10, transcendentals=cells, bytes_accessed=16 << 20),
        name="back",
    )(plen, conts, q, kp, vp, ko, vo, lse, wq_all, an, anp, x, px, ctx, wp, wi_all, wo_all, wp_own, wi_own, wo_own, ws_all, *vecs, dy)


def shards(layer_in, prompt_len, cont_len, w_qkv, b_qv, w_proj, b_proj, ln1_gain, ln1_bias,
           ln2_gain, ln2_bias, w_in, b_in, w_out, b_out, out_grad):
    rows, width = layer_in.shape
    part = w_qkv.shape[2]
    (q, kp, vp, ko, vo, ctx, lse, attn_input, prompt_input, prompt_rows, wq_all, wp_all, wi_all, wo_all, ws_all) = front_call(
        prompt_len, cont_len, layer_in, ln1_gain, ln1_bias, b_qv, b_in, w_qkv.transpose(0, 2, 1), w_proj, w_in, w_out
    )
    layer_out, in_grad, ffn, qkv, small = back_call(
        prompt_len, cont_len, q, kp, vp, ko, vo, lse, wq_all, attn_input, prompt_input, layer_in, prompt_rows, ctx,
        wp_all.reshape(width, width), wi_all, wo_all, w_proj, w_in, w_out, ws_all,
        (ln1_gain, b_proj, ln2_gain, ln2_bias, b_out), out_grad
    )
    ffn = beyond(ffn.astype(F32))
    qkv = beyond(qkv.astype(F32))
    small = beyond(small)
    per = ffn.shape[0] // 2
    grad_w_in = ffn[:per].reshape(width, -1)
    grad_w_out = ffn[per : 2 * per].reshape(-1, width)
    return (layer_out, in_grad, qkv.transpose(0, 2, 1), small[8:10, :part], ffn[2 * per], small[1], small[10], small[11],
            small[2], small[3], grad_w_in, small[0, : w_in.shape[1]], grad_w_out, small[4])


def solution(mesh):
    in_specs = (
        P(("dp", "tensor"), None),
        P("dp"),
        P("dp", None),
        P(None, None, "tensor"),
        P(None, "tensor"),
        P("tensor", None),
        P(),
        P(),
        P(),
        P(),
        P(),
        P(None, "tensor"),
        P("tensor"),
        P("tensor", None),
        P(),
        P(("dp", "tensor"), None),
    )
    out_specs = (
        P(("dp", "tensor"), None),
        P(("dp", "tensor"), None),
        P(None, None, "tensor"),
        P(None, "tensor"),
        P("tensor", None),
        P(),
        P(),
        P(),
        P(),
        P(),
        P(None, "tensor"),
        P("tensor"),
        P("tensor", None),
        P(),
    )
    return jax.shard_map(shards, mesh=mesh, in_specs=in_specs, out_specs=out_specs, check_vma=False)
```

```python
import functools

import jax
import jax.numpy as jnp
from jax import lax
from jax.experimental import pallas as pl
from jax.experimental.pallas import tpu as pltpu
from jax.sharding import PartitionSpec as P

HEAD = 64
PROMPT = 1024
CONT = 8
CLEN = 256
PIECES = 4
MESH = pl.DeviceIdType.MESH
ANY = pl.BlockSpec(memory_space=pl.ANY)

EPS = 1e-06
MASKED = -1000000000.0
BF = jnp.bfloat16
F32 = jnp.float32


def nt(a, b):
    return lax.dot_general(a, b, (((1,), (1,)), ((), ())), preferred_element_type=F32)


def nn(a, b):
    return lax.dot_general(a, b, (((1,), (0,)), ((), ())), preferred_element_type=F32)


def tn(a, b):
    return lax.dot_general(a, b, (((0,), (0,)), ((), ())), preferred_element_type=F32)


NEAR = 8


class Peers:
    def __init__(self):
        self.t = lax.axis_index("tensor")
        self.d = lax.axis_index("dp")
        self.odd = lax.rem(self.t, 2)
        self.p = lax.rem(self.d, 2)
        self.z = lax.div(lax.rem(self.d, NEAR), 2)
        self.base = self.d - lax.rem(self.d, NEAR)
        self.core = {"tensor": self.t + 1 - 2 * self.odd}
        self.x = {"tensor": lax.rem(self.t + 2, 4)}
        self.y = {"dp": self.d + 1 - 2 * self.p}

    def along(self, k, count):
        return {"dp": self.base + lax.rem(self.z + k, count) * 2 + self.p}


def enter(devices):
    barrier = pltpu.get_barrier_semaphore()
    for device in devices:
        pl.semaphore_signal(barrier, inc=1, device_id=device, device_id_type=MESH)
    pl.semaphore_wait(barrier, len(devices))


def remote(src, dst, send, recv, device):
    return pltpu.make_async_remote_copy(
        src_ref=src, dst_ref=dst, send_sem=send, recv_sem=recv, device_id=device, device_id_type=MESH
    )


def beyond(value):
    size = lax.axis_size("dp")
    step = NEAR
    while step < size:
        value = value + lax.ppermute(value, "dp", [(i, i ^ step) for i in range(size)])
        step *= 2
    return value


def own_lanes(rows, h):
    lane = lax.broadcasted_iota(jnp.int32, (rows, 128), 1)
    return ((lane < 64) if h == 0 else (lane >= 64)), lane - (64 if h == 0 else 0)


def key_aug(k, h, length, base):
    rows = k.shape[0]
    own, extra = own_lanes(rows, h)
    row = lax.broadcasted_iota(jnp.int32, (rows, 128), 0) + base
    bias = jnp.where(jnp.logical_and(extra == 0, row >= length), MASKED, 0.0)
    return jnp.where(own, k.astype(F32), bias).astype(BF)


def query_aug(q, h):
    own, extra = own_lanes(q.shape[0], h)
    return jnp.where(own, q.astype(F32) * 0.125, jnp.where(extra == 0, 1.0, 0.0)).astype(BF)


def value_aug(v, h):
    own, extra = own_lanes(v.shape[0], h)
    ones = jnp.where(jnp.logical_and(extra >= 0, extra < 3), 1.0, 0.0)
    return jnp.where(own, v.astype(F32), ones).astype(BF)


def transposed(v):
    return v.astype(F32).T


def wide_keys(k, length, base):
    rows = k.shape[0]
    lane = lax.broadcasted_iota(jnp.int32, (rows, 128), 1)
    row = lax.broadcasted_iota(jnp.int32, (rows, 128), 0) + base
    bias = jnp.where(jnp.logical_and(lane == 0, row >= length), MASKED, 0.0).astype(BF)
    return jnp.concatenate([k, bias], axis=1)


def wide_values(v):
    lane = lax.broadcasted_iota(jnp.int32, v.shape, 1)
    return jnp.concatenate([v, jnp.where(lane < 3, 1.0, 0.0).astype(BF)], axis=1)


def wide_queries(q):
    lane = lax.broadcasted_iota(jnp.int32, q.shape, 1)
    qf = q.astype(F32) * 0.125
    one = jnp.where(lane == 0, 1.0, 0.0)
    heads = [jnp.where(lane < 64, qf, 0.0), jnp.where(lane < 64, 0.0, qf)]
    return jnp.concatenate([jnp.concatenate([h, one], axis=1) for h in heads], axis=0).astype(BF)


def wide_grads(do, ctx):
    lane = lax.broadcasted_iota(jnp.int32, do.shape, 1)
    do = do.astype(F32)
    prod = do * ctx.astype(F32)
    out = []
    for h in range(2):
        mine = (lane < 64) if h == 0 else (lane >= 64)
        d = -jnp.sum(jnp.where(mine, prod, 0.0), axis=1, keepdims=True)
        hi = d.astype(BF).astype(F32)
        mid = (d - hi).astype(BF).astype(F32)
        low = d - hi - mid
        aug = jnp.where(lane == 0, hi, jnp.where(lane == 1, mid, jnp.where(lane == 2, low, 0.0)))
        out.append(jnp.concatenate([jnp.where(mine, do, 0.0), aug], axis=1))
    return jnp.concatenate(out, axis=0).astype(BF)


def attn_specs(rows, prompt, blocks):
    def col(n):
        return pl.BlockSpec((n, 128), lambda i, *l: (0, i))

    logs = pl.BlockSpec((1, blocks, 8, CLEN), lambda i, *l: (i, 0, 0, 0))
    return col(rows), col(prompt), logs

def own_length(conts, t, blocks, b):
    c = t * blocks + b - PROMPT // CLEN
    return jnp.where(c >= 0, conts[0, jnp.maximum(c, 0)], 0)


class Weight:
    def __init__(self, me, own, spots, view, sems, direct=False):
        self.me, self.own, self.spots, self.view, self.direct = me, own, spots, view, direct
        self.send, self.recv = sems

    def side(self):
        return remote(self.own, self.spots(1), self.send.at[0], self.recv.at[0], self.me.core)

    def across(self):
        p = self.me.p
        src, dst = (self.own, self.spots(2)) if self.direct else (self.view(None, p), self.view(2, p))
        return remote(src, dst, self.send.at[1], self.recv.at[1], self.me.x)

    def pair(self):
        p = self.me.p
        return remote(self.view(2, p), self.view(2, p), self.send.at[2], self.recv.at[2], self.me.y)

    def over(self, which):
        h = self.me.p if which == 0 else 1 - self.me.p
        src, dst = (self.spots(2), self.spots(3)) if self.direct else (self.view(2, h), self.view(3, h))
        return remote(src, dst, self.send.at[3 + which], self.recv.at[3 + which], self.me.core)

    def start(self):
        self.side().start()
        self.across().start()

    def relay(self):
        self.across().wait_recv()
        if not self.direct:
            self.pair().start()
        self.over(0).start()

    def relay_pair(self):
        self.pair().wait_recv()
        self.over(1).start()

    def finish(self):
        self.side().wait()
        self.across().wait_send()
        self.over(0).wait()
        if not self.direct:
            self.pair().wait_send()
            self.over(1).wait()


def norm_rows(x, gain, shift):
    x = x.astype(F32)
    centred = x - jnp.mean(x, axis=-1, keepdims=True)
    scale = lax.rsqrt(jnp.mean(centred * centred, axis=-1, keepdims=True) + EPS)
    return (centred * scale * gain + shift).astype(BF)


def flat(ref):
    return ref[...].astype(F32).reshape(1, ref.shape[0])


def front_kernel(plen, conts, x_ref, gain_ref, shift_ref, bqv_ref, bin_ref, wq, wp, wi, wo,
                 q_ref, kp_ref, vp_ref, ko_ref, vo_ref, ctx_ref, lse_ref, an_ref, anp_ref, px_ref,
                 wq_all, wp_all, wi_all, wo_all, ws_all,
                 px, wv, wsv, kph, vpt, px_s, px_r, send, recv, loc):
    me = Peers()
    step = pl.program_id(0)
    rows = x_ref.shape[0]
    blocks = rows // CLEN
    prompt = px.shape[0]
    part = wq.shape[1]
    own_chunks = rows // CLEN
    chunks = prompt // CLEN

    def qkv_view(r, h):
        n = part // 2
        if r is None:
            return wq.at[:, pl.ds(h * n, n)]
        return wv.at[:, pl.ds(r * part + h * n, n)]

    def plain(own, everything):
        n = own.shape[0] // 2

        def view(r, h):
            return own.at[pl.ds(h * n, n)] if r is None else everything.at[r, pl.ds(h * n, n)]

        return view

    def weight(i, own, everything):
        return Weight(me, own, lambda r: everything.at[r], plain(own, everything), (send.at[i], recv.at[i]))

    w_qkv = Weight(me, wq, lambda r: wv.at[:, pl.ds(r * part, part)], qkv_view, (send.at[0], recv.at[0]))
    w_small = weight(1, wsv.at[0], wsv)
    w_proj = weight(2, wp, wp_all)
    half_in = wi.shape[0] // 2
    half_out = wo.shape[0] // 2

    def rows_of(i, own, everything, first, n, direct=False):
        part_rows = pl.ds(first, n)
        sub = n // 2

        def view(r, h):
            at = pl.ds(first + h * sub, sub)
            return own.at[at] if r is None else everything.at[r, at]

        return Weight(me, own.at[part_rows], lambda r: everything.at[r, part_rows], view, (send.at[i], recv.at[i]), direct)

    in_a = rows_of(3, wi, wi_all, 0, half_in)
    in_b = rows_of(4, wi, wi_all, half_in, half_in)
    out_a = rows_of(5, wo, wo_all, 0, half_out)
    out_b = rows_of(6, wo, wo_all, half_out, half_out, True)
    later = [w_proj, in_a, in_b, out_a, out_b]

    def keep(own, spot, i):
        return pltpu.make_async_copy(own, spot, loc.at[i])

    mine = [keep(wq, wv.at[:, pl.ds(0, part)], 0), keep(wv, wq_all, 1), keep(wsv, ws_all, 2), keep(px, px_ref, 3)]

    def chunk(k):
        return px.at[pl.ds(k * CLEN, CLEN)]

    def held(k):
        at = k if k < own_chunks else k - own_chunks
        return x_ref.at[pl.ds(at * CLEN, CLEN)]

    def hop(k, src, n, device):
        return remote(src, chunk(k), px_s.at[n, k], px_r.at[n, k], device)

    first = [k for k in range(chunks) if k < own_chunks]
    second = [k for k in range(chunks) if k >= own_chunks]
    low = [k for k in range(chunks) if k < chunks // 2]
    high = second + [k for k in range(chunks // 2, own_chunks)]

    def normed(k):
        anp_ref[k * CLEN : (k + 1) * CLEN, :] = norm_rows(px[k * CLEN : (k + 1) * CLEN, :], flat(gain_ref), flat(shift_ref))

    @pl.when(step == 0)
    def _():
        enter([me.core, me.x, me.y])

        @pl.when(me.t == 0)
        def _():
            for k in low:
                hop(k, held(k), 1, me.x).start()
            for k in reversed(first):
                hop(k, held(k), 0, me.core).start()

        @pl.when(me.t == 1)
        def _():
            for k in second:
                hop(k, held(k), 1, me.x).start()
                hop(k, held(k), 0, me.core).start()

        spot = lax.broadcasted_iota(jnp.int32, wsv.shape[1:], 0)
        table = jnp.where(spot == 16, flat(bin_ref), 0.0)
        width = wsv.shape[2]
        for i in range(2):
            row = jnp.concatenate([bqv_ref[i : i + 1, :].astype(F32), jnp.zeros((1, width - part), F32)], axis=1)
            for r in range(PIECES):
                moved = pltpu.roll(row, r * part, 1) if r else row
                table = jnp.where(spot == i * PIECES + r, moved, table)
        wsv[0] = table.astype(BF)
        for w in (w_qkv, w_small):
            w.side().start()
        mine[0].start()

        @pl.when(me.t >= 2)
        def _():
            for w in (w_qkv, w_small):
                w.across().start()

        @pl.when(me.t == 1)
        def _():
            for k in reversed(first):
                hop(k, held(k), 0, me.core).wait_recv()
                if k in high:
                    hop(k, chunk(k), 1, me.x).start()

        for w in later:
            w.side().start()
        for b in range(blocks):
            an_ref[b * CLEN : (b + 1) * CLEN, :] = norm_rows(x_ref[b * CLEN : (b + 1) * CLEN, :], flat(gain_ref), flat(shift_ref))

        @pl.when(me.t == 0)
        def _():
            for k in first:
                px[k * CLEN : (k + 1) * CLEN, :] = x_ref[k * CLEN : (k + 1) * CLEN, :]
            for k in second:
                hop(k, held(k), 0, me.core).wait_recv()
            for k in first:
                hop(k, held(k), 0, me.core).wait_send()
            for k in low:
                hop(k, held(k), 1, me.x).wait_send()

        @pl.when(me.t == 1)
        def _():
            for k in second:
                px[k * CLEN : (k + 1) * CLEN, :] = held(k)[...]
                hop(k, held(k), 0, me.core).wait_send()
            for k in high:
                hop(k, chunk(k), 1, me.x).wait_send()

        @pl.when(me.t == 2)
        def _():
            for k in low:
                hop(k, chunk(k), 1, me.x).wait_recv()
                hop(k, chunk(k), 0, me.core).start()
            for k in high:
                hop(k, chunk(k), 0, me.core).wait_recv()
            for k in low:
                hop(k, chunk(k), 0, me.core).wait_send()

        @pl.when(me.t == 3)
        def _():
            for k in high:
                hop(k, chunk(k), 1, me.x).wait_recv()
                hop(k, chunk(k), 0, me.core).start()
            for k in low:
                hop(k, chunk(k), 0, me.core).wait_recv()
            for k in high:
                hop(k, chunk(k), 0, me.core).wait_send()

        @pl.when(me.t < 2)
        def _():
            for w in (w_qkv, w_small):
                w.across().start()

        for k in range(chunks):
            normed(k)
        for w in (w_qkv, w_small):
            w.side().wait_recv()
        mine[0].wait()

    @pl.when(step == 3)
    def _():
        for w in (w_qkv, w_small):
            w.over(0).wait_recv()
            w.over(1).wait_recv()
        for i in range(1, 4):
            mine[i].start()

    def moves(slot):
        def at(k, *steps):
            @pl.when(slot == k)
            def _():
                for s in steps:
                    s()

        def go(w):
            return lambda: w.across().start()

        at(1, w_small.relay, w_qkv.relay, go(w_proj), go(in_a))
        at(4, w_proj.relay, go(in_b))
        at(6, w_qkv.relay_pair, w_small.relay_pair)
        at(7, in_a.relay, go(out_a))
        at(9, w_proj.relay_pair)
        at(11, in_b.relay, go(out_b))
        at(13, in_a.relay_pair)
        at(14, out_a.relay)
        at(16, in_b.relay_pair)

    pick = pl.ds(pl.multiple_of(step * 128, 128), 128)
    w3 = jnp.concatenate([wv[0, pick], wv[1, pick], wv[2, pick]], axis=0)
    u = 2 * lax.div(step, 3)
    left = wsv[u, :16, pick].astype(F32)
    right = wsv[u + 1, :16, pick].astype(F32)
    spot = lax.broadcasted_iota(jnp.int32, left.shape, 0)

    def bias(k):
        return jnp.sum(jnp.where(spot == u + k, left, 0.0) + jnp.where(spot == u + 1 + k, right, 0.0), axis=0, keepdims=True)

    bq = bias(0)
    bv = bias(PIECES)
    for b in range(blocks):
        at = slice(b * CLEN, (b + 1) * CLEN)
        got = nt(an_ref[at, :], w3)
        q_ref[at, :] = (got[:, :128] + bq).astype(BF)
        ko_ref[at, :] = got[:, 128:256].astype(BF)
        vo_ref[at, :] = (got[:, 256:] + bv).astype(BF)
    for c in range(chunks):
        at = slice(c * CLEN, (c + 1) * CLEN)
        got = nt(anp_ref[at, :], w3[128:])
        kp_ref[at, :] = got[:, :128].astype(BF)
        vp_ref[at, :] = (got[:, 128:] + bv).astype(BF)

    kph[...] = wide_keys(kp_ref[...], plen[0], 0)
    ones = jnp.ones((16, prompt), BF)
    vpt[...] = jnp.concatenate([transposed(vp_ref[...]).astype(BF), ones], axis=0)

    def block(b, _):
        moves(step * blocks + b)
        at = pl.ds(pl.multiple_of(b * CLEN, CLEN), CLEN)
        q2 = wide_queries(q_ref[at, :])
        vot = jnp.concatenate([transposed(vo_ref[at, :]).astype(BF), ones[:, :CLEN]], axis=0)
        sp = nt(kph[...], q2)
        so = nt(wide_keys(ko_ref[at, :], own_length(conts, me.t, blocks, b), 0), q2)
        top = jnp.maximum(jnp.max(sp, axis=0, keepdims=True), jnp.max(so, axis=0, keepdims=True))
        pp = jnp.exp(sp - top).astype(BF)
        po = jnp.exp(so - top).astype(BF)
        ot = nn(vpt[...], pp) + nn(vot, po)
        total = ot[128:129]
        ot = ot[:128] * (1.0 / total)
        logs = top + jnp.log(total)
        ctx_ref[at, :] = jnp.concatenate([ot[:64, :CLEN], ot[64:, CLEN:]], axis=0).T.astype(BF)
        lse_ref[0, b] = jnp.concatenate([logs[:, :CLEN], logs[:, CLEN:], jnp.zeros((6, CLEN), F32)], axis=0)
        return 0

    lax.fori_loop(0, blocks, block, 0)

    @pl.when(step == pl.num_programs(0) - 1)
    def _():
        out_b.relay()
        out_a.relay_pair()
        for w in [w_qkv, w_small]:
            w.side().wait_send()
            w.across().wait_send()
            w.pair().wait_send()
            w.over(0).wait_send()
            w.over(1).wait_send()
        for w in later:
            w.finish()
        for i in range(1, 4):
            mine[i].wait()


def front_call(plen, conts, x, gain, shift, bqv, b_in, wq, wp, wi, wo):
    rows, width = x.shape
    blocks = rows // CLEN
    pairs = width // 128
    r, p, logs = attn_specs(rows, PROMPT, blocks)
    cells = rows * (PROMPT + CLEN) * pairs * 2

    def whole(n):
        return pl.BlockSpec((n, width), lambda i, *l: (0, 0))

    def shape(*s):
        return jax.ShapeDtypeStruct(s, BF)

    part = wq.shape[1]
    small = (PIECES, 32, width)

    def raw(v):
        return pl.BlockSpec(v.shape, lambda i, *l: (0,) * v.ndim)

    return pl.pallas_call(
        front_kernel,
        out_shape=(
            shape(rows, width), shape(PROMPT, width), shape(PROMPT, width), shape(rows, width), shape(rows, width),
            shape(rows, width), jax.ShapeDtypeStruct((pairs, blocks, 8, CLEN), F32),
            shape(rows, width), shape(PROMPT, width), shape(PROMPT, width),
            shape(3, PIECES * part, width), shape(PIECES, *wp.shape), shape(PIECES, *wi.shape),
            shape(PIECES, *wo.shape), shape(*small),
        ),
        grid_spec=pltpu.PrefetchScalarGridSpec(
            num_scalar_prefetch=2,
            grid=(pairs,),
            in_specs=[whole(rows), raw(gain), raw(shift), raw(bqv), raw(b_in), ANY, ANY, ANY, ANY],
            out_specs=[r, p, p, r, r, r, logs, whole(rows), whole(PROMPT), ANY, ANY, ANY, ANY, ANY, ANY],
            scratch_shapes=[
                pltpu.VMEM((PROMPT, width), BF),
                pltpu.VMEM((3, PIECES * part, width), BF),
                pltpu.VMEM(small, BF),
                pltpu.VMEM((PROMPT, 256), BF),
                pltpu.VMEM((144, PROMPT), BF),
                pltpu.SemaphoreType.DMA((2, PROMPT // CLEN)),
                pltpu.SemaphoreType.DMA((2, PROMPT // CLEN)),
                pltpu.SemaphoreType.DMA((7, 5)),
                pltpu.SemaphoreType.DMA((7, 5)),
                pltpu.SemaphoreType.DMA((4,)),
            ],
        ),
        compiler_params=pltpu.CompilerParams(collective_id=0, has_side_effects=True, vmem_limit_bytes=62 << 20),
        cost_estimate=pl.CostEstimate(flops=cells * 256 * 4, transcendentals=cells, bytes_accessed=4 << 20),
        name="front",
    )(plen, conts, x, gain, shift, bqv, b_in, wq, wp, wi, wo)


STAGES = 7


def chunk_rows(rows, dp):
    unit = 16 * (min(dp, NEAR) // 2)
    return -(-rows // unit) * unit


class Sums:
    def __init__(self, me, half, held, scratch):
        self.me, self.half, self.held = me, half, held
        (self.r1, self.r3, self.xr, self.yr, self.zr, self.own,
         self.core_s, self.core_r, self.xs, self.ys, self.zs, self.zrs, self.fs, self.frs, self.gs) = scratch
        self.chunks, self.rows, self.width = self.r1.shape
        self.wide = self.width // 2
        self.share = self.rows // half
        self.mine = pl.ds(pl.multiple_of(me.p * self.wide, 128), self.wide)
        self.other = pl.ds(pl.multiple_of((1 - me.p) * self.wide, 128), self.wide)

    @staticmethod
    def scratch(chunks, rows, width, half):
        def buf(*s, dtype=BF):
            return pltpu.VMEM((chunks,) + s, dtype)

        def dma(n):
            return pltpu.SemaphoreType.DMA((chunks, n))

        wide = width // 2
        return [
            buf(rows, width), buf(rows, width), buf(rows, width), buf(rows, wide),
            buf(half, rows // half, wide), buf(rows // half, wide, dtype=F32),
            dma(2), dma(2), dma(2), dma(2), dma(half), dma(half), dma(half), dma(half), dma(2),
        ]

    def from_core(self, c, i, src=None):
        into = (self.r1, self.r3)[i].at[c]
        return remote(into if src is None else src, into, self.core_s.at[c, i], self.core_r.at[c, i], self.me.core)

    def across(self, c):
        return remote(self.held(c, 2), self.xr.at[c], self.xs.at[c, 0], self.xs.at[c, 1], self.me.x)

    def pair(self, c):
        return remote(self.held(c, 0).at[:, self.other], self.yr.at[c], self.ys.at[c, 0], self.ys.at[c, 1], self.me.y)

    def rows_of(self, k):
        at = lax.rem(self.me.z + k, self.half) * self.share
        return pl.ds(pl.multiple_of(at, 16), self.share)

    def rest(self, c, k):
        return remote(self.held(c, 0).at[self.rows_of(k), self.mine], self.zr.at[c, k],
                      self.zs.at[c, k], self.zrs.at[c, k], self.me.along(k, self.half))

    def back(self, c, k):
        spot = self.xr.at[c, self.rows_of(0), self.mine]
        return remote(spot, spot, self.fs.at[c, k], self.frs.at[c, k], self.me.along(k, self.half))

    def back_pair(self, c):
        spot = self.xr.at[c, :, self.mine]
        return remote(spot, spot, self.gs.at[c, 0], self.gs.at[c, 1], self.me.y)

    def start(self, c, i, src):
        self.from_core(c, i, src).start()

    def blocks(self, body):
        def one(k, _):
            body(pl.ds(pl.multiple_of(k * self.share, 16), self.share))
            return 0

        lax.fori_loop(0, self.half, one, 0)

    def to_chip(self, c):
        self.from_core(c, 1).wait_recv()
        g2 = self.held(c, 2)

        def body(s):
            g2[s, :] = (g2[s, :].astype(F32) + self.r3[c, s, :].astype(F32)).astype(BF)

        self.blocks(body)
        self.across(c).start()

    def term(self, c, s, lanes):
        g0 = self.held(c, 0)
        return g0[s, lanes].astype(F32) + self.r1[c, s, lanes].astype(F32) + self.xr[c, s, lanes].astype(F32)

    def to_pair(self, c):
        self.from_core(c, 0).wait()
        self.across(c).wait()
        g0 = self.held(c, 0)

        def body(s):
            g0[s, self.other] = self.term(c, s, self.other).astype(BF)

        self.blocks(body)
        self.pair(c).start()

    def to_rest(self, c):
        self.pair(c).wait()
        g0 = self.held(c, 0)
        at = self.rows_of(0)
        self.own[c] = self.term(c, at, self.mine) + self.yr[c, at, :].astype(F32)

        def body(s):
            g0[s, self.mine] = (self.term(c, s, self.mine) + self.yr[c, s, :].astype(F32)).astype(BF)

        self.blocks(body)
        for k in range(1, self.half):
            self.rest(c, k).start()

    def to_back(self, c):
        total = self.own[c]
        for k in range(1, self.half):
            self.rest(c, k).wait()
            total = total + self.zr[c, k].astype(F32)
        self.xr[c, self.rows_of(0), self.mine] = total.astype(BF)
        for k in range(1, self.half):
            self.back(c, k).start()

    def to_back_pair(self, c):
        for k in range(1, self.half):
            self.back(c, k).wait()
        self.back_pair(c).start()

    def finish(self, c):
        self.back_pair(c).wait()

    def progress(self, plan, slot):
        steps = [None, self.to_chip, self.to_pair, self.to_rest, self.to_back, self.to_back_pair]
        for k in plan["order"]:
            since = slot - plan[k]
            c = lax.div(since, plan["gap"])
            due = since >= 0
            if plan["gap"] > 1:
                due = jnp.logical_and(due, lax.rem(since, plan["gap"]) == 0)

            @pl.when(jnp.logical_and(due, c < self.chunks))
            def _():
                steps[k](c)

    def finish_all(self):
        for c in range(self.chunks):
            self.finish(c)


class SmallSum:
    def __init__(self, me, half, sm, scratch):
        self.me, self.half, self.sm = me, half, sm
        self.got, self.z, self.s, self.r = scratch

    @staticmethod
    def scratch(rows, width, half):
        return [
            pltpu.VMEM((4, rows, width), F32),
            pltpu.VMEM((half, rows, width), F32),
            pltpu.SemaphoreType.DMA((4 + half,)),
            pltpu.SemaphoreType.DMA((4 + half,)),
        ]

    def copy(self, i):
        src, device = [(1, self.me.core), (3, self.me.core), (2, self.me.x), (0, self.me.y)][i]
        return remote(self.sm.at[src], self.got.at[i], self.s.at[i], self.r.at[i], device)

    def rest(self, k):
        return remote(self.sm.at[0], self.z.at[k], self.s.at[4 + k], self.r.at[4 + k], self.me.along(k, self.half))

    def start(self):
        self.copy(1).start()
        self.copy(0).start()

    def to_chip(self):
        self.copy(1).wait()
        self.sm[2] = self.sm[2] + self.got[1]
        self.copy(2).start()

    def to_pair(self):
        self.copy(0).wait()
        self.copy(2).wait()
        self.sm[0] = self.sm[0] + self.got[0] + self.got[2]
        self.copy(3).start()

    def to_rest(self):
        self.copy(3).wait()
        self.sm[0] = self.sm[0] + self.got[3]
        for k in range(1, self.half):
            self.rest(k).start()

    def finish(self):
        total = self.sm[0]
        for k in range(1, self.half):
            self.rest(k).wait()
            total = total + self.z[k]
        return total


SUB = 3
FFN_PLAN = {"gap": 2, "order": (5, 4, 3, 2, 1), 1: 6, 2: 12, 3: 15, 4: 18, 5: 21}
QKV_PLAN = {"gap": 2, "order": (5, 4, 3, 2, 1), 1: 24, 2: 30, 3: 33, 4: 36, 5: 39}
QKV_START = (21, 30)
SMALL_PLAN = (31, 34, 37, 40)
PROMPT_PLAN = (37,)
LAST_SLOT = 45


def back_kernel(half, grid_pairs, plen, conts, q_ref, kp_ref, vp_ref, ko_ref, vo_ref, lse_ref,
                w_any, an_any, anp_any, x_ref, px_any, ctx_ref, wp_any, wi_any, wo_any, wp_own, wi_own, wo_own, bias_ref,
                g1_ref, b_proj_ref, ln2_g_ref, ln2_b_ref, b_out_ref, dy_any,
                lo_any, ig_any, ffn_out, qkv_out, small_out,
                wbuf, wp_ref, l_s, dy, hid, gs, g0, g2,
                kx, vx, kt_s, acc, dqt, dkt, dvt, prompt_acc, own_acc, share_s, gq, sm, qv, sums,
                came, over, tail, w_s, f_s, p_s, p_r, o_s, *scratch):
    me = Peers()
    step = pl.program_id(0)
    rows = x_ref.shape[0]
    width = x_ref.shape[1]
    blocks = rows // CLEN
    prompt = kp_ref.shape[0]
    chunks = prompt // CLEN
    part = width // PIECES
    feats = grid_pairs // 2 * 128
    per = width // part
    ffn_scratch, qkv_scratch, small_scratch = scratch[:15], scratch[15:30], scratch[30:]
    branch, gmi, gel, gp, mlp, mlpt = prompt_acc, own_acc, gq.at[0], gq.at[1], gq.at[2], share_s.at[pl.ds(0, width)]
    an_ref = wbuf.at[pl.ds(0, rows)]
    anp_ref = wbuf.at[pl.ds(rows, prompt)]
    loads = [pltpu.make_async_copy(a, b, l_s.at[i]) for i, (a, b) in enumerate(((an_any, an_ref), (anp_any, anp_ref)))]

    def w_rows(j):
        return pl.ds(rows + prompt + j * feats, feats)

    def load_w(unit):
        return [
            pltpu.make_async_copy(w_any.at[j, pl.ds(unit * feats, feats)], wbuf.at[w_rows(j)], w_s.at[j]) for j in range(3)
        ]

    def ffn_rows(k, j):
        return pl.ds(pl.multiple_of((lax.rem(k, 2) * 2 + j) * width, 16), width)

    def load_ffn(k, own=False):
        srcs = (wi_own, wo_own) if own else [a.at[PIECES - 1 - k] for a in (wi_any, wo_any)]
        return [
            pltpu.make_async_copy(a, wbuf.at[ffn_rows(k, j)], f_s.at[lax.rem(k, 2), j]) for j, a in enumerate(srcs)
        ]

    px_parts = [(at, min(part, prompt - at)) for at in range(0, prompt, part)]
    load_px = [
        pltpu.make_async_copy(px_any.at[pl.ds(at, m)], gs.at[i, pl.ds(0, m)], l_s.at[4 + i]) for i, (at, m) in enumerate(px_parts)
    ]
    g1, b_proj, ln2_g, ln2_b, b_out = (flat(v) for v in (g1_ref, b_proj_ref, ln2_g_ref, ln2_b_ref, b_out_ref))

    def piece_rows(r):
        return pl.ds(pl.multiple_of(r * part, 16), part)

    ffn = Sums(me, half, lambda c, r: (g0 if r == 0 else g2).at[c], ffn_scratch)
    qkv = Sums(me, half, lambda c, r: gq.at[c, piece_rows(r)], qkv_scratch)
    smalls = SmallSum(me, half, sm, small_scratch)
    n = prompt // 2
    spare = rows - n
    mine = pl.ds(pl.multiple_of(me.odd * n, 16), n)
    side = remote(share_s.at[pl.ds(pl.multiple_of((1 - me.odd) * n, 16), n)], came, p_s.at[0], p_r.at[0], me.core)
    across = remote(share_s.at[mine], over, p_s.at[1], p_r.at[1], me.x)
    end = remote(share_s.at[pl.ds(pl.multiple_of(me.odd * n, 16), spare)], tail, p_s.at[2], p_r.at[2], me.core)

    def block_rows(b):
        return slice(b * CLEN, (b + 1) * CLEN)

    def normal_of(x):
        x = x - jnp.mean(x, axis=-1, keepdims=True)
        scale = lax.rsqrt(jnp.mean(x * x, axis=-1, keepdims=True) + EPS)
        return x * scale, scale

    def norm_back(e, normal, scale):
        return scale * (e - jnp.mean(e, axis=-1, keepdims=True) - normal * jnp.mean(e * normal, axis=-1, keepdims=True))

    @pl.when(step == 0)
    def _():
        got = pltpu.make_async_copy(dy_any, dy, o_s.at[0])
        first = pl.ds(0, part)
        rest = pl.ds(part, width - part)
        wp = [
            pltpu.make_async_copy(wp_own, wp_ref.at[first], l_s.at[2]),
            pltpu.make_async_copy(wp_any.at[rest], wp_ref.at[rest], l_s.at[3]),
        ]
        for c in wp:
            c.start()
        got.start()
        for c in load_ffn(0) + load_ffn(1):
            c.start()
        enter([me.core, me.x, me.y] + [me.along(k, half) for k in range(1, half)])
        for c in wp:
            c.wait()
        for b in range(blocks):
            at = block_rows(b)
            h = x_ref[at, :].astype(F32) + nn(ctx_ref[at, :], wp_ref[...]) + b_proj
            hid[at, :] = h
            normal, _ = normal_of(h)
            m = (normal * ln2_g + ln2_b).astype(BF)
            mlp[at, :] = m
            mlpt[:, at] = transposed(m).astype(BF)
        got.wait()
        branch[...] = jnp.zeros_like(branch)
        gmi[...] = jnp.zeros_like(gmi)
        sums[...] = jnp.zeros_like(sums)

    def ffn_block(b):
        at = pl.ds(pl.multiple_of(b * CLEN, CLEN), CLEN)
        r = PIECES - 1 - step
        wi = wbuf[ffn_rows(step, 0), :]
        wo = wbuf[ffn_rows(step, 1), :]
        pre = nn(mlp[at, :], wi) + bias_ref[r, 16:17, :].astype(F32)
        cdf = 0.5 * (1.0 + lax.erf(pre * (0.5**0.5)))
        pdf = jnp.exp(-0.5 * pre * pre) * 0.3989422804014327
        g = (pre * cdf).astype(BF)
        d = (nt(dy[at, :], wo) * (cdf + pre * pdf)).astype(BF)
        gel[at, :] = g
        gp[at, :] = d
        branch[at, :] += nn(g, wo)
        gmi[at, :] += nt(d, wi)
        sums[pl.ds(r, 1), :] += jnp.sum(d.astype(F32), axis=0, keepdims=True)

    def weight_grads():
        @pl.when(step == 2)
        def _():
            for c in range(2 * per):
                ffn.from_core(c, 1, gs.at[c]).wait_send()

        def one(j, _):
            two = pl.ds(pl.multiple_of(j * 2 * part, 128), 2 * part)
            both = (nn(mlpt[two, :], gp[...]), tn(gel[:, two], dy[...]))
            for k, got in enumerate(both):
                got = got.astype(BF).reshape(2, part, width)
                spot = pl.ds(2 * j + k * per, 2)

                @pl.when(lax.rem(step, 2) == 0)
                def _():
                    gs[spot] = got

                @pl.when(step == 1)
                def _():
                    g2[spot] = got

                @pl.when(step == 3)
                def _():
                    g0[spot] = got

            return 0

        lax.fori_loop(0, per // 2, one, 0)
        for at, i in ((0, 1), (2, 0)):
            @pl.when(step == at)
            def _():
                for c in range(2 * per):
                    ffn.start(c, i, gs.at[c])

    def after_ffn():
        for b in range(blocks):
            at = block_rows(b)
            g = gmi[at, :]
            h = hid[at, :]
            d = dy[at, :].astype(F32)
            normal, scale = normal_of(h)
            mlp[at, :] = (h + (branch[at, :] + b_out)).astype(BF)
            gh = d + norm_back(g * ln2_g, normal, scale)
            hid[at, :] = gh
            ga = gh.astype(BF)
            gel[at, :] = ga
            for k, v in enumerate((ga.astype(F32), g * normal, g, d)):
                sums[PIECES + k : PIECES + k + 1, :] += jnp.sum(v, axis=0, keepdims=True)
            dy[at, :] = nt(ga, wp_ref[...]).astype(BF)
        for c in loads + load_w(1):
            c.start()
        spots = (g0.at[2 * per], gs.at[2 * per + 1], g2.at[2 * per], gs.at[2 * per])
        for r in range(0, PIECES, 2):
            got = tn(ctx_ref[:, r * part : (r + 2) * part], gel[...]).astype(BF)
            spots[r][...] = got[:part]
            spots[r + 1][...] = got[part:]
        ffn.start(2 * per, 1, gs.at[2 * per])
        ffn.start(2 * per, 0, gs.at[2 * per + 1])
        pltpu.make_async_copy(mlp, lo_any, o_s.at[1]).start()
        own_acc[...] = jnp.zeros_like(own_acc)
        prompt_acc[...] = jnp.zeros_like(prompt_acc)

    sp = step - PIECES
    spot = lax.rem(jnp.maximum(sp, 0), grid_pairs // 2)
    pair = lax.rem(jnp.maximum(sp, 0) + grid_pairs // 2, grid_pairs)
    lanes = pl.ds(pl.multiple_of(pair * 128, 128), 128)
    attending = jnp.logical_and(sp >= 0, sp < grid_pairs)

    @pl.when(attending)
    def _():
        acc[...] = jnp.zeros_like(acc)
        kx[:prompt] = wide_keys(kp_ref[...], plen[0], 0)
        vx[:prompt] = wide_values(vp_ref[...])
        vx[prompt:] = wide_values(vo_ref[...])
        kt_s[:, :prompt] = transposed(kp_ref[...]).astype(BF)
        kt_s[:, prompt:] = transposed(ko_ref[...]).astype(BF)
        for b in range(blocks):
            at = block_rows(b)
            kx[prompt + b * CLEN : prompt + (b + 1) * CLEN] = wide_keys(ko_ref[at, :], own_length(conts, me.t, blocks, b), 0)

    def block(b):
        at = pl.ds(pl.multiple_of(b * CLEN, CLEN), CLEN)
        own = pl.ds(pl.multiple_of(prompt + b * CLEN, CLEN), CLEN)
        q = q_ref[at, :]
        do = dy[at, lanes]
        q2 = wide_queries(q)
        do2 = wide_grads(do, ctx_ref[at, lanes])
        qt = transposed(q).astype(BF)
        dot = transposed(do).astype(BF)
        logs = jnp.concatenate([lse_ref[0, b, 0:1, :], lse_ref[0, b, 1:2, :]], axis=1)

        def scores(keys):
            p = jnp.exp(nt(kx[keys, :], q2) - logs)
            ds = (p * nt(vx[keys, :], do2)).astype(BF)
            p = p.astype(BF)
            parts = []
            for left, m in ((qt, ds), (dot, p)):
                parts.append([nt(left[64 * h : 64 * h + 64], m[:, h * CLEN : (h + 1) * CLEN]) for h in range(2)])
            return parts, nn(kt_s[:, keys], ds)

        (dk, dv), dq = scores(pl.ds(0, prompt))
        for h in range(2):
            rows_h = slice(64 * h, 64 * h + 64)
            acc[0, rows_h, :] += dk[h]
            acc[1, rows_h, :] += dv[h]
        (dk, dv), dq_own = scores(own)
        dkt[spot, :, own] = (jnp.concatenate(dk, axis=0) * 0.125).astype(BF)
        dvt[spot, :, own] = jnp.concatenate(dv, axis=0).astype(BF)
        dq = dq + dq_own
        dqt[spot, :, at] = (jnp.concatenate([dq[:64, :CLEN], dq[64:, CLEN:]], axis=0) * 0.125).astype(BF)

        @pl.when(b == blocks - 1)
        def _():
            dkt[spot, :, :prompt] = (acc[0] * 0.125).astype(BF)
            dvt[spot, :, :prompt] = acc[1].astype(BF)

    def sub_step(sub, _):
        slot = step * SUB + sub
        ffn.progress(FFN_PLAN, slot)

        def at(k, body):
            @pl.when(slot == k)
            def _():
                body()

        def qkv_start(i):
            for c in range(3):
                qkv.start(c, i, gq.at[c, piece_rows(1 + 2 * i)])

        def prompt_chip():
            side.wait()
            share_s[mine, :] = (share_s[mine, :].astype(F32) + came[...].astype(F32)).astype(BF)

            @pl.when(me.t >= 2)
            def _():
                across.start()

        def qkv_sent():
            for c in range(3):
                qkv.from_core(c, 1, gq.at[c, piece_rows(3)]).wait_send()

        at(QKV_START[0], lambda: qkv_start(1))
        at(QKV_START[1], lambda: qkv_start(0))
        at(QKV_START[1], qkv_sent)
        qkv.progress(QKV_PLAN, slot)
        at(SMALL_PLAN[0], smalls.start)
        at(SMALL_PLAN[1], smalls.to_chip)
        at(SMALL_PLAN[2], smalls.to_pair)
        at(SMALL_PLAN[3], smalls.to_rest)
        at(PROMPT_PLAN[0], prompt_chip)

        @pl.when(step < PIECES)
        def _():
            ffn_block(sub)

        @pl.when(attending)
        def _():
            block(sub)

        return 0

    @pl.when(step < PIECES)
    def _():
        for c in load_ffn(step, True):
            c.wait()

    lax.fori_loop(0, SUB, sub_step, 0)

    @pl.when(step < PIECES)
    def _():
        @pl.when(step == 0)
        def _():
            for c in load_ffn(2):
                c.start()

        @pl.when(step == 1)
        def _():
            for c in load_ffn(3, True):
                c.start()

        weight_grads()

    @pl.when(step == PIECES - 1)
    def _():
        after_ffn()

    @pl.when(jnp.logical_and(attending, spot == grid_pairs // 2 - 1))
    def _():
        late = sp < grid_pairs // 2

        @pl.when(late)
        def _():
            for c in loads + [pltpu.make_async_copy(mlp, lo_any, o_s.at[1])]:
                c.wait()

        for c in load_w(0):
            c.wait()
        dq, dk, dv = (r[...].reshape(feats, -1) for r in (dqt, dkt, dvt))
        an = an_ref[...]
        anp = anp_ref[...]
        for j, d in enumerate((dq, dk, dv)):
            g = nn(d, an) if j == 0 else nn(d[:, prompt:], an) + nn(d[:, :prompt], anp)
            gq[j, pl.ds(pl.multiple_of(jnp.where(late, feats, 0), 16), feats), :] = g.astype(BF)
        sum_q = jnp.sum(dq.astype(F32), axis=1, keepdims=True)
        sum_v = jnp.sum(dv.astype(F32), axis=1, keepdims=True)
        both = jnp.concatenate([jnp.broadcast_to(sum_q, (feats, 128)), jnp.broadcast_to(sum_v, (feats, 128))], axis=1).T
        unit_lanes = pl.ds(pl.multiple_of(jnp.where(late, feats, 0), 128), feats)
        qv[0:1, unit_lanes] = both[0:1]
        qv[1:2, unit_lanes] = both[128:129]
        def turned(ref, at, j):
            return tn(ref[:, :, at : at + CLEN].reshape(feats, CLEN), wbuf[w_rows(j), :])

        for b in range(blocks):
            at = b * CLEN
            own_acc[at : at + CLEN, :] += (
                turned(dqt, at, 0) + turned(dkt, prompt + at, 1) + turned(dvt, prompt + at, 2)
            )
        for c in range(chunks):
            at = c * CLEN
            prompt_acc[at : at + CLEN, :] += turned(dkt, at, 1) + turned(dvt, at, 2)

        @pl.when(late)
        def _():
            for c in load_w(0):
                c.start()

        @pl.when(jnp.logical_not(late))
        def _():
            for c in load_px:
                c.start()

    @pl.when(sp == grid_pairs - 1)
    def _():
        for c in range(chunks):
            at = block_rows(c)
            share_s[at, :] = prompt_acc[at, :].astype(BF)
        side.start()
        sum_g = jnp.zeros((1, width), F32)
        sum_c = jnp.zeros((1, width), F32)
        raws = [(own_acc, at, m, x_ref.at[pl.ds(at, m)]) for at, m in [(part * k, part) for k in range(rows // part)]]
        raws += [(prompt_acc, at, m, gs.at[i, pl.ds(0, m)]) for i, (at, m) in enumerate(px_parts)]
        for i, (grad, at, m, raw) in enumerate(raws):
            if grad is prompt_acc:
                load_px[i - rows // part].wait()
            normal, _ = normal_of(raw[...].astype(F32))
            g = grad[at : at + m, :]
            sum_g = sum_g + jnp.sum(g * normal, axis=0, keepdims=True)
            sum_c = sum_c + jnp.sum(g, axis=0, keepdims=True)
        for r in range(PIECES):
            sm[r] = jnp.zeros_like(sm[r])
            sm[r, 0:1, :] = sums[r : r + 1, :]
            sm[r, 1:5, :] = sums[PIECES : PIECES + 4, :]
            for i in range(2):
                row = qv[i : i + 1, :]
                sm[r, 8 + i : 9 + i, :] = row if r == 0 else pltpu.roll(row, width - r * part, 1)
            sm[r, 10:11, :] = sum_g
            sm[r, 11:12, :] = sum_c

    @pl.when(step == pl.num_programs(0) - 1)
    def _():
        ffn.finish_all()
        copies = [pltpu.make_async_copy(ffn.xr, ffn_out, o_s.at[2])]
        copies[0].start()
        ffn.from_core(2 * per, 1, gs.at[2 * per]).wait_send()

        @pl.when(me.t >= 2)
        def _():
            across.wait_send()

        @pl.when(me.t < 2)
        def _():
            across.wait_recv()
            share_s[mine, :] = (share_s[mine, :].astype(F32) + over[...].astype(F32)).astype(BF)

        @pl.when(me.t == 1)
        def _():
            end.start()
            for at in range(0, n - spare, CLEN):
                own_acc[at : at + CLEN, :] += share_s[n + spare + at : n + spare + at + CLEN, :].astype(F32)
            end.wait_send()

        @pl.when(me.t == 0)
        def _():
            for at in range(0, n, CLEN):
                own_acc[at : at + CLEN, :] += share_s[at : at + CLEN, :].astype(F32)
            end.wait_recv()
            own_acc[n:, :] += tail[...].astype(F32)

        for b in range(blocks):
            at = block_rows(b)
            normal, scale = normal_of(x_ref[at, :].astype(F32))
            hid[at, :] += norm_back(own_acc[at, :] * g1, normal, scale)
        last = pltpu.make_async_copy(hid, ig_any, o_s.at[0])
        last.start()
        qkv.finish_all()
        copies.append(pltpu.make_async_copy(qkv.xr, qkv_out, o_s.at[3]))
        copies[1].start()
        small_out[...] = smalls.finish()
        for c in copies + [last]:
            c.wait()


def back_call(plen, conts, q, kp, vp, ko, vo, lse, wq_all, an, anp, x, px, ctx, wp, wi_all, wo_all, wp_own, wi_own, wo_own, ws_all, vecs, dy):
    rows, width = q.shape
    prompt = kp.shape[0]
    blocks = rows // CLEN
    pairs = width // 128
    part = width // PIECES
    half = min(lax.axis_size("dp"), NEAR) // 2
    cells = rows * (prompt + CLEN) * pairs * 2
    n_ffn = 2 * (width // part) + 1
    steps = -(-LAST_SLOT // SUB)
    assert blocks == SUB and wi_all.shape[1:] == (width, width) and rows == width and part % (16 * half) == 0
    small_n = 16

    def pair(i):
        return lax.rem(jnp.clip(i - PIECES, 0, pairs - 1) + pairs // 2, pairs)

    def col(n):
        return pl.BlockSpec((n, 128), lambda i, *l: (0, pair(i)))

    def whole(*s):
        return pl.BlockSpec(s, lambda i, *l: (0,) * len(s), pipeline_mode=pl.Buffered(1))

    r, p = col(rows), col(prompt)
    logs = pl.BlockSpec((1, blocks, 8, CLEN), lambda i, *l: (pair(i), 0, 0, 0))
    return pl.pallas_call(
        functools.partial(back_kernel, half, pairs),
        out_shape=(
            jax.ShapeDtypeStruct((rows, width), BF),
            jax.ShapeDtypeStruct((rows, width), F32),
            jax.ShapeDtypeStruct((n_ffn, part, width), BF),
            jax.ShapeDtypeStruct((3, part, width), BF),
            jax.ShapeDtypeStruct((small_n, width), F32),
        ),
        grid_spec=pltpu.PrefetchScalarGridSpec(
            num_scalar_prefetch=2,
            grid=(steps,),
            in_specs=[r, p, p, r, r, logs, ANY, ANY, ANY, whole(rows, width),
                      ANY, whole(rows, width)] + [ANY] * 6 + [whole(*ws_all.shape)] + [whole(width)] * 5 + [ANY],
            out_specs=[ANY, ANY, ANY, ANY, pl.BlockSpec((small_n, width), lambda i, *l: (0, 0))],
            scratch_shapes=[
                pltpu.VMEM((max(4 * width, rows + prompt + 3 * pairs // 2 * 128), width), BF),
                pltpu.VMEM((width, width), BF),
                pltpu.SemaphoreType.DMA((4 + -(-prompt // part),)),
                pltpu.VMEM((rows, width), BF),
                pltpu.VMEM((rows, width), F32),
                pltpu.VMEM((n_ffn + 1, part, width), BF),
                pltpu.VMEM((n_ffn, part, width), BF),
                pltpu.VMEM((n_ffn, part, width), BF),
                pltpu.VMEM((prompt + rows, 256), BF),
                pltpu.VMEM((prompt + rows, 256), BF),
                pltpu.VMEM((128, prompt + rows), BF),
                pltpu.VMEM((2, 128, prompt), F32),
                pltpu.VMEM((pairs // 2, 128, rows), BF),
                pltpu.VMEM((pairs // 2, 128, prompt + rows), BF),
                pltpu.VMEM((pairs // 2, 128, prompt + rows), BF),
                pltpu.VMEM((prompt, width), F32),
                pltpu.VMEM((rows, width), F32),
                pltpu.VMEM((prompt, width), BF),
                pltpu.VMEM((3, width, width), BF),
                pltpu.VMEM((PIECES, small_n, width), F32),
                pltpu.VMEM((8, width), F32),
                pltpu.VMEM((8, width), F32),
                pltpu.VMEM((prompt // 2, width), BF),
                pltpu.VMEM((prompt // 2, width), BF),
                pltpu.VMEM((rows - prompt // 2, width), BF),
                pltpu.SemaphoreType.DMA((3,)),
                pltpu.SemaphoreType.DMA((2, 2)),
                pltpu.SemaphoreType.DMA((3,)),
                pltpu.SemaphoreType.DMA((3,)),
                pltpu.SemaphoreType.DMA((4,)),
            ]
            + Sums.scratch(n_ffn, part, width, half)
            + Sums.scratch(3, part, width, half)
            + SmallSum.scratch(small_n, width, half),
        ),
        compiler_params=pltpu.CompilerParams(collective_id=1, has_side_effects=True, vmem_limit_bytes=63 << 20),
        cost_estimate=pl.CostEstimate(flops=cells * 256 * 10, transcendentals=cells, bytes_accessed=16 << 20),
        name="back",
    )(plen, conts, q, kp, vp, ko, vo, lse, wq_all, an, anp, x, px, ctx, wp, wi_all, wo_all, wp_own, wi_own, wo_own, ws_all, *vecs, dy)


def shards(layer_in, prompt_len, cont_len, w_qkv, b_qv, w_proj, b_proj, ln1_gain, ln1_bias,
           ln2_gain, ln2_bias, w_in, b_in, w_out, b_out, out_grad):
    rows, width = layer_in.shape
    part = w_qkv.shape[2]
    (q, kp, vp, ko, vo, ctx, lse, attn_input, prompt_input, prompt_rows, wq_all, wp_all, wi_all, wo_all, ws_all) = front_call(
        prompt_len, cont_len, layer_in, ln1_gain, ln1_bias, b_qv, b_in, w_qkv.transpose(0, 2, 1), w_proj, w_in, w_out
    )
    layer_out, in_grad, ffn, qkv, small = back_call(
        prompt_len, cont_len, q, kp, vp, ko, vo, lse, wq_all, attn_input, prompt_input, layer_in, prompt_rows, ctx,
        wp_all.reshape(width, width), wi_all, wo_all, w_proj, w_in, w_out, ws_all,
        (ln1_gain, b_proj, ln2_gain, ln2_bias, b_out), out_grad
    )
    ffn = beyond(ffn.astype(F32))
    qkv = beyond(qkv.astype(F32))
    small = beyond(small)
    per = ffn.shape[0] // 2
    grad_w_in = ffn[:per].reshape(width, -1)
    grad_w_out = ffn[per : 2 * per].reshape(-1, width)
    return (layer_out, in_grad, qkv.transpose(0, 2, 1), small[8:10, :part], ffn[2 * per], small[1], small[10], small[11],
            small[2], small[3], grad_w_in, small[0, : w_in.shape[1]], grad_w_out, small[4])


def solution(mesh):
    in_specs = (
        P(("dp", "tensor"), None),
        P("dp"),
        P("dp", None),
        P(None, None, "tensor"),
        P(None, "tensor"),
        P("tensor", None),
        P(),
        P(),
        P(),
        P(),
        P(),
        P(None, "tensor"),
        P("tensor"),
        P("tensor", None),
        P(),
        P(("dp", "tensor"), None),
    )
    out_specs = (
        P(("dp", "tensor"), None),
        P(("dp", "tensor"), None),
        P(None, None, "tensor"),
        P(None, "tensor"),
        P("tensor", None),
        P(),
        P(),
        P(),
        P(),
        P(),
        P(None, "tensor"),
        P("tensor"),
        P("tensor", None),
        P(),
    )
    return jax.shard_map(shards, mesh=mesh, in_specs=in_specs, out_specs=out_specs, check_vma=False)
```
